32 devices in a mesh: parts: 2 (over x), pts: 16 (over z, y, core).
Axes of the slice: x: 2, y: 2, z: 4, core: 2. Of those that a mesh axis runs over, the one named last changes fastest.
Arguments:
- grid_weights: float32 [256, 128, 128], P(('parts', 'pts')), parts along dimension 0, may hold values from -6 to 6
- direction: float32 [256, 128, 128], P(('parts', 'pts')), parts along dimension 0, may hold values from -6 to 6
- kern_x: float32 [128, 128], replicated
- kern_y: float32 [128, 128], replicated
- kern_z: float32 [128, 128], replicated
- interp: bfloat16 [4096, 128, 256], P(('parts', 'pts')), parts along dimension 0, may hold values from -4 to 4
- block_corner: int32 [3, 4096], P(None, ('parts', 'pts')), parts along dimension 1, may hold values from 0 to 120, as said below
- block_offsets: int32 [4096, 256], P(('parts', 'pts')), parts along dimension 0, may hold values from 0 to 2047, as said below
- labels: int32 [4096, 128], P(('parts', 'pts')), parts along dimension 0, may hold values 0 or 1
- trial_steps: float32 [5], replicated, may hold values from 0.05 to 2
- accept: int32 [1], replicated, may hold values from 0 to 4
Outputs:
- new_weights: float32 [256, 128, 128], P(('parts', 'pts')), parts along dimension 0
- grid_gradient: float32 [256, 128, 128], P(('parts', 'pts')), parts along dimension 0
- curvature: float32 [4096, 128], P(('parts', 'pts')), parts along dimension 0
- trial_objective: float32 [10], P('parts'), parts along dimension 0
- trial_slope: float32 [10], P('parts'), parts along dimension 0
The draws below stay inside these ranges and needn't reach their ends.
There are 2 independent parts, one for each index of `parts`. The reference program is written for one: setup_inputs(seed, part) draws one part's arguments, and reference() takes and returns one part's arrays. A program takes and returns all parts, laid end to end along the dimension named above; an argument that names none is the same for every part. Nothing has to cross between parts.
Inputs may be any that keep to these rules, and one draw needn't show every extreme that they name: `block_corner`: row 0 lies in 0 to 112, row 1 in 0 to 112, row 2 in 0 to 120. `block_offsets`: the 256 offsets of one block are distinct.
All inputs are finite; a program needn't handle non-finite values. No bound on the sum of `labels` on one device may be relied on, other than what follows from the above.
Results may differ from the reference program's by a relative error of at most 0.0075.
The reference program's roundings to bfloat16 on the way count: a program that leaves them out, or rounds other values in their place, can miss the bound.
Values may be sent and summed in bfloat16 or wider, within the bound.
A program may use at most 128 MiB of HBM per device.

```python
import math
import jax
import jax.numpy as jnp
from jax import lax

GX = 128
GY = 128
GZ = 128
BOXX = 16
BOXY = 16
BOXZ = 8
COLS = 256
PTS_BLOCK = 128
NTRIAL = 5
NB = 128
BLOCKS = 2048
POINTS = 262144
N_PTS = 16


def kernel_table(key, size, salt):
    key = jax.random.fold_in(key, salt)
    key_len, key_noise, key_gain = jax.random.split(key, 3)
    length = jax.random.uniform(key_len, (), jnp.float32, 4.0, 16.0)
    noise_scale = 0.15
    position = jnp.arange(size, dtype=jnp.float32)
    spacing = jnp.abs(position[:, None] - position[None, :])
    smooth = jnp.exp(-spacing / length)
    noise = jax.random.normal(key_noise, (size, size), jnp.float32)
    symmetric = (noise + noise.T) * 0.7071
    gains = jax.random.uniform(key_gain, (size,), jnp.float32, 0.7, 1.4)
    table = gains[:, None] * (smooth + noise_scale * symmetric) * gains[None, :] / jnp.sqrt(length)
    return table.astype(jnp.float32)


def draw_kern_x(key, part):
    return kernel_table(key, GX, 11)


def draw_kern_y(key, part):
    return kernel_table(key, GY, 23)


def draw_kern_z(key, part):
    return kernel_table(key, GZ, 37)


def draw_interp(key, part):
    key = jax.random.fold_in(key, 53)
    ratio = 6.0
    base = jnp.clip(jax.random.normal(key, (BLOCKS, PTS_BLOCK, COLS), jnp.float32), -4.0, 4.0)
    level = jnp.arange(BLOCKS, dtype=jnp.float32) / max(BLOCKS - 1, 1)
    scale = jnp.exp(jnp.log(ratio) * level) / jnp.sqrt(ratio)
    table = base * scale[:, None, None] / jnp.sqrt(jnp.float32(COLS))
    return jnp.clip(table, -4.0, 4.0).astype(jnp.bfloat16)


def draw_block_corner(key, part):
    limits = jnp.array([GX - BOXX, GY - BOXY, GZ - BOXZ], jnp.int32)
    corner = jax.random.randint(key, (3, BLOCKS), 0, limits[:, None] + 1)
    corner = corner.at[:, 0].set(limits)
    corner = corner.at[:, BLOCKS - 1].set(0)
    return corner.astype(jnp.int32)


def draw_block_offsets(key, part):
    keys = jax.random.split(key, BLOCKS)

    def choose_cells(one_key):
        return jax.random.permutation(one_key, BOXX * BOXY * BOXZ)[:COLS]
    return jax.vmap(choose_cells)(keys).astype(jnp.int32)


def place_ends(values, rng, smallest, top_value):
    longest = values.shape.index(max(values.shape))
    spots = []
    for shift in (0, 1):
        where = [jax.random.randint(jax.random.fold_in(rng, axis), (), 0, length) for axis, length in enumerate(values.shape)]
        where[longest] = (where[longest] + shift) % values.shape[longest]
        spots.append(tuple(where))
    return values.at[spots[0]].set(smallest).at[spots[1]].set(top_value)


def levels(rng, shape, pieces, smallest, top_value):
    def one(dim, blocks):
        steps = jax.random.uniform(jax.random.fold_in(jax.random.fold_in(rng, 6), dim), (blocks,), jnp.float32, smallest / len(pieces), top_value / len(pieces))
        return jnp.repeat(jnp.exp(steps), shape[dim] // blocks).reshape((-1,) + (1,) * (len(shape) - dim - 1))

    level = one(*pieces[0])
    for cut in pieces[1:]:
        level = level * one(*cut)
    return level


def bell_draw(rng, dims, width, limit, shards=(), held_as=jnp.bfloat16):
    values = width * jax.random.normal(rng, dims, jnp.float32)
    if shards:
        values = values * levels(rng, dims, shards, -0.22, 0.18)
    return jnp.clip(values, -limit, limit).astype(held_as)


def setup_inputs(seed: int = 0, part: int = 0) -> dict:
    key_list = jax.random.split(jax.random.key(seed), 12)
    own_keys = jax.random.split(jax.random.fold_in(key_list[11], part), 12)
    grid_weights = bell_draw(own_keys[0], (GX, GY, GZ), 1.0, 6.0, ((0, 16),), jnp.float32)
    direction = bell_draw(own_keys[1], (GX, GY, GZ), 1.0, 6.0, ((0, 16),), jnp.float32)
    kern_x = draw_kern_x(jax.random.fold_in(key_list[11], 71), part)
    kern_y = draw_kern_y(jax.random.fold_in(key_list[11], 71), part)
    kern_z = draw_kern_z(jax.random.fold_in(key_list[11], 71), part)
    interp = draw_interp(jax.random.fold_in(jax.random.fold_in(key_list[11], part), 71), part)
    block_corner = draw_block_corner(jax.random.fold_in(jax.random.fold_in(key_list[11], part), 71), part)
    block_offsets = draw_block_offsets(jax.random.fold_in(jax.random.fold_in(key_list[11], part), 71), part)
    labels = place_ends((jax.random.randint(own_keys[8], (BLOCKS, PTS_BLOCK), 0, 2) < 1).astype(jnp.int32), jax.random.fold_in(own_keys[8], 1), 0, 1)
    trial_steps = jnp.clip(jnp.exp(jax.random.uniform(key_list[9], (NTRIAL,), jnp.float32, math.log(0.05), math.log(2.0))), 0.05, 2.0)
    accept = jax.random.randint(key_list[10], (1,), 0, NTRIAL).astype(jnp.int32)
    return dict(grid_weights=grid_weights, direction=direction, kern_x=kern_x, kern_y=kern_y, kern_z=kern_z, interp=interp, block_corner=block_corner, block_offsets=block_offsets, labels=labels, trial_steps=trial_steps, accept=accept)


HIGHEST = lax.Precision.HIGHEST


def plane_mix(fields, kern_y, kern_z):
    inner_mix = jnp.einsum('...bc,zc->...bz', fields, kern_z, precision=HIGHEST)
    return jnp.einsum('...xbz,yb->...xyz', inner_mix, kern_y, precision=HIGHEST).astype(jnp.bfloat16)


def depth_mix(partial_value, kern_x):
    return jnp.einsum('xa,...ayz->...xyz', kern_x, partial_value.astype(jnp.float32), precision=HIGHEST)


def cell_ids_of(block_corner, block_offsets):
    plane_off = block_offsets // (BOXY * BOXZ)
    row_off = (block_offsets // BOXZ) % BOXY
    depth_off = block_offsets % BOXZ
    cell_x = block_corner[0][:, None] + plane_off
    cell_y = block_corner[1][:, None] + row_off
    cell_z = block_corner[2][:, None] + depth_off
    return ((cell_x * GY + cell_y) * GZ + cell_z).astype(jnp.int32)


def interpolate(interp, values):
    count_fields = values.shape[0]
    groups = interp.reshape(N_PTS, NB, PTS_BLOCK, COLS)
    grouped = jnp.moveaxis(values.reshape(count_fields, N_PTS, NB, COLS), 1, 0)

    def one_group(operands):
        return jnp.einsum('bpc,fbc->fbp', operands[0].astype(jnp.float32), operands[1].astype(jnp.float32), precision=HIGHEST)

    result = lax.map(one_group, (groups, grouped))
    return jnp.moveaxis(result, 0, 1).reshape(count_fields, N_PTS * NB, PTS_BLOCK)


def column_terms(interp, residual):
    groups = interp.reshape(N_PTS, NB, PTS_BLOCK, COLS)
    grouped = residual.reshape(N_PTS, NB, PTS_BLOCK)

    def one_group(operands):
        return jnp.einsum('bpc,bp->bc', operands[0].astype(jnp.float32), operands[1].astype(jnp.float32), precision=HIGHEST)

    return lax.map(one_group, (groups, grouped)).reshape(N_PTS * NB, COLS)


def reference(grid_weights, direction, kern_x, kern_y, kern_z, interp, block_corner, block_offsets, labels, trial_steps, accept):
    fields = jnp.stack([grid_weights, direction])
    mixed_grid = depth_mix(plane_mix(fields, kern_y, kern_z), kern_x)
    quad_gu = jnp.sum(grid_weights * mixed_grid[0])
    quad_du = jnp.sum(direction * mixed_grid[0])
    quad_dv = jnp.sum(direction * mixed_grid[1])
    cell_ids = cell_ids_of(block_corner, block_offsets)
    flat_grid = mixed_grid.astype(jnp.bfloat16).reshape(2, -1)
    values = jnp.take(flat_grid, cell_ids, axis=1)
    latent_pair = interpolate(interp, values)
    latent = latent_pair[0]
    slope_pt = latent_pair[1]
    target = labels.astype(jnp.float32)
    signed = 2.0 * target - 1.0
    trial_latent = latent[None] + trial_steps[:, None, None] * slope_pt[None]
    loglik = jnp.sum(jax.nn.log_sigmoid(signed[None] * trial_latent), axis=(1, 2))
    descent = jnp.sum((target[None] - jax.nn.sigmoid(trial_latent)) * slope_pt[None], axis=(1, 2))
    prior = 0.5 * (quad_gu + 2.0 * trial_steps * quad_du + trial_steps * trial_steps * quad_dv)
    trial_objective = (loglik - prior) / POINTS
    trial_slope = (descent - quad_du - trial_steps * quad_dv) / POINTS
    chosen = jnp.sum(jnp.where(jnp.arange(NTRIAL) == accept[0], trial_steps, 0.0))
    probability = jax.nn.sigmoid(latent + chosen * slope_pt)
    residual = (target - probability).astype(jnp.bfloat16)
    column_term = column_terms(interp, residual)
    spread = jnp.zeros((GX * GY * GZ,), jnp.float32).at[cell_ids.reshape(-1)].add(column_term.reshape(-1)).reshape(GX, GY, GZ)
    new_weights = grid_weights + chosen * direction
    grid_gradient = spread - new_weights
    bend_grid = depth_mix(plane_mix(grid_gradient[None], kern_y, kern_z), kern_x)
    bend_values = jnp.take(bend_grid.astype(jnp.bfloat16).reshape(1, -1), cell_ids, axis=1)
    bend_pt = interpolate(interp, bend_values)[0]
    curvature = probability * (1.0 - probability) * bend_pt
    return new_weights, grid_gradient, curvature, trial_objective, trial_slope
```

```python
import functools

import jax
import jax.numpy as jnp
from jax import lax
from jax.experimental import pallas as pl
from jax.experimental.pallas import tpu as pltpu
from jax.sharding import PartitionSpec as P

BOXX = 16
BOXY = 16
BOXZ = 8
NTRIAL = 5
PACK = 16
VMEM_BYTES = 62 * 1024 * 1024
UP, DOWN, SIDE, TWIN = range(4)

HIGHEST = lax.Precision.HIGHEST
F32 = jnp.float32
BF16 = jnp.bfloat16
NT = (((1,), (1,)), ((), ()))
MESH = pl.DeviceIdType.MESH


def high_part(value):
    return lax.reduce_precision(value, 8, 7)


def plane_mix(fields_zc, kern_y, kern_z):
    inner = jnp.einsum("zc,fabc->zfab", kern_z, fields_zc, precision=HIGHEST)
    return jnp.einsum("zfab,yb->zfay", inner, kern_y, precision=HIGHEST).astype(BF16)


def widen_kern(kern_x, devices, slab, group):
    size_x = kern_x.shape[0]
    parts = kern_x.reshape(1, size_x, devices, 1, slab)
    same = jnp.eye(group, dtype=F32).reshape(group, 1, 1, group, 1)
    wide = (parts * same).reshape(group * size_x, devices * group * slab)
    high = high_part(wide)
    return high.astype(BF16), (wide - high).astype(BF16)


class Place:
    def __init__(self, devices):
        me = lax.axis_index("pts")
        self.devices = devices
        self.depths = devices // 4
        self.me = me
        self.core = lax.rem(me, 2)
        self.side = lax.rem(lax.div(me, 2), 2)
        self.depth = lax.div(me, 4)

    def slot(self, depth, side, core):
        return (depth * 2 + side) * 2 + core

    def target(self, kind):
        if kind == UP:
            return self.slot(self.depth + 1, self.side, self.core)
        if kind == DOWN:
            return self.slot(self.depth - 1, self.side, self.core)
        if kind == SIDE:
            return self.slot(self.depth, 1 - self.side, self.core)
        return self.slot(self.depth, self.side, 1 - self.core)

    def greet(self):
        barrier = pltpu.get_barrier_semaphore()

        def tell(kind):
            pl.semaphore_signal(
                barrier, inc=1, device_id={"pts": self.target(kind)}, device_id_type=MESH
            )

        tell(SIDE)
        tell(TWIN)

        @pl.when(self.depth + 1 < self.depths)
        def _():
            tell(UP)

        @pl.when(self.depth > 0)
        def _():
            tell(DOWN)

        above = jnp.where(self.depth + 1 < self.depths, 1, 0)
        below = jnp.where(self.depth > 0, 1, 0)
        pl.semaphore_wait(barrier, 2 + above + below)


class Relay:
    def __init__(self, place, own, buf, send, recv):
        self.place = place
        self.own = own
        self.buf = buf
        self.send = send
        self.recv = recv
        self.pieces = recv.shape[1]
        self.size = own.shape[0] // self.pieces

    def copy(self, slot, piece, kind, mine=False):
        rows = pl.ds(piece * self.size, self.size)
        landing = self.buf.at[slot, rows]
        return pltpu.make_async_remote_copy(
            src_ref=self.own.at[rows] if mine else landing,
            dst_ref=landing,
            send_sem=self.send.at[kind, lax.div(slot, 2), piece],
            recv_sem=self.recv.at[slot, piece],
            device_id={"pts": self.place.target(kind)},
            device_id_type=MESH,
        )

    def take(self, slot, piece):
        self.copy(slot, piece, TWIN).wait_recv()

    def line_sends(self, depth, piece, act, mine=False):
        here = self.place
        slot = here.slot(depth, here.side, here.core)

        @pl.when((depth <= here.depth) & (here.depth + 1 < here.depths))
        def _():
            act(self.copy(slot, piece, UP, mine))

        @pl.when((depth >= here.depth) & (here.depth > 0))
        def _():
            act(self.copy(slot, piece, DOWN, mine))

        act(self.copy(slot, piece, SIDE, mine))
        act(self.copy(slot, piece, TWIN, mine))

    def side_sends(self, depth, piece, act):
        here = self.place
        act(self.copy(here.slot(depth, 1 - here.side, here.core), piece, TWIN))

    def start_own(self, piece):
        self.line_sends(self.place.depth, piece, lambda c: c.start(), mine=True)

    def line_events(self, piece, far):
        here = self.place
        for way in (-1, 1):
            depth = here.depth + way * far

            @pl.when((far > 0) & (depth >= 0) & (depth < here.depths))
            def _():
                self.take(here.slot(depth, here.side, here.core), piece)
                self.line_sends(depth, piece, lambda c: c.start())

    def side_events(self, piece, far):
        here = self.place
        for way in (-1, 1):
            depth = here.depth + way * far
            wanted = (depth >= 0) & (depth < here.depths)
            if way > 0:
                wanted = wanted & (far > 0)

            @pl.when(wanted)
            def _():
                self.take(here.slot(depth, 1 - here.side, here.core), piece)
                self.side_sends(depth, piece, lambda c: c.start())

    def twin_events(self, piece):
        here = self.place

        def one(pair, carry):
            self.take(pair * 2 + (1 - here.core), piece)
            return carry

        lax.fori_loop(0, here.devices // 2, one, 0)

    def run(self, work=None, mix=None, tail=None):
        depths = self.place.depths

        def one(piece, carry):
            @pl.when(piece + 1 < self.pieces)
            def _():
                self.start_own(piece + 1)

            def near(far, carry):
                self.line_events(piece, far)

                @pl.when(piece > 0)
                def _():
                    self.side_events(piece - 1, far)

                if work is not None:
                    work(piece * depths + far)
                return carry

            lax.fori_loop(0, depths, near, 0)

            @pl.when(piece > 0)
            def _():
                self.twin_events(piece - 1)
                if mix is not None:
                    mix(piece - 1)

            return carry

        lax.fori_loop(0, self.pieces, one, 0)
        if tail is not None:
            tail()

        def last(far, carry):
            self.side_events(self.pieces - 1, far)
            return carry

        lax.fori_loop(0, depths, last, 0)
        self.twin_events(self.pieces - 1)
        if mix is not None:
            mix(self.pieces - 1)

    def finish(self):
        def one(step, carry):
            piece = lax.div(step, self.place.depths)
            depth = lax.rem(step, self.place.depths)
            self.line_sends(depth, piece, lambda c: c.wait_send())
            self.side_sends(depth, piece, lambda c: c.wait_send())
            return carry

        lax.fori_loop(0, self.pieces * self.place.depths, one, 0)


def relay_sems(devices, pieces):
    return [
        pltpu.SemaphoreType.DMA((4, devices // 2, pieces)),
        pltpu.SemaphoreType.DMA((devices, pieces)),
    ]


def mix_depth(planes_ref, kh_ref, kl_ref, image, group, size_x, first, count):
    devices, _, pack, lanes = planes_ref.shape

    def one(step, carry):
        at = first + step * 2
        pair = [planes_ref[:, at + t].reshape(devices * pack, lanes) for t in range(2)]
        rhs = jnp.concatenate(pair, axis=1)
        mixed = jnp.dot(kh_ref[...], rhs, preferred_element_type=F32)
        mixed = mixed + jnp.dot(kl_ref[...], rhs, preferred_element_type=F32)
        for t in range(2):
            for g in range(group):
                image[(at + t) * group + g] = mixed[
                    g * size_x : (g + 1) * size_x, t * lanes : (t + 1) * lanes
                ]
        return carry

    lax.fori_loop(0, count // 2, one, 0)


def pick_values(image, corner_ref, y_ref, row_ref, block):
    size_y = image.shape[-1]
    cols = y_ref.shape[-1]
    box_rows = BOXZ * BOXX
    at_z = corner_ref[2, block]
    at_x = corner_ref[0, block]
    box = image[pl.ds(at_z, BOXZ), pl.ds(at_x, BOXX), :]
    box = box.reshape(box_rows, size_y).astype(BF16)
    y_line = lax.broadcasted_iota(jnp.int32, (size_y, cols), 0)
    pick_y = jnp.where(y_line == y_ref[pl.ds(block, 1), :], 1.0, 0.0).astype(BF16)
    lines = jnp.dot(box, pick_y, preferred_element_type=F32)
    row_line = lax.broadcasted_iota(jnp.int32, (box_rows, cols), 0)
    line = jnp.where(row_line == row_ref[pl.ds(block, 1), :], lines, 0.0)
    value = jnp.sum(line, axis=0, keepdims=True)
    return jnp.broadcast_to(value, (8, cols)).astype(BF16)


def interpolate_blocks(image, corner_ref, y_ref, row_ref, interp, out_ref, first, count):
    unroll = min(8, count)

    def some(part, carry):
        for k in range(unroll):
            block = first + part * unroll + k
            values = pick_values(image, corner_ref, y_ref, row_ref, block)
            line = lax.dot_general(values, interp[block], NT, preferred_element_type=F32)
            out_ref[pl.ds(block, 1), :] = line[0:1]
        return carry

    lax.fori_loop(0, count // unroll, some, 0)


def log_sigmoid(value):
    return jnp.minimum(value, 0.0) - jnp.log1p(jnp.exp(-jnp.abs(value)))


def forward_kernel(
    group,
    corner_ref,
    chosen_ref,
    trial_ref,
    own_u,
    own_d,
    offs_ref,
    kh_ref,
    kl_ref,
    y_ref,
    row_ref,
    labels_ref,
    weights_ref,
    direction_ref,
    interp_ref,
    prob_ref,
    sums_ref,
    all_offs,
    all_terms,
    buf_u,
    buf_d,
    image_u,
    image_d,
    interp,
    latent_ref,
    slope_ref,
    res_ref,
    term_ref,
    own_terms,
    local_sem,
    *sems,
):
    devices, units, pack, lanes = buf_u.shape
    blocks, per_block = labels_ref.shape
    slab = pack // group
    size_x = image_u.shape[1]
    place = Place(devices)
    load = pltpu.make_async_copy(interp_ref, interp, local_sem)
    load.start()
    u = Relay(place, own_u, buf_u, sems[0], sems[1])
    d = Relay(place, own_d, buf_d, sems[2], sems[3])
    o = Relay(place, offs_ref, all_offs, sems[4], sems[5])
    t = Relay(place, own_terms, all_terms, sems[6], sems[7])
    place.greet()
    u.start_own(0)
    buf_u[place.me] = own_u[...]
    buf_d[place.me] = own_d[...]
    all_offs[place.me] = offs_ref[...]

    def mixer(buf, image):
        return lambda piece: mix_depth(
            buf, kh_ref, kl_ref, image, group, size_x, piece * u.size, u.size
        )

    u.run(mix=mixer(buf_u, image_u), tail=lambda: d.start_own(0))
    load.wait()
    steps = u.pieces * place.depths
    some = blocks // steps

    def early(step):
        interpolate_blocks(
            image_u, corner_ref, y_ref, row_ref, interp, latent_ref, step * some, some
        )

    d.run(work=early, mix=mixer(buf_d, image_d), tail=lambda: o.start_own(0))
    part = blocks // place.depths

    def late(step):
        interpolate_blocks(
            image_d, corner_ref, y_ref, row_ref, interp, slope_ref, step * part, part
        )

    o.run(work=late)
    slope = slope_ref[...]
    latent = latent_ref[...]
    prob = jax.nn.sigmoid(latent + chosen_ref[0] * slope)
    prob_ref[...] = prob
    target = labels_ref[...].astype(F32)
    res_ref[...] = (target - prob).astype(BF16).astype(F32)
    unroll = 8

    def back(step, carry):
        for k in range(unroll):
            block = step * unroll + k
            row = jnp.broadcast_to(res_ref[pl.ds(block, 1), :], (8, per_block))
            term = jnp.dot(row.astype(BF16), interp[block], preferred_element_type=F32)
            term_ref[pl.ds(block, 1), :] = term[0:1]
        return carry

    lax.fori_loop(0, blocks // unroll, back, 0)
    own_terms[...] = term_ref[...].astype(BF16)
    all_terms[place.me] = own_terms[...]
    u.finish()
    d.finish()
    o.finish()
    at = pl.multiple_of(place.me * slab, slab)
    image_w = image_u[:, pl.ds(at, slab), :]
    image_t = image_d[:, pl.ds(at, slab), :]
    sums = [
        jnp.sum(weights_ref[...] * image_w),
        jnp.sum(direction_ref[...] * image_w),
        jnp.sum(direction_ref[...] * image_t),
    ]
    t.start_own(0)
    signed = 2.0 * target - 1.0
    loglik, descent = [], []
    for k in range(NTRIAL):
        at_trial = latent + trial_ref[k] * slope
        loglik.append(jnp.sum(log_sigmoid(signed * at_trial)))
        descent.append(jnp.sum((target - jax.nn.sigmoid(at_trial)) * slope))
    lane = lax.broadcasted_iota(jnp.int32, sums_ref.shape, 1)
    row = jnp.zeros(sums_ref.shape, F32)
    for k, value in enumerate(loglik + descent + sums):
        row = jnp.where(lane == k, value, row)
    sums_ref[...] = row
    t.run()
    t.finish()


def bend_kernel(
    group,
    corner_ref,
    own_ref,
    split_ref,
    kh_ref,
    kl_ref,
    y_ref,
    row_ref,
    prob_ref,
    interp_ref,
    out_ref,
    total_ref,
    buf,
    all_split,
    image,
    interp,
    local_sem,
    *sems,
):
    devices = buf.shape[0]
    blocks = prob_ref.shape[0]
    size_x = image.shape[1]
    place = Place(devices)
    load = pltpu.make_async_copy(interp_ref, interp, local_sem)
    load.start()
    b = Relay(place, own_ref, buf, sems[0], sems[1])
    s = Relay(place, split_ref, all_split, sems[2], sems[3])
    place.greet()
    b.start_own(0)
    buf[place.me] = own_ref[...]
    all_split[place.me] = split_ref[...]
    b.run(
        mix=lambda piece: mix_depth(
            buf, kh_ref, kl_ref, image, group, size_x, piece * b.size, b.size
        ),
        tail=lambda: s.start_own(0),
    )
    load.wait()
    part = blocks // place.depths

    def late(step):
        interpolate_blocks(
            image, corner_ref, y_ref, row_ref, interp, out_ref, step * part, part
        )

    s.run(work=late)
    total_ref[...] = jnp.sum(all_split[...].astype(F32), axis=0)
    prob = prob_ref[...]
    out_ref[...] = prob * (1.0 - prob) * out_ref[...]
    b.finish()
    s.finish()


def scatter_kernel(slab, unroll, ids_ref, count_ref, z_ref, y_ref, key_ref, term_ref, out_ref):
    cols = y_ref.shape[-1]
    size_y = out_ref.shape[-1]
    rows = BOXZ * slab
    out_ref[...] = jnp.zeros_like(out_ref)

    def some(part, carry):
        sums = []
        for k in range(unroll):
            block = ids_ref[part * unroll + k]
            row_line = lax.broadcasted_iota(jnp.int32, (rows, cols), 0)
            y_line = lax.broadcasted_iota(jnp.int32, (size_y, cols), 0)
            wanted = row_line == key_ref[pl.ds(block, 1), :]
            left = jnp.where(wanted, term_ref[pl.ds(block, 1), :], 0.0).astype(BF16)
            right = jnp.where(y_line == y_ref[pl.ds(block, 1), :], 1.0, 0.0).astype(BF16)
            sums.append((block, lax.dot_general(left, right, NT, preferred_element_type=F32)))
        for block, piece in sums:
            at = pl.multiple_of(z_ref[block] * slab, slab)
            out_ref[pl.ds(at, rows), :] += piece
        return carry

    lax.fori_loop(0, lax.div(count_ref[0] + unroll - 1, unroll), some, 0)


def whole(shape):
    return pl.BlockSpec(
        shape, lambda i, *_: (0,) * len(shape), pipeline_mode=pl.Buffered(buffer_count=1)
    )


def body(
    grid_weights,
    direction,
    kern_x,
    kern_y,
    kern_z,
    interp,
    block_corner,
    block_offsets,
    labels,
    trial_steps,
    accept,
):
    slab, size_y, size_z = grid_weights.shape
    size_x = kern_x.shape[0]
    devices = lax.axis_size("pts")
    me = lax.axis_index("pts")
    blocks, cols = block_offsets.shape
    per_block = interp.shape[1]
    points = blocks * per_block * devices
    group = max(1, PACK // slab)
    pack = group * slab
    unroll = 8
    units = size_z // group
    pieces = max(1, 64 // devices)

    spare = jnp.pad(block_corner, ((0, PACK - 3), (0, cols - blocks)))
    sent = jnp.concatenate([block_offsets, spare], axis=0).astype(jnp.int16)
    planes_w, planes_d = (
        plane_mix(field[None], kern_y, kern_z).reshape(units, pack, size_y)
        for field in (grid_weights, direction)
    )
    kern_high, kern_low = widen_kern(kern_x, devices, slab, group)
    y_cell = block_corner[1][:, None] + block_offsets // BOXZ % BOXY
    box_row = block_offsets % BOXZ * BOXX + block_offsets // (BOXY * BOXZ)
    chosen = jnp.sum(jnp.where(jnp.arange(NTRIAL) == accept[0], trial_steps, 0.0))
    weights_t = jnp.transpose(grid_weights, (2, 0, 1))
    direction_t = jnp.transpose(direction, (2, 0, 1))

    smem = pl.BlockSpec(memory_space=pltpu.SMEM)
    vmem = pl.BlockSpec(memory_space=pltpu.VMEM)
    hbm = pl.BlockSpec(memory_space=pl.ANY)
    planes_scratch = pltpu.VMEM((devices, units, pack, size_y), BF16)
    image_scratch = pltpu.VMEM((size_z, size_x, size_y), F32)
    interp_scratch = pltpu.VMEM(interp.shape, BF16)
    point_scratch = pltpu.VMEM((blocks, per_block), F32)
    point_shape = jax.ShapeDtypeStruct((blocks, per_block), F32)

    probability, sums, everyone, terms = pl.pallas_call(
        functools.partial(forward_kernel, group),
        in_specs=[smem] * 3 + [vmem] * 10 + [hbm],
        out_specs=[vmem] * 4,
        out_shape=[
            point_shape,
            jax.ShapeDtypeStruct((8, 128), F32),
            jax.ShapeDtypeStruct((devices,) + sent.shape, jnp.int16),
            jax.ShapeDtypeStruct((devices, blocks, cols), BF16),
        ],
        scratch_shapes=[
            planes_scratch,
            planes_scratch,
            image_scratch,
            image_scratch,
            interp_scratch,
            point_scratch,
            point_scratch,
            point_scratch,
            pltpu.VMEM((blocks, cols), F32),
            pltpu.VMEM((blocks, cols), BF16),
            pltpu.SemaphoreType.DMA,
            *relay_sems(devices, pieces),
            *relay_sems(devices, pieces),
            *relay_sems(devices, 1),
            *relay_sems(devices, 1),
        ],
        compiler_params=pltpu.CompilerParams(
            vmem_limit_bytes=VMEM_BYTES, collective_id=0, has_side_effects=True
        ),
        name="forward",
    )(
        block_corner,
        chosen.reshape(1),
        trial_steps,
        planes_w,
        planes_d,
        sent,
        kern_high,
        kern_low,
        y_cell,
        box_row,
        labels,
        weights_t,
        direction_t,
        interp,
    )
    terms = terms.reshape(devices * blocks, cols).astype(F32)

    far_offsets = everyone[:, :blocks].astype(jnp.int32).reshape(devices * blocks, cols)
    far = everyone[:, blocks : blocks + 3, :blocks].astype(jnp.int32)
    far_x, far_y, far_z = (far[:, k].reshape(-1) for k in range(3))
    x_from = far_x - me * slab
    far_cell = x_from[:, None] + far_offsets // (BOXY * BOXZ)
    inside = (far_cell >= 0) & (far_cell < slab)
    key = jnp.where(inside, far_offsets % BOXZ * slab + far_cell, -1)
    far_line = far_y[:, None] + far_offsets // BOXZ % BOXY
    total = devices * blocks
    touches = (x_from < slab) & (x_from > -BOXX)
    ranks = jnp.arange(total, dtype=jnp.int32)
    ids = lax.sort(jnp.where(touches, ranks, ranks + total))
    ids = jnp.where(ids >= total, ids - total, ids)
    touched = jnp.sum(touches.astype(jnp.int32)).reshape(1)

    spread = pl.pallas_call(
        functools.partial(scatter_kernel, slab, unroll),
        grid_spec=pltpu.PrefetchScalarGridSpec(
            num_scalar_prefetch=3,
            grid=(1,),
            in_specs=[whole((total, cols))] * 3,
            out_specs=pl.BlockSpec((size_z * slab, size_y), lambda i, *_: (0, 0)),
        ),
        out_shape=jax.ShapeDtypeStruct((size_z * slab, size_y), F32),
        compiler_params=pltpu.CompilerParams(vmem_limit_bytes=VMEM_BYTES),
        name="spread",
    )(ids, touched, far_z, far_line, key, terms)

    new_weights = grid_weights + chosen * direction
    grid_gradient = (
        jnp.transpose(spread.reshape(size_z, slab, size_y), (1, 2, 0)) - new_weights
    )

    sums = sums[0]
    first = high_part(sums)
    second = high_part(sums - first)
    third = sums - first - second
    split = jnp.stack([first, second, third]).astype(BF16)
    split = jnp.pad(split, ((0, PACK - 3), (0, 0)))

    bend_planes = plane_mix(grid_gradient[None], kern_y, kern_z)
    bend_planes = bend_planes.reshape(units, pack, size_y)
    curvature, totals = pl.pallas_call(
        functools.partial(bend_kernel, group),
        in_specs=[smem] + [vmem] * 7 + [hbm],
        out_specs=[vmem] * 2,
        out_shape=[point_shape, jax.ShapeDtypeStruct((PACK, 128), F32)],
        scratch_shapes=[
            planes_scratch,
            pltpu.VMEM((devices, PACK, 128), BF16),
            image_scratch,
            interp_scratch,
            pltpu.SemaphoreType.DMA,
            *relay_sems(devices, pieces),
            *relay_sems(devices, 1),
        ],
        compiler_params=pltpu.CompilerParams(
            vmem_limit_bytes=VMEM_BYTES, collective_id=1, has_side_effects=True
        ),
        name="bend",
    )(
        block_corner,
        bend_planes,
        split,
        kern_high,
        kern_low,
        y_cell,
        box_row,
        probability,
        interp,
    )

    everything = totals[0] + totals[1] + totals[2]
    loglik = everything[:NTRIAL]
    descent = everything[NTRIAL : 2 * NTRIAL]
    quad_gu, quad_du, quad_dv = (everything[2 * NTRIAL + k] for k in range(3))
    prior = 0.5 * (quad_gu + 2.0 * trial_steps * quad_du + trial_steps * trial_steps * quad_dv)
    trial_objective = (loglik - prior) / points
    trial_slope = (descent - quad_du - trial_steps * quad_dv) / points
    return (new_weights, grid_gradient, curvature, trial_objective, trial_slope)


def solution(mesh):
    return jax.shard_map(
        body,
        mesh=mesh,
        in_specs=(
            P(("parts", "pts"), None, None),
            P(("parts", "pts"), None, None),
            P(),
            P(),
            P(),
            P(("parts", "pts"), None, None),
            P(None, ("parts", "pts")),
            P(("parts", "pts"), None),
            P(("parts", "pts"), None),
            P(),
            P(),
        ),
        out_specs=(
            P(("parts", "pts"), None, None),
            P(("parts", "pts"), None, None),
            P(("parts", "pts"), None),
            P("parts"),
            P("parts"),
        ),
        check_vma=False,
    )
```

```python
import functools

import jax
import jax.numpy as jnp
from jax import lax
from jax.experimental import pallas as pl
from jax.experimental.pallas import tpu as pltpu
from jax.sharding import PartitionSpec as P

BOXX = 16
BOXY = 16
BOXZ = 8
NTRIAL = 5
PACK = 16
VMEM_BYTES = 62 * 1024 * 1024
UP, DOWN, SIDE, TWIN = range(4)

HIGHEST = lax.Precision.HIGHEST
F32 = jnp.float32
BF16 = jnp.bfloat16
NT = (((1,), (1,)), ((), ()))
MESH = pl.DeviceIdType.MESH


def high_part(value):
    return lax.reduce_precision(value, 8, 7)


def widen_kern(kern_x, devices, slab, group):
    size_x = kern_x.shape[0]
    parts = kern_x.reshape(1, size_x, devices, 1, slab)
    same = jnp.eye(group, dtype=F32).reshape(group, 1, 1, group, 1)
    wide = (parts * same).reshape(group * size_x, devices * group * slab)
    high = high_part(wide)
    return high.astype(BF16), (wide - high).astype(BF16)


class Place:
    def __init__(self, devices):
        me = lax.axis_index("pts")
        self.devices = devices
        self.depths = devices // 4
        self.me = me
        self.core = lax.rem(me, 2)
        self.side = lax.rem(lax.div(me, 2), 2)
        self.depth = lax.div(me, 4)

    def slot(self, depth, side, core):
        return (depth * 2 + side) * 2 + core

    def target(self, kind):
        if kind == UP:
            return self.slot(self.depth + 1, self.side, self.core)
        if kind == DOWN:
            return self.slot(self.depth - 1, self.side, self.core)
        if kind == SIDE:
            return self.slot(self.depth, 1 - self.side, self.core)
        return self.slot(self.depth, self.side, 1 - self.core)

    def greet(self):
        barrier = pltpu.get_barrier_semaphore()

        def tell(kind):
            pl.semaphore_signal(
                barrier, inc=1, device_id={"pts": self.target(kind)}, device_id_type=MESH
            )

        tell(SIDE)
        tell(TWIN)

        @pl.when(self.depth + 1 < self.depths)
        def _():
            tell(UP)

        @pl.when(self.depth > 0)
        def _():
            tell(DOWN)

        above = jnp.where(self.depth + 1 < self.depths, 1, 0)
        below = jnp.where(self.depth > 0, 1, 0)
        pl.semaphore_wait(barrier, 2 + above + below)


class Relay:
    def __init__(self, place, own, buf, send, recv):
        self.place = place
        self.own = own
        self.buf = buf
        self.send = send
        self.recv = recv
        self.pieces = recv.shape[1]
        self.size = own.shape[0] // self.pieces

    def copy(self, slot, piece, kind, mine=False):
        rows = pl.ds(piece * self.size, self.size)
        landing = self.buf.at[slot, rows]
        return pltpu.make_async_remote_copy(
            src_ref=self.own.at[rows] if mine else landing,
            dst_ref=landing,
            send_sem=self.send.at[kind, lax.div(slot, 2), piece],
            recv_sem=self.recv.at[slot, piece],
            device_id={"pts": self.place.target(kind)},
            device_id_type=MESH,
        )

    def take(self, slot, piece):
        self.copy(slot, piece, TWIN).wait_recv()

    def line_sends(self, depth, piece, act, mine=False):
        here = self.place
        slot = here.slot(depth, here.side, here.core)

        @pl.when((depth <= here.depth) & (here.depth + 1 < here.depths))
        def _():
            act(self.copy(slot, piece, UP, mine))

        @pl.when((depth >= here.depth) & (here.depth > 0))
        def _():
            act(self.copy(slot, piece, DOWN, mine))

        act(self.copy(slot, piece, SIDE, mine))
        act(self.copy(slot, piece, TWIN, mine))

    def side_sends(self, depth, piece, act):
        here = self.place
        act(self.copy(here.slot(depth, 1 - here.side, here.core), piece, TWIN))

    def start_own(self):
        def one(piece, carry):
            self.line_sends(self.place.depth, piece, lambda c: c.start(), mine=True)
            return carry

        lax.fori_loop(0, self.pieces, one, 0)

    def line_events(self, piece, far):
        here = self.place
        for way in (-1, 1):
            depth = here.depth + way * far

            @pl.when((far > 0) & (depth >= 0) & (depth < here.depths))
            def _():
                self.take(here.slot(depth, here.side, here.core), piece)
                self.line_sends(depth, piece, lambda c: c.start())

    def side_events(self, piece, far):
        here = self.place
        for way in (-1, 1):
            depth = here.depth + way * far
            wanted = (depth >= 0) & (depth < here.depths)
            if way > 0:
                wanted = wanted & (far > 0)

            @pl.when(wanted)
            def _():
                self.take(here.slot(depth, 1 - here.side, here.core), piece)
                self.side_sends(depth, piece, lambda c: c.start())

    def twin_events(self, piece):
        here = self.place

        def one(pair, carry):
            self.take(pair * 2 + (1 - here.core), piece)
            return carry

        lax.fori_loop(0, here.devices // 2, one, 0)

    def run(self, work=None, steps=0, mix=None, tail=None, riders=()):
        depths, pieces = self.place.depths, self.pieces

        def one(wave, carry):
            def near(far, carry):
                piece = wave - far

                @pl.when((piece >= 0) & (piece < pieces))
                def _():
                    self.line_events(piece, far)

                @pl.when((piece >= 1) & (piece < pieces + 1))
                def _():
                    self.side_events(piece - 1, far)

                for rider in riders:

                    @pl.when(piece == 0)
                    def _():
                        rider.line_events(0, far)

                    @pl.when(piece == 1)
                    def _():
                        rider.side_events(0, far)

                return carry

            lax.fori_loop(0, depths, near, 0)
            if tail is not None:

                @pl.when(wave == pieces + depths - 2)
                def _():
                    tail()

            if work is not None:

                @pl.when(wave < steps)
                def _():
                    work(wave)

            full = wave - depths - 1

            @pl.when(full >= 0)
            def _():
                self.twin_events(full)
                if mix is not None:
                    mix(full)

            for rider in riders:

                @pl.when(full == 0)
                def _():
                    rider.twin_events(0)

            return carry

        lax.fori_loop(0, pieces + depths + 1, one, 0)

    def finish(self):
        def one(step, carry):
            piece = lax.div(step, self.place.depths)
            depth = lax.rem(step, self.place.depths)
            self.line_sends(depth, piece, lambda c: c.wait_send())
            self.side_sends(depth, piece, lambda c: c.wait_send())
            return carry

        lax.fori_loop(0, self.pieces * self.place.depths, one, 0)


def relay_sems(devices, pieces):
    return [
        pltpu.SemaphoreType.DMA((4, devices // 2, pieces)),
        pltpu.SemaphoreType.DMA((devices, pieces)),
    ]


def mix_depth(planes_ref, kh_ref, kl_ref, image, group, size_x, first, count):
    devices, _, pack, lanes = planes_ref.shape

    def one(step, carry):
        at = first + step * 2
        pair = [planes_ref[:, at + t].reshape(devices * pack, lanes) for t in range(2)]
        rhs = jnp.concatenate(pair, axis=1)
        mixed = jnp.dot(kh_ref[...], rhs, preferred_element_type=F32)
        mixed = mixed + jnp.dot(kl_ref[...], rhs, preferred_element_type=F32)
        for t in range(2):
            for g in range(group):
                image[(at + t) * group + g] = mixed[
                    g * size_x : (g + 1) * size_x, t * lanes : (t + 1) * lanes
                ]
        return carry

    lax.fori_loop(0, count // 2, one, 0)


def split_offset(offset):
    bits_y, bits_z = BOXY.bit_length() - 1, BOXZ.bit_length() - 1
    return offset >> (bits_y + bits_z), (offset >> bits_z) & (BOXY - 1), offset & (BOXZ - 1)


def pick_values(image, corner_ref, offsets_ref, block):
    size_y = image.shape[-1]
    cols = offsets_ref.shape[-1]
    box_rows = BOXZ * BOXX
    at_x, at_y, at_z = (corner_ref[k, block] for k in range(3))
    off_x, off_y, off_z = split_offset(offsets_ref[pl.ds(block, 1), :])
    y_cell = at_y + off_y
    box_row = off_z * BOXX + off_x
    box = image[pl.ds(at_z, BOXZ), pl.ds(at_x, BOXX), :]
    box = box.reshape(box_rows, size_y).astype(BF16)
    y_line = lax.broadcasted_iota(jnp.int32, (size_y, cols), 0)
    pick_y = jnp.where(y_line == y_cell, 1.0, 0.0).astype(BF16)
    lines = jnp.dot(box, pick_y, preferred_element_type=F32)
    row_line = lax.broadcasted_iota(jnp.int32, (box_rows, cols), 0)
    line = jnp.where(row_line == box_row, lines, 0.0)
    value = jnp.sum(line, axis=0, keepdims=True)
    return jnp.broadcast_to(value, (8, cols)).astype(BF16)


def interpolate_blocks(image, corner_ref, offsets_ref, interp, out_ref, first, count):
    unroll = min(16, count)

    def some(part, carry):
        for k in range(unroll):
            block = first + part * unroll + k
            values = pick_values(image, corner_ref, offsets_ref, block)
            line = lax.dot_general(values, interp[block], NT, preferred_element_type=F32)
            out_ref[pl.ds(block, 1), :] = line[0:1]
        return carry

    lax.fori_loop(0, count // unroll, some, 0)


def power_below(value):
    return 1 << (value.bit_length() - 1)


def mix_planes(field_of, kern_y_ref, kern_z_ref, rows, planes_ref, slab):
    size_z = kern_z_ref.shape[0]
    for x in range(slab):
        inner = lax.dot_general(
            kern_z_ref[...], field_of(x), NT, precision=HIGHEST, preferred_element_type=F32
        )
        plane = lax.dot_general(
            inner, kern_y_ref[...], NT, precision=HIGHEST, preferred_element_type=F32
        )
        rows[pl.ds(x, size_z, stride=slab), :] = plane
    planes_ref[...] = rows[...].astype(BF16).reshape(planes_ref.shape)


def planes_kernel(weights_ref, direction_ref, kern_y_ref, kern_z_ref, out_u, out_d, rows):
    slab = weights_ref.shape[0]
    mix_planes(lambda x: weights_ref[x], kern_y_ref, kern_z_ref, rows, out_u, slab)
    mix_planes(lambda x: direction_ref[x], kern_y_ref, kern_z_ref, rows, out_d, slab)


def rank_blocks(corners, me, slab, ranks_ref, list_ref):
    devices, blocks = corners.shape
    from_x = (corners & 255) - me * slab
    touch = jnp.where((from_x < slab) & (from_x > -BOXX), 1.0, 0.0)
    earlier = lax.broadcasted_iota(jnp.int32, (blocks, blocks), 0)
    earlier = earlier < lax.broadcasted_iota(jnp.int32, (blocks, blocks), 1)
    within = jnp.dot(
        touch.astype(BF16), jnp.where(earlier, 1.0, 0.0).astype(BF16), preferred_element_type=F32
    )
    count = jnp.sum(touch, axis=1, keepdims=True)
    below = lax.broadcasted_iota(jnp.int32, (devices, devices), 1)
    below = below < lax.broadcasted_iota(jnp.int32, (devices, devices), 0)
    base = jnp.dot(
        jnp.where(below, 1.0, 0.0).astype(BF16),
        jnp.broadcast_to(count, (devices, blocks)).astype(BF16),
        preferred_element_type=F32,
    )
    ranks = jnp.where(touch > 0.0, base + within, -1.0)
    for device in range(devices):
        line = jnp.broadcast_to(ranks[device : device + 1], (blocks, blocks))
        ranks_ref[device] = jnp.transpose(line)
    total = jnp.sum(touch)
    list_ref[pl.ds(devices, 8), :] = jnp.full((8, blocks), total, F32).astype(jnp.int32)


def list_blocks(ranks_ref, list_ref, line):
    devices, blocks, _ = ranks_ref.shape
    wanted = lax.broadcasted_iota(jnp.int32, (blocks, blocks), 1) + line * blocks
    wanted = wanted.astype(F32)
    block = lax.broadcasted_iota(jnp.int32, (blocks, blocks), 0).astype(F32)

    def one(device, ids):
        hit = ranks_ref[device] == wanted
        start = (device * blocks).astype(F32)
        return ids + jnp.where(hit, block + start, 0.0)

    ids = lax.fori_loop(0, devices, one, jnp.zeros((blocks, blocks), F32))
    ids = jnp.sum(ids, axis=0, keepdims=True)
    list_ref[pl.ds(line, 1), :] = ids.astype(jnp.int32)


def log_sigmoid(value):
    return jnp.minimum(value, 0.0) - jnp.log1p(jnp.exp(-jnp.abs(value)))


def forward_kernel(
    group,
    corner_ref,
    trial_ref,
    accept_ref,
    own_u,
    own_d,
    packed_ref,
    kh_ref,
    kl_ref,
    offsets_ref,
    labels_ref,
    weights_ref,
    direction_ref,
    interp_ref,
    prob_ref,
    split_ref,
    list_ref,
    corners_ref,
    all_offs,
    all_terms,
    buf_u,
    buf_d,
    all_packed,
    image_u,
    image_d,
    interp,
    latent_ref,
    slope_ref,
    res_ref,
    term_ref,
    own_terms,
    own_offs,
    weights_t,
    direction_t,
    ranks_ref,
    local_sem,
    *sems,
):
    devices, units, pack, lanes = buf_u.shape
    blocks, per_block = labels_ref.shape
    slab = pack // group
    size_z, size_x, size_y = image_u.shape
    place = Place(devices)
    load = pltpu.make_async_copy(interp_ref, interp, local_sem)
    load.start()
    u = Relay(place, own_u, buf_u, sems[0], sems[1])
    d = Relay(place, own_d, buf_d, sems[2], sems[3])
    o = Relay(place, own_offs, all_offs, sems[4], sems[5])
    t = Relay(place, own_terms, all_terms, sems[6], sems[7])
    c = Relay(place, packed_ref, all_packed, sems[8], sems[9])
    place.greet()
    c.start_own()
    u.start_own()
    buf_u[place.me] = own_u[...]
    buf_d[place.me] = own_d[...]
    all_packed[place.me] = packed_ref[...]
    own_offs[...] = offsets_ref[...].astype(jnp.int16)
    all_offs[place.me] = own_offs[...]
    for x in range(slab):
        weights_t[pl.ds(x, size_z, stride=slab), :] = jnp.transpose(weights_ref[x])
        direction_t[pl.ds(x, size_z, stride=slab), :] = jnp.transpose(direction_ref[x])

    def mixer(buf, image):
        return lambda piece: mix_depth(
            buf, kh_ref, kl_ref, image, group, size_x, piece * u.size, u.size
        )

    u.run(mix=mixer(buf_u, image_u), tail=d.start_own, riders=(c,))
    corners = all_packed[:, 0, :]
    corners_ref[...] = corners
    rank_blocks(corners, place.me, slab, ranks_ref, list_ref)
    load.wait()
    steps = power_below(u.pieces + place.depths)
    some, lines = blocks // steps, -(-devices // steps)

    def early(step):
        interpolate_blocks(
            image_u, corner_ref, offsets_ref, interp, latent_ref, step * some, some
        )
        for k in range(lines):
            list_blocks(ranks_ref, list_ref, step * lines + k)

    d.run(work=early, steps=steps, mix=mixer(buf_d, image_d), tail=o.start_own)
    steps = power_below(place.depths)
    part = blocks // steps

    def late(step):
        interpolate_blocks(
            image_d, corner_ref, offsets_ref, interp, slope_ref, step * part, part
        )

    o.run(work=late, steps=steps)
    slope = slope_ref[...]
    latent = latent_ref[...]
    prob = jax.nn.sigmoid(latent + trial_ref[accept_ref[0]] * slope)
    prob_ref[...] = prob
    target = labels_ref[...].astype(F32)
    res_ref[...] = (target - prob).astype(BF16).astype(F32)
    unroll = 16

    def back(step, carry):
        for k in range(unroll):
            block = step * unroll + k
            row = jnp.broadcast_to(res_ref[pl.ds(block, 1), :], (8, per_block))
            term = jnp.dot(row.astype(BF16), interp[block], preferred_element_type=F32)
            term_ref[pl.ds(block, 1), :] = term[0:1]
        return carry

    lax.fori_loop(0, blocks // unroll, back, 0)
    own_terms[...] = term_ref[...].astype(BF16)
    all_terms[place.me] = own_terms[...]
    for relay in (c, u, d, o):
        relay.finish()
    at = pl.multiple_of(place.me * slab, slab)
    image_w = image_u[:, pl.ds(at, slab), :]
    image_t = image_d[:, pl.ds(at, slab), :]
    weights_rows = weights_t[...].reshape(size_z, slab, size_y)
    direction_rows = direction_t[...].reshape(size_z, slab, size_y)
    sums = [
        jnp.sum(weights_rows * image_w),
        jnp.sum(direction_rows * image_w),
        jnp.sum(direction_rows * image_t),
    ]
    t.start_own()
    signed = 2.0 * target - 1.0
    loglik, descent = [], []
    for k in range(NTRIAL):
        at_trial = latent + trial_ref[k] * slope
        loglik.append(jnp.sum(log_sigmoid(signed * at_trial)))
        descent.append(jnp.sum((target - jax.nn.sigmoid(at_trial)) * slope))
    lane = lax.broadcasted_iota(jnp.int32, split_ref.shape, 1)
    row = jnp.zeros(split_ref.shape, F32)
    for k, value in enumerate(loglik + descent + sums):
        row = jnp.where(lane == k, value, row)
    first = row.astype(BF16).astype(F32)
    second = (row - first).astype(BF16).astype(F32)
    third = row - first - second
    line = lax.broadcasted_iota(jnp.int32, split_ref.shape, 0)
    split = jnp.where(line == 0, first, jnp.where(line == 1, second, third))
    split_ref[...] = jnp.where(line < 3, split, 0.0).astype(BF16)
    t.run()
    t.finish()


def bend_kernel(
    group,
    corner_ref,
    own_ref,
    split_ref,
    kh_ref,
    kl_ref,
    offsets_ref,
    prob_ref,
    interp_ref,
    out_ref,
    total_ref,
    buf,
    all_split,
    image,
    interp,
    local_sem,
    *sems,
):
    devices = buf.shape[0]
    blocks = prob_ref.shape[0]
    size_x = image.shape[1]
    place = Place(devices)
    load = pltpu.make_async_copy(interp_ref, interp, local_sem)
    load.start()
    b = Relay(place, own_ref, buf, sems[0], sems[1])
    s = Relay(place, split_ref, all_split, sems[2], sems[3])
    place.greet()
    s.start_own()
    b.start_own()
    buf[place.me] = own_ref[...]
    all_split[place.me] = split_ref[...]
    b.run(
        mix=lambda piece: mix_depth(
            buf, kh_ref, kl_ref, image, group, size_x, piece * b.size, b.size
        ),
        riders=(s,),
    )
    load.wait()
    total = jnp.sum(all_split[...].astype(F32), axis=0)
    total_ref[...] = total[0:1] + total[1:2] + total[2:3]
    interpolate_blocks(image, corner_ref, offsets_ref, interp, out_ref, 0, blocks)
    prob = prob_ref[...]
    out_ref[...] = prob * (1.0 - prob) * out_ref[...]
    b.finish()
    s.finish()


def spread_kernel(
    list_ref,
    corners_ref,
    trial_ref,
    accept_ref,
    offs_ref,
    terms_ref,
    weights_ref,
    direction_ref,
    kern_y_ref,
    kern_z_ref,
    new_ref,
    grad_ref,
    planes_ref,
    offs,
    terms,
    spread,
):
    devices, blocks, cols = offs_ref.shape
    slab, size_y, size_z = weights_ref.shape
    rows = BOXZ * slab
    unroll = 8
    me = lax.axis_index("pts")
    spread[...] = jnp.zeros_like(spread)

    def widen(device, carry):
        offs[pl.ds(pl.multiple_of(device * blocks, blocks), blocks)] = offs_ref[device].astype(
            jnp.int32
        )
        terms[pl.ds(pl.multiple_of(device * blocks, blocks), blocks)] = terms_ref[device].astype(
            F32
        )
        return carry

    lax.fori_loop(0, devices, widen, 0)
    count = list_ref[devices, 0]

    def some(part, carry):
        sums = []
        for k in range(unroll):
            at = part * unroll + k
            block = list_ref[lax.div(at, blocks), lax.rem(at, blocks)]
            packed = corners_ref[lax.div(block, blocks), lax.rem(block, blocks)]
            from_x = jnp.where(at < count, (packed & 255) - me * slab, -2 * BOXX)
            at_y = (packed >> 8) & 255
            at_z = packed >> 16
            off_x, off_y, off_z = split_offset(offs[pl.ds(block, 1), :])
            cell = off_x + from_x
            key = jnp.where((cell >= 0) & (cell < slab), off_z * slab + cell, -1)
            y_cell = off_y + at_y
            row_line = lax.broadcasted_iota(jnp.int32, (rows, cols), 0)
            y_line = lax.broadcasted_iota(jnp.int32, (size_y, cols), 0)
            left = jnp.where(row_line == key, terms[pl.ds(block, 1), :], 0.0).astype(BF16)
            right = jnp.where(y_line == y_cell, 1.0, 0.0).astype(BF16)
            sums.append((at_z, lax.dot_general(left, right, NT, preferred_element_type=F32)))
        for at_z, piece in sums:
            spread[pl.ds(pl.multiple_of(at_z * slab, slab), rows), :] += piece
        return carry

    lax.fori_loop(0, lax.div(count + unroll - 1, unroll), some, 0)
    chosen = trial_ref[accept_ref[0]]
    for x in range(slab):
        new = weights_ref[x] + chosen * direction_ref[x]
        new_ref[x] = new
        grad_ref[x] = jnp.transpose(spread[pl.ds(x, size_z, stride=slab), :]) - new
    mix_planes(lambda x: grad_ref[x], kern_y_ref, kern_z_ref, spread, planes_ref, slab)


def body(
    grid_weights,
    direction,
    kern_x,
    kern_y,
    kern_z,
    interp,
    block_corner,
    block_offsets,
    labels,
    trial_steps,
    accept,
):
    slab, size_y, size_z = grid_weights.shape
    size_x = kern_x.shape[0]
    devices = lax.axis_size("pts")
    blocks, cols = block_offsets.shape
    per_block = interp.shape[1]
    points = blocks * per_block * devices
    group = max(1, PACK // slab)
    pack = group * slab
    units = size_z // group
    pieces = max(1, 64 // devices)

    packed = block_corner[0] + block_corner[1] * 256 + block_corner[2] * 65536
    packed = jnp.broadcast_to(packed[None], (8, blocks))
    kern_high, kern_low = widen_kern(kern_x, devices, slab, group)

    smem = pl.BlockSpec(memory_space=pltpu.SMEM)
    vmem = pl.BlockSpec(memory_space=pltpu.VMEM)
    hbm = pl.BlockSpec(memory_space=pl.ANY)
    limit = dict(vmem_limit_bytes=VMEM_BYTES)
    planes_shape = jax.ShapeDtypeStruct((units, pack, size_y), BF16)
    rows_scratch = pltpu.VMEM((size_z * slab, size_y), F32)
    planes_scratch = pltpu.VMEM((devices, units, pack, size_y), BF16)
    image_scratch = pltpu.VMEM((size_z, size_x, size_y), F32)
    interp_scratch = pltpu.VMEM(interp.shape, BF16)
    point_scratch = pltpu.VMEM((blocks, per_block), F32)
    point_shape = jax.ShapeDtypeStruct((blocks, per_block), F32)

    planes_w, planes_d = pl.pallas_call(
        planes_kernel,
        in_specs=[vmem] * 4,
        out_specs=[vmem] * 2,
        out_shape=[planes_shape] * 2,
        scratch_shapes=[rows_scratch],
        compiler_params=pltpu.CompilerParams(**limit),
        name="planes",
    )(grid_weights, direction, kern_y, kern_z)

    probability, split, block_list, corners, offsets, terms = pl.pallas_call(
        functools.partial(forward_kernel, group),
        in_specs=[smem] * 3 + [vmem] * 9 + [hbm],
        out_specs=[vmem] * 6,
        out_shape=[
            point_shape,
            jax.ShapeDtypeStruct((PACK, 128), BF16),
            jax.ShapeDtypeStruct((devices + 8, blocks), jnp.int32),
            jax.ShapeDtypeStruct((devices, blocks), jnp.int32),
            jax.ShapeDtypeStruct((devices, blocks, cols), jnp.int16),
            jax.ShapeDtypeStruct((devices, blocks, cols), BF16),
        ],
        scratch_shapes=[
            planes_scratch,
            planes_scratch,
            pltpu.VMEM((devices, 8, blocks), jnp.int32),
            image_scratch,
            image_scratch,
            interp_scratch,
            point_scratch,
            point_scratch,
            point_scratch,
            pltpu.VMEM((blocks, cols), F32),
            pltpu.VMEM((blocks, cols), BF16),
            pltpu.VMEM((blocks, cols), jnp.int16),
            rows_scratch,
            rows_scratch,
            pltpu.VMEM((devices, blocks, blocks), F32),
            pltpu.SemaphoreType.DMA,
            *relay_sems(devices, pieces),
            *relay_sems(devices, pieces),
            *relay_sems(devices, 1),
            *relay_sems(devices, 1),
            *relay_sems(devices, 1),
        ],
        compiler_params=pltpu.CompilerParams(collective_id=0, has_side_effects=True, **limit),
        name="forward",
    )(
        block_corner,
        trial_steps,
        accept,
        planes_w,
        planes_d,
        packed,
        kern_high,
        kern_low,
        block_offsets,
        labels,
        grid_weights,
        direction,
        interp,
    )

    new_weights, grid_gradient, bend_planes = pl.pallas_call(
        spread_kernel,
        in_specs=[smem] * 4 + [vmem] * 6,
        out_specs=[vmem] * 3,
        out_shape=[
            jax.ShapeDtypeStruct(grid_weights.shape, F32),
            jax.ShapeDtypeStruct(grid_weights.shape, F32),
            planes_shape,
        ],
        scratch_shapes=[
            pltpu.VMEM((devices * blocks, cols), jnp.int32),
            pltpu.VMEM((devices * blocks, cols), F32),
            rows_scratch,
        ],
        compiler_params=pltpu.CompilerParams(**limit),
        name="spread",
    )(
        block_list,
        corners,
        trial_steps,
        accept,
        offsets,
        terms,
        grid_weights,
        direction,
        kern_y,
        kern_z,
    )

    curvature, totals = pl.pallas_call(
        functools.partial(bend_kernel, group),
        in_specs=[smem] + [vmem] * 6 + [hbm],
        out_specs=[vmem] * 2,
        out_shape=[point_shape, jax.ShapeDtypeStruct((1, 128), F32)],
        scratch_shapes=[
            planes_scratch,
            pltpu.VMEM((devices, PACK, 128), BF16),
            image_scratch,
            interp_scratch,
            pltpu.SemaphoreType.DMA,
            *relay_sems(devices, pieces),
            *relay_sems(devices, 1),
        ],
        compiler_params=pltpu.CompilerParams(collective_id=1, has_side_effects=True, **limit),
        name="bend",
    )(
        block_corner,
        bend_planes,
        split,
        kern_high,
        kern_low,
        block_offsets,
        probability,
        interp,
    )

    everything = totals[0]
    loglik = everything[:NTRIAL]
    descent = everything[NTRIAL : 2 * NTRIAL]
    quad_gu, quad_du, quad_dv = (everything[2 * NTRIAL + k] for k in range(3))
    prior = 0.5 * (quad_gu + 2.0 * trial_steps * quad_du + trial_steps * trial_steps * quad_dv)
    trial_objective = (loglik - prior) / points
    trial_slope = (descent - quad_du - trial_steps * quad_dv) / points
    return (new_weights, grid_gradient, curvature, trial_objective, trial_slope)


def solution(mesh):
    return jax.shard_map(
        body,
        mesh=mesh,
        in_specs=(
            P(("parts", "pts"), None, None),
            P(("parts", "pts"), None, None),
            P(),
            P(),
            P(),
            P(("parts", "pts"), None, None),
            P(None, ("parts", "pts")),
            P(("parts", "pts"), None),
            P(("parts", "pts"), None),
            P(),
            P(),
        ),
        out_specs=(
            P(("parts", "pts"), None, None),
            P(("parts", "pts"), None, None),
            P(("parts", "pts"), None),
            P("parts"),
            P("parts"),
        ),
        check_vma=False,
    )
```

```python
import functools

import jax
import jax.numpy as jnp
from jax import lax
from jax.experimental import pallas as pl
from jax.experimental.pallas import tpu as pltpu
from jax.sharding import PartitionSpec as P

BOXX = 16
BOXY = 16
BOXZ = 8
NTRIAL = 5
PACK = 16
VMEM_BYTES = 62 * 1024 * 1024

F32 = jnp.float32
BF16 = jnp.bfloat16
NT = (((1,), (1,)), ((), ()))
MESH = pl.DeviceIdType.MESH


class Place:
    def __init__(self, devices):
        me = lax.axis_index("pts")
        self.devices = devices
        self.depths = devices // 4
        self.me = me
        self.core = lax.rem(me, 2)
        self.side = lax.rem(lax.div(me, 2), 2)
        self.depth = lax.div(me, 4)
        self.half = lax.rem(self.depth, 2)
        self.beside = self.slot(self.depth, 1 - self.side, self.core)
        self.twin = self.slot(self.depth, self.side, 1 - self.core)
        self.mate = self.slot(self.depth + 1 - 2 * self.half, self.side, self.core)

    def slot(self, depth, side, core):
        return (depth * 2 + side) * 2 + core

    def along(self, depth):
        return self.slot(depth, self.side, self.core)

    def others(self, act):
        def one(far, carry):
            for way in (-1, 1):
                depth = self.depth + way * far

                @pl.when((depth >= 0) & (depth < self.depths))
                def _():
                    act(depth)

            return carry

        lax.fori_loop(1, self.depths, one, 0)

    def greet(self):
        barrier = pltpu.get_barrier_semaphore()

        def tell(device):
            pl.semaphore_signal(
                barrier, inc=1, device_id={"pts": device}, device_id_type=MESH
            )

        self.others(lambda depth: tell(self.along(depth)))
        tell(self.beside)
        tell(self.twin)
        pl.semaphore_wait(barrier, self.depths + 1)

    def push(self, source, landing, send_sem, recv_sem, device):
        return pltpu.make_async_remote_copy(
            src_ref=source,
            dst_ref=landing,
            send_sem=send_sem,
            recv_sem=recv_sem,
            device_id={"pts": device},
            device_id_type=MESH,
        )


class Relay:
    def __init__(self, place, own, buf, sems, halved=False):
        self.place = place
        self.own = own
        self.buf = buf
        self.line_sem, self.side_sem, self.twin_sem, self.recv = sems
        self.pieces = self.recv.shape[1]
        self.size = buf.shape[1] // self.pieces
        self.halved = halved

    def own_rows(self, piece, depth):
        first = piece * self.size
        if self.halved:
            first = first + lax.rem(depth, 2) * self.buf.shape[1]
        return self.own.at[pl.ds(first, self.size)]

    def landing(self, slot, piece):
        return self.buf.at[slot, pl.ds(piece * self.size, self.size)]

    def line_copy(self, piece, depth):
        here = self.place
        return here.push(
            self.own_rows(piece, depth),
            self.landing(here.me, piece),
            self.line_sem.at[depth, piece],
            self.recv.at[here.me, piece],
            here.along(depth),
        )

    def side_copy(self, piece, depth, mine=False):
        here = self.place
        slot = here.along(depth)
        landing = self.landing(slot, piece)
        return here.push(
            self.own_rows(piece, depth) if mine else landing,
            landing,
            self.side_sem.at[depth, piece],
            self.recv.at[slot, piece],
            here.beside,
        )

    def twin_copy(self, piece, depth, side, mine=False):
        here = self.place
        slot = here.slot(depth, side, here.core)
        landing = self.landing(slot, piece)
        return here.push(
            self.own_rows(piece, depth) if mine else landing,
            landing,
            self.twin_sem.at[depth * 2 + side, piece],
            self.recv.at[slot, piece],
            here.twin,
        )

    def take(self, slot, piece):
        here = self.place
        landing = self.landing(slot, piece)
        here.push(
            landing, landing, self.twin_sem.at[0, piece], self.recv.at[slot, piece], here.twin
        ).wait_recv()

    def keep_own(self):
        here = self.place
        count = self.buf.shape[1]
        first = here.half * count if self.halved else 0
        self.buf[here.me] = self.own[pl.ds(first, count)]

    def start_own(self):
        here = self.place

        def one(piece, carry):
            here.others(lambda depth: self.line_copy(piece, depth).start())
            self.side_copy(piece, here.depth, mine=True).start()
            self.twin_copy(piece, here.depth, here.side, mine=True).start()
            return carry

        lax.fori_loop(0, self.pieces, one, 0)

    def line_events(self, piece):
        here = self.place

        def one(depth):
            self.take(here.along(depth), piece)
            self.side_copy(piece, depth).start()
            self.twin_copy(piece, depth, here.side).start()

        here.others(one)

    def side_events(self, piece):
        here = self.place

        def one(depth):
            self.take(here.slot(depth, 1 - here.side, here.core), piece)
            self.twin_copy(piece, depth, 1 - here.side).start()

        one(here.depth)
        here.others(one)

    def twin_events(self, piece):
        here = self.place

        def one(pair, carry):
            self.take(pair * 2 + (1 - here.core), piece)
            return carry

        lax.fori_loop(0, here.devices // 2, one, 0)

    def run(self, work=None, steps=0, mix=None, tail=None, riders=()):
        pieces = self.pieces

        def one(wave, carry):
            for rider in riders:

                @pl.when(wave == 0)
                def _():
                    rider.line_events(0)

                @pl.when(wave == 1)
                def _():
                    rider.side_events(0)

                @pl.when(wave == 2)
                def _():
                    rider.twin_events(0)

            @pl.when(wave < pieces)
            def _():
                self.line_events(wave)

            if tail is not None:

                @pl.when(wave == pieces - 1)
                def _():
                    tail()

            @pl.when((wave >= 1) & (wave < pieces + 1))
            def _():
                self.side_events(wave - 1)

            if work is not None:

                @pl.when(wave < steps)
                def _():
                    work(wave)

            @pl.when(wave >= 2)
            def _():
                self.twin_events(wave - 2)
                if mix is not None:
                    mix(wave - 2)

            return carry

        lax.fori_loop(0, pieces + 2, one, 0)

    def finish(self):
        here = self.place

        def one(step, carry):
            piece = lax.div(step, here.depths)
            depth = lax.rem(step, here.depths)

            @pl.when(depth != here.depth)
            def _():
                self.line_copy(piece, depth).wait_send()

            self.side_copy(piece, depth).wait_send()
            self.twin_copy(piece, depth, 0).wait_send()
            self.twin_copy(piece, depth, 1).wait_send()
            return carry

        lax.fori_loop(0, self.pieces * here.depths, one, 0)


def relay_sems(devices, pieces):
    depths = devices // 4
    return [
        pltpu.SemaphoreType.DMA((depths, pieces)),
        pltpu.SemaphoreType.DMA((depths, pieces)),
        pltpu.SemaphoreType.DMA((depths * 2, pieces)),
        pltpu.SemaphoreType.DMA((devices, pieces)),
    ]


def mix_depth(planes_ref, kh_ref, kl_ref, image, group, size_x, first, count):
    devices, _, pack, lanes = planes_ref.shape

    def one(step, carry):
        at = first + step * 2
        pair = [planes_ref[:, at + t].reshape(devices * pack, lanes) for t in range(2)]
        rhs = jnp.concatenate(pair, axis=1)
        mixed = jnp.dot(kh_ref[...], rhs, preferred_element_type=F32)
        mixed = mixed + jnp.dot(kl_ref[...], rhs, preferred_element_type=F32)
        for t in range(2):
            for g in range(group):
                image[(at + t) * group + g] = mixed[
                    g * size_x : (g + 1) * size_x, t * lanes : (t + 1) * lanes
                ]
        return carry

    lax.fori_loop(0, count // 2, one, 0)


def split_offset(offset):
    bits_y, bits_z = BOXY.bit_length() - 1, BOXZ.bit_length() - 1
    return offset >> (bits_y + bits_z), (offset >> bits_z) & (BOXY - 1), offset & (BOXZ - 1)


def pick_values(image, half, corner, offset):
    half_z, _, size_y = image.shape
    cols = offset.shape[-1]
    box_rows = BOXZ * BOXX
    at_x, at_y, at_z = corner & 255, (corner >> 8) & 255, corner >> 16
    from_z = at_z - half * half_z
    first = jnp.clip(from_z, 0, half_z - BOXZ)
    off_x, off_y, off_z = split_offset(offset)
    y_cell = at_y + off_y
    box_row = (off_z + (from_z - first)) * BOXX + off_x
    box = image[pl.ds(first, BOXZ), pl.ds(at_x, BOXX), :]
    box = box.reshape(box_rows, size_y).astype(BF16)
    y_line = lax.broadcasted_iota(jnp.int32, (size_y, cols), 0)
    pick_y = jnp.where(y_line == y_cell, 1.0, 0.0).astype(BF16)
    lines = jnp.dot(box, pick_y, preferred_element_type=F32)
    row_line = lax.broadcasted_iota(jnp.int32, (box_rows, cols), 0)
    line = jnp.where(row_line == box_row, lines, 0.0)
    return jnp.sum(line, axis=0, keepdims=True)


def pick_blocks(image, half, corner_ref, line, offsets_ref, base, values, first, count):
    unroll = min(16, count)

    def some(part, carry):
        for k in range(unroll):
            block = first + part * unroll + k
            values[pl.ds(block, 1), :] = pick_values(
                image, half, corner_ref[line, block], offsets_ref[pl.ds(base + block, 1), :]
            )
        return carry

    lax.fori_loop(0, count // unroll, some, 0)


def power_below(value):
    return 1 << (value.bit_length() - 1)


def two_parts(value):
    high = value.astype(BF16)
    return high, (value - high.astype(F32)).astype(BF16)


def dot_parts(left, right):
    (left_high, left_low), (right_high, right_low) = left, right
    small = lax.dot_general(left_high, right_low, NT, preferred_element_type=F32)
    small = small + lax.dot_general(left_low, right_high, NT, preferred_element_type=F32)
    return small + lax.dot_general(left_high, right_high, NT, preferred_element_type=F32)


def mix_planes(field_of, kern_y, kern_z, rows, planes_ref, slab):
    size_z = kern_z[0].shape[0]
    for x in range(slab):
        inner = dot_parts(kern_z, two_parts(field_of(x)))
        rows[pl.ds(x, size_z, stride=slab), :] = dot_parts(two_parts(inner), kern_y)
    planes_ref[...] = rows[...].astype(BF16).reshape(planes_ref.shape)


def planes_kernel(
    weights_ref,
    direction_ref,
    kern_x_ref,
    kern_y_ref,
    kern_z_ref,
    corner_ref,
    offsets_ref,
    out_u,
    out_d,
    kh_ref,
    kl_ref,
    packed_ref,
    offs_ref,
    rows,
    rows_d,
):
    slab = weights_ref.shape[0]
    kern_y, kern_z = two_parts(kern_y_ref[...]), two_parts(kern_z_ref[...])
    mix_planes(lambda x: weights_ref[x], kern_y, kern_z, rows, out_u, slab)
    mix_planes(lambda x: direction_ref[x], kern_y, kern_z, rows_d, out_d, slab)
    packed = corner_ref[0:1] + corner_ref[1:2] * 256 + corner_ref[2:3] * 65536
    packed_ref[...] = jnp.broadcast_to(packed, packed_ref.shape)
    offs_ref[...] = offsets_ref[...].astype(jnp.int16)
    size_x, wide = kern_x_ref.shape[0], kh_ref.shape[1]
    group = kh_ref.shape[0] // size_x
    pack = group * slab
    source = lax.broadcasted_iota(jnp.int32, (size_x, wide), 0)
    column = lax.broadcasted_iota(jnp.int32, (size_x, wide), 1)
    same = source == lax.div(column, pack) * slab + lax.rem(column, slab)
    layer = lax.div(lax.rem(column, pack), slab)
    for part, out_ref in zip(two_parts(kern_x_ref[...]), (kh_ref, kl_ref)):
        for g in range(group):
            select = jnp.where(same & (layer == g), 1.0, 0.0).astype(BF16)
            spot = jnp.dot(part, select, preferred_element_type=F32)
            out_ref[g * size_x : (g + 1) * size_x] = spot.astype(BF16)


def rank_blocks(corners, me, slab, ranks_ref, list_ref):
    devices, blocks = corners.shape
    from_x = (corners & 255) - me * slab
    touch = jnp.where((from_x < slab) & (from_x > -BOXX), 1.0, 0.0)
    earlier = lax.broadcasted_iota(jnp.int32, (blocks, blocks), 0)
    earlier = earlier < lax.broadcasted_iota(jnp.int32, (blocks, blocks), 1)
    within = jnp.dot(
        touch.astype(BF16), jnp.where(earlier, 1.0, 0.0).astype(BF16), preferred_element_type=F32
    )
    count = jnp.sum(touch, axis=1, keepdims=True)
    below = lax.broadcasted_iota(jnp.int32, (devices, devices), 1)
    below = below < lax.broadcasted_iota(jnp.int32, (devices, devices), 0)
    base = jnp.dot(
        jnp.where(below, 1.0, 0.0).astype(BF16),
        jnp.broadcast_to(count, (devices, blocks)).astype(BF16),
        preferred_element_type=F32,
    )
    ranks = jnp.where(touch > 0.0, base + within, -1.0)
    for device in range(devices):
        line = jnp.broadcast_to(ranks[device : device + 1], (blocks, blocks))
        ranks_ref[device] = jnp.transpose(line)
    total = jnp.sum(touch)
    list_ref[pl.ds(devices, 8), :] = jnp.full((8, blocks), total, F32).astype(jnp.int32)


def list_blocks(ranks_ref, list_ref, line):
    devices, blocks, _ = ranks_ref.shape
    wanted = lax.broadcasted_iota(jnp.int32, (blocks, blocks), 1) + line * blocks
    wanted = wanted.astype(F32)
    block = lax.broadcasted_iota(jnp.int32, (blocks, blocks), 0).astype(F32)

    def one(device, ids):
        hit = ranks_ref[device] == wanted
        start = (device * blocks).astype(F32)
        return ids + jnp.where(hit, block + start, 0.0)

    ids = lax.fori_loop(0, devices, one, jnp.zeros((blocks, blocks), F32))
    ids = jnp.sum(ids, axis=0, keepdims=True)
    list_ref[pl.ds(line, 1), :] = ids.astype(jnp.int32)


def log_sigmoid(value):
    return jnp.minimum(value, 0.0) - jnp.log1p(jnp.exp(-jnp.abs(value)))


def apply_interp(values, interp, outs, first, count):
    unroll = min(16, count)
    cols = values[0].shape[1]

    def some(part, carry):
        for k in range(unroll):
            block = first + part * unroll + k
            top = lax.broadcasted_iota(jnp.int32, (8, cols), 0)
            rows = jnp.broadcast_to(values[0][pl.ds(block, 1), :], (8, cols))
            for f in range(1, len(values)):
                rows = jnp.where(top == f, values[f][pl.ds(block, 1), :], rows)
            line = lax.dot_general(
                rows.astype(BF16), interp[block], NT, preferred_element_type=F32
            )
            for f, out_ref in enumerate(outs):
                out_ref[pl.ds(block, 1), :] = line[f : f + 1]
        return carry

    lax.fori_loop(0, count // unroll, some, 0)


def forward_kernel(
    group,
    trial_ref,
    accept_ref,
    own_u,
    own_d,
    packed_ref,
    offs_ref,
    kh_ref,
    kl_ref,
    offsets_ref,
    labels_ref,
    weights_ref,
    direction_ref,
    interp_ref,
    prob_ref,
    split_ref,
    list_ref,
    corners_ref,
    pair_packed,
    pair_offsets,
    all_offs,
    all_terms,
    buf_u,
    buf_d,
    all_packed,
    image_u,
    image_d,
    interp,
    mine_u,
    mine_d,
    theirs,
    out_u,
    out_d,
    in_u,
    in_d,
    mate_offs,
    mate_u,
    mate_d,
    latent_ref,
    slope_ref,
    res_ref,
    own_terms,
    weights_t,
    direction_t,
    ranks_ref,
    corner_smem,
    local_sem,
    mate_send,
    mate_recv,
    *sems,
):
    devices = buf_u.shape[0]
    blocks, per_block = labels_ref.shape
    slab, size_y, size_z = weights_ref.shape
    half_z, size_x, _ = image_u.shape
    place = Place(devices)
    load = pltpu.make_async_copy(interp_ref, interp, local_sem.at[0])
    load.start()
    u = Relay(place, own_u, buf_u, sems[0:4], halved=True)
    d = Relay(place, own_d, buf_d, sems[4:8], halved=True)
    o = Relay(place, offs_ref, all_offs, sems[8:12])
    t = Relay(place, own_terms, all_terms, sems[12:16])
    c = Relay(place, packed_ref, all_packed, sems[16:20])

    def swap(source, landing, k):
        return place.push(source, landing, mate_send.at[k], mate_recv.at[k], place.mate)

    mate_rows = pl.ds(pl.multiple_of(place.mate * slab, slab), slab)
    swaps = [
        swap(offs_ref, mate_offs, 0),
        swap(out_u, in_u, 1),
        swap(out_d, in_d, 2),
        swap(image_u.at[:, mate_rows, :], mate_u, 3),
        swap(image_d.at[:, mate_rows, :], mate_d, 4),
    ]
    place.greet()
    c.start_own()
    u.start_own()
    swaps[0].start()
    for relay in (c, u, d, o):
        relay.keep_own()
    pair_offsets[pl.ds(0, blocks)] = offsets_ref[...]
    for x in range(slab):
        weights_t[pl.ds(x, size_z, stride=slab), :] = jnp.transpose(weights_ref[x])
        direction_t[pl.ds(x, size_z, stride=slab), :] = jnp.transpose(direction_ref[x])

    def mixer(relay, image):
        return lambda piece: mix_depth(
            relay.buf, kh_ref, kl_ref, image, group, size_x, piece * relay.size, relay.size
        )

    u.run(mix=mixer(u, image_u), tail=d.start_own, riders=(c,))
    swaps[0].wait()
    pair_offsets[pl.ds(blocks, blocks)] = mate_offs[...].astype(jnp.int32)
    corners = all_packed[:, 0, :]
    corners_ref[...] = corners
    pair_packed[...] = jnp.concatenate([packed_ref[0:4], all_packed[place.mate, 0:4]], axis=0)
    rank_blocks(corners, place.me, slab, ranks_ref, list_ref)
    to_smem = pltpu.make_async_copy(pair_packed, corner_smem, local_sem.at[1])
    to_smem.start()
    to_smem.wait()
    steps = power_below(u.pieces + 2)
    some, lines = blocks // steps, -(-devices // steps)

    def pick(image, mine, first, count):
        line, base = (0, 0) if mine is not theirs else (4, blocks)
        pick_blocks(
            image, place.half, corner_smem, line, pair_offsets, base, mine, first, count
        )

    def early(step):
        pick(image_u, theirs, step * some, some)
        pick(image_u, mine_u, step * some, some)
        for k in range(lines):
            list_blocks(ranks_ref, list_ref, step * lines + k)

    d.run(work=early, steps=steps, mix=mixer(d, image_d), tail=o.start_own)
    swaps[3].start()
    out_u[...] = theirs[...].astype(BF16)
    pick(image_d, theirs, 0, blocks)
    swaps[1].start()
    out_d[...] = theirs[...].astype(BF16)
    o.line_events(0)
    pick(image_d, mine_d, 0, blocks // 4)
    swaps[2].start()
    pick(image_d, mine_d, blocks // 4, blocks - blocks // 4)
    swaps[4].start()
    o.side_events(0)
    swaps[1].wait()
    swaps[2].wait()
    mine_u[...] = mine_u[...] + in_u[...].astype(F32)
    mine_d[...] = mine_d[...] + in_d[...].astype(F32)
    load.wait()
    apply_interp((mine_u, mine_d), interp, (latent_ref, slope_ref), 0, blocks)
    slope = slope_ref[...]
    latent = latent_ref[...]
    prob = jax.nn.sigmoid(latent + trial_ref[accept_ref[0]] * slope)
    prob_ref[...] = prob
    target = labels_ref[...].astype(F32)
    res_ref[...] = (target - prob).astype(BF16).astype(F32)
    unroll = 16

    def back(step, carry):
        for k in range(unroll):
            block = step * unroll + k
            row = jnp.broadcast_to(res_ref[pl.ds(block, 1), :], (8, per_block))
            term = jnp.dot(row.astype(BF16), interp[block], preferred_element_type=F32)
            theirs[pl.ds(block, 1), :] = term[0:1]
        return carry

    lax.fori_loop(0, blocks // unroll, back, 0)
    own_terms[...] = theirs[...].astype(BF16)
    t.keep_own()
    o.twin_events(0)
    for relay in (c, u, d, o):
        relay.finish()
    t.start_own()
    swaps[3].wait()
    swaps[4].wait()
    own_rows = pl.ds(pl.multiple_of(place.me * slab, slab), slab)
    here_z = pl.ds(pl.multiple_of(place.half * half_z * slab, slab), half_z * slab)
    there_z = pl.ds(pl.multiple_of((1 - place.half) * half_z * slab, slab), half_z * slab)

    def quad(field_t, image, mate):
        both = (half_z * slab, size_y)
        near = field_t[here_z] * image[:, own_rows, :].reshape(both)
        return jnp.sum(near + field_t[there_z] * mate[...].reshape(both))

    signed = 2.0 * target - 1.0
    line = lax.broadcasted_iota(jnp.int32, (8, 128), 0)
    lane = lax.broadcasted_iota(jnp.int32, (8, 128), 1)
    sums = jnp.zeros((8, 128), F32)
    for k in range(NTRIAL):
        at_trial = latent + trial_ref[k] * slope
        loglik = jnp.sum(log_sigmoid(signed * at_trial))
        descent = jnp.sum((target - jax.nn.sigmoid(at_trial)) * slope)
        sums = jnp.where((line == 0) & (lane == k), loglik, sums)
        sums = jnp.where((line == 1) & (lane == k), descent, sums)
    sums = jnp.where(line == 2, quad(weights_t, image_u, mate_u), sums)
    sums = jnp.where(line == 3, quad(direction_t, image_u, mate_u), sums)
    sums = jnp.where(line == 4, quad(direction_t, image_d, mate_d), sums)
    first = sums.astype(BF16).astype(F32)
    second = (sums - first).astype(BF16).astype(F32)
    third = sums - first - second
    split_ref[...] = jnp.concatenate([first, second, third], axis=0).astype(BF16)
    t.run()
    t.finish()


def bend_kernel(
    group,
    points,
    corner_smem,
    trial_ref,
    own_ref,
    split_ref,
    kh_ref,
    kl_ref,
    pair_offsets,
    prob_ref,
    interp_ref,
    out_ref,
    trials_ref,
    buf,
    all_split,
    image,
    interp,
    mine,
    theirs,
    sent,
    got,
    local_sem,
    mate_send,
    mate_recv,
    *sems,
):
    devices = buf.shape[0]
    blocks = prob_ref.shape[0]
    size_x = image.shape[1]
    place = Place(devices)
    load = pltpu.make_async_copy(interp_ref, interp, local_sem)
    load.start()
    b = Relay(place, own_ref, buf, sems[0:4], halved=True)
    s = Relay(place, split_ref, all_split, sems[4:8])
    swap = place.push(sent, got, mate_send, mate_recv, place.mate)
    place.greet()
    s.start_own()
    b.start_own()
    b.keep_own()
    s.keep_own()
    b.run(
        mix=lambda piece: mix_depth(
            buf, kh_ref, kl_ref, image, group, size_x, piece * b.size, b.size
        ),
        riders=(s,),
    )

    def pick(line, base, values, first, count):
        pick_blocks(
            image, place.half, corner_smem, line, pair_offsets, base, values, first, count
        )

    pick(4, blocks, theirs, 0, blocks)
    sent[...] = theirs[...].astype(BF16)
    pick(0, 0, mine, 0, blocks // 4)
    swap.start()
    pick(0, 0, mine, blocks // 4, blocks - blocks // 4)
    total = jnp.sum(all_split[...].astype(F32), axis=0)
    total = total[0:8] + total[8:16] + total[16:24]
    lane = lax.broadcasted_iota(jnp.int32, (1, 128), 1)
    step = jnp.zeros((1, 128), F32)
    for k in range(NTRIAL):
        step = jnp.where(lane == k, trial_ref[k], step)
    loglik, descent, quad_gu, quad_du, quad_dv = (total[k : k + 1] for k in range(5))
    prior = 0.5 * (quad_gu + 2.0 * step * quad_du + step * step * quad_dv)
    trials_ref[0:1] = (loglik - prior) / points
    trials_ref[1:2] = (descent - quad_du - step * quad_dv) / points
    load.wait()
    swap.wait()
    mine[...] = mine[...] + got[...].astype(F32)
    apply_interp((mine,), interp, (out_ref,), 0, blocks)
    prob = prob_ref[...]
    out_ref[...] = prob * (1.0 - prob) * out_ref[...]
    b.finish()
    s.finish()


def spread_kernel(
    list_ref,
    corners_ref,
    trial_ref,
    accept_ref,
    offs_ref,
    terms_ref,
    weights_ref,
    direction_ref,
    kern_y_ref,
    kern_z_ref,
    new_ref,
    grad_ref,
    planes_ref,
    offs,
    terms,
    spread,
):
    devices, blocks, cols = offs_ref.shape
    slab, size_y, size_z = weights_ref.shape
    rows = BOXZ * slab
    unroll = 8
    me = lax.axis_index("pts")
    spread[...] = jnp.zeros_like(spread)

    def widen(device, carry):
        offs[pl.ds(pl.multiple_of(device * blocks, blocks), blocks)] = offs_ref[device].astype(
            jnp.int32
        )
        terms[pl.ds(pl.multiple_of(device * blocks, blocks), blocks)] = terms_ref[device].astype(
            F32
        )
        return carry

    lax.fori_loop(0, devices, widen, 0)
    count = list_ref[devices, 0]

    def some(part, carry):
        sums = []
        for k in range(unroll):
            at = part * unroll + k
            block = list_ref[lax.div(at, blocks), lax.rem(at, blocks)]
            packed = corners_ref[lax.div(block, blocks), lax.rem(block, blocks)]
            from_x = jnp.where(at < count, (packed & 255) - me * slab, -2 * BOXX)
            at_y = (packed >> 8) & 255
            at_z = packed >> 16
            off_x, off_y, off_z = split_offset(offs[pl.ds(block, 1), :])
            cell = off_x + from_x
            key = jnp.where((cell >= 0) & (cell < slab), off_z * slab + cell, -1)
            y_cell = off_y + at_y
            row_line = lax.broadcasted_iota(jnp.int32, (rows, cols), 0)
            y_line = lax.broadcasted_iota(jnp.int32, (size_y, cols), 0)
            left = jnp.where(row_line == key, terms[pl.ds(block, 1), :], 0.0).astype(BF16)
            right = jnp.where(y_line == y_cell, 1.0, 0.0).astype(BF16)
            sums.append((at_z, lax.dot_general(left, right, NT, preferred_element_type=F32)))
        for at_z, piece in sums:
            spread[pl.ds(pl.multiple_of(at_z * slab, slab), rows), :] += piece
        return carry

    lax.fori_loop(0, lax.div(count + unroll - 1, unroll), some, 0)
    chosen = trial_ref[accept_ref[0]]
    for x in range(slab):
        new = weights_ref[x] + chosen * direction_ref[x]
        new_ref[x] = new
        grad_ref[x] = jnp.transpose(spread[pl.ds(x, size_z, stride=slab), :]) - new
    kern_y, kern_z = two_parts(kern_y_ref[...]), two_parts(kern_z_ref[...])
    mix_planes(lambda x: grad_ref[x], kern_y, kern_z, spread, planes_ref, slab)


def body(
    grid_weights,
    direction,
    kern_x,
    kern_y,
    kern_z,
    interp,
    block_corner,
    block_offsets,
    labels,
    trial_steps,
    accept,
):
    slab, size_y, size_z = grid_weights.shape
    size_x = kern_x.shape[0]
    devices = lax.axis_size("pts")
    blocks, cols = block_offsets.shape
    per_block = interp.shape[1]
    points = blocks * per_block * devices
    group = max(1, PACK // slab)
    pack = group * slab
    units = size_z // group
    pieces = max(1, 64 // devices)

    smem = pl.BlockSpec(memory_space=pltpu.SMEM)
    vmem = pl.BlockSpec(memory_space=pltpu.VMEM)
    hbm = pl.BlockSpec(memory_space=pl.ANY)
    limit = dict(vmem_limit_bytes=VMEM_BYTES)
    planes_shape = jax.ShapeDtypeStruct((units, pack, size_y), BF16)
    rows_scratch = pltpu.VMEM((size_z * slab, size_y), F32)
    planes_scratch = pltpu.VMEM((devices, units // 2, pack, size_y), BF16)
    image_scratch = pltpu.VMEM((size_z // 2, size_x, size_y), F32)
    interp_scratch = pltpu.VMEM(interp.shape, BF16)
    point_scratch = pltpu.VMEM((blocks, per_block), F32)
    point_shape = jax.ShapeDtypeStruct((blocks, per_block), F32)

    wide_shape = jax.ShapeDtypeStruct((group * size_x, devices * pack), BF16)
    planes_w, planes_d, kern_high, kern_low, packed, offs = pl.pallas_call(
        planes_kernel,
        in_specs=[vmem] * 7,
        out_specs=[vmem] * 6,
        out_shape=[
            planes_shape,
            planes_shape,
            wide_shape,
            wide_shape,
            jax.ShapeDtypeStruct((8, blocks), jnp.int32),
            jax.ShapeDtypeStruct((blocks, cols), jnp.int16),
        ],
        scratch_shapes=[rows_scratch, rows_scratch],
        compiler_params=pltpu.CompilerParams(**limit),
        name="planes",
    )(grid_weights, direction, kern_x, kern_y, kern_z, block_corner, block_offsets)

    pick_scratch = pltpu.VMEM((blocks, cols), F32)
    swap_scratch = pltpu.VMEM((blocks, cols), BF16)
    mate_scratch = pltpu.VMEM((size_z // 2, slab, size_y), F32)
    probability, split, block_list, corners, pair_packed, pair_offsets, offsets, terms = (
        pl.pallas_call(
            functools.partial(forward_kernel, group),
            in_specs=[smem] * 2 + [vmem] * 10 + [hbm],
            out_specs=[vmem] * 8,
            out_shape=[
                point_shape,
                jax.ShapeDtypeStruct((24, 128), BF16),
                jax.ShapeDtypeStruct((devices + 8, blocks), jnp.int32),
                jax.ShapeDtypeStruct((devices, blocks), jnp.int32),
                jax.ShapeDtypeStruct((8, blocks), jnp.int32),
                jax.ShapeDtypeStruct((2 * blocks, cols), jnp.int32),
                jax.ShapeDtypeStruct((devices, blocks, cols), jnp.int16),
                jax.ShapeDtypeStruct((devices, blocks, cols), BF16),
            ],
            scratch_shapes=[
                planes_scratch,
                planes_scratch,
                pltpu.VMEM((devices, 8, blocks), jnp.int32),
                image_scratch,
                image_scratch,
                interp_scratch,
                pick_scratch,
                pick_scratch,
                pick_scratch,
                swap_scratch,
                swap_scratch,
                swap_scratch,
                swap_scratch,
                pltpu.VMEM((blocks, cols), jnp.int16),
                mate_scratch,
                mate_scratch,
                point_scratch,
                point_scratch,
                point_scratch,
                swap_scratch,
                rows_scratch,
                rows_scratch,
                pltpu.VMEM((devices, blocks, blocks), F32),
                pltpu.SMEM((8, blocks), jnp.int32),
                pltpu.SemaphoreType.DMA((2,)),
                pltpu.SemaphoreType.DMA((5,)),
                pltpu.SemaphoreType.DMA((5,)),
                *relay_sems(devices, pieces),
                *relay_sems(devices, pieces),
                *relay_sems(devices, 1),
                *relay_sems(devices, 1),
                *relay_sems(devices, 1),
            ],
            compiler_params=pltpu.CompilerParams(
                collective_id=0, has_side_effects=True, **limit
            ),
            name="forward",
        )(
            trial_steps,
            accept,
            planes_w,
            planes_d,
            packed,
            offs,
            kern_high,
            kern_low,
            block_offsets,
            labels,
            grid_weights,
            direction,
            interp,
        )
    )

    new_weights, grid_gradient, bend_planes = pl.pallas_call(
        spread_kernel,
        in_specs=[smem] * 4 + [vmem] * 6,
        out_specs=[vmem] * 3,
        out_shape=[
            jax.ShapeDtypeStruct(grid_weights.shape, F32),
            jax.ShapeDtypeStruct(grid_weights.shape, F32),
            planes_shape,
        ],
        scratch_shapes=[
            pltpu.VMEM((devices * blocks, cols), jnp.int32),
            pltpu.VMEM((devices * blocks, cols), F32),
            rows_scratch,
        ],
        compiler_params=pltpu.CompilerParams(**limit),
        name="spread",
    )(
        block_list,
        corners,
        trial_steps,
        accept,
        offsets,
        terms,
        grid_weights,
        direction,
        kern_y,
        kern_z,
    )

    curvature, trials = pl.pallas_call(
        functools.partial(bend_kernel, group, points),
        in_specs=[smem] * 2 + [vmem] * 6 + [hbm],
        out_specs=[vmem] * 2,
        out_shape=[point_shape, jax.ShapeDtypeStruct((2, 128), F32)],
        scratch_shapes=[
            planes_scratch,
            pltpu.VMEM((devices, 24, 128), BF16),
            image_scratch,
            interp_scratch,
            pick_scratch,
            pick_scratch,
            swap_scratch,
            swap_scratch,
            pltpu.SemaphoreType.DMA,
            pltpu.SemaphoreType.DMA,
            pltpu.SemaphoreType.DMA,
            *relay_sems(devices, pieces),
            *relay_sems(devices, 1),
        ],
        compiler_params=pltpu.CompilerParams(collective_id=1, has_side_effects=True, **limit),
        name="bend",
    )(
        pair_packed,
        trial_steps,
        bend_planes,
        split,
        kern_high,
        kern_low,
        pair_offsets,
        probability,
        interp,
    )
    return (new_weights, grid_gradient, curvature, trials[0, :NTRIAL], trials[1, :NTRIAL])


def solution(mesh):
    return jax.shard_map(
        body,
        mesh=mesh,
        in_specs=(
            P(("parts", "pts"), None, None),
            P(("parts", "pts"), None, None),
            P(),
            P(),
            P(),
            P(("parts", "pts"), None, None),
            P(None, ("parts", "pts")),
            P(("parts", "pts"), None),
            P(("parts", "pts"), None),
            P(),
            P(),
        ),
        out_specs=(
            P(("parts", "pts"), None, None),
            P(("parts", "pts"), None, None),
            P(("parts", "pts"), None),
            P("parts"),
            P("parts"),
        ),
        check_vma=False,
    )
```

```python
import functools

import jax
import jax.numpy as jnp
from jax import lax
from jax.experimental import pallas as pl
from jax.experimental.pallas import tpu as pltpu
from jax.sharding import PartitionSpec as P

BOXX = 16
BOXY = 16
BOXZ = 8
NTRIAL = 5
PACK = 16
BESIDE = 4
UNROLL = 32
VMEM_BYTES = 62 * 1024 * 1024

F32 = jnp.float32
BF16 = jnp.bfloat16
NT = (((1,), (1,)), ((), ()))
MESH = pl.DeviceIdType.MESH


class Place:
    def __init__(self, devices):
        me = lax.axis_index("pts")
        self.devices = devices
        self.depths = devices // 4
        self.me = me
        self.core = lax.rem(me, 2)
        self.side = lax.rem(lax.div(me, 2), 2)
        self.depth = lax.div(me, 4)
        self.half = lax.rem(self.depth, 2)
        self.beside = self.slot(self.depth, 1 - self.side, self.core)
        self.twin = self.slot(self.depth, self.side, 1 - self.core)
        self.mate = self.slot(self.depth + 1 - 2 * self.half, self.side, self.core)

    def slot(self, depth, side, core):
        return (depth * 2 + side) * 2 + core

    def along(self, depth):
        return self.slot(depth, self.side, self.core)

    def others(self, act):
        def one(far, carry):
            for way in (-1, 1):
                depth = self.depth + way * far

                @pl.when((depth >= 0) & (depth < self.depths))
                def _():
                    act(depth)

            return carry

        lax.fori_loop(1, self.depths, one, 0)

    def greet(self):
        barrier = pltpu.get_barrier_semaphore()

        def tell(device):
            pl.semaphore_signal(
                barrier, inc=1, device_id={"pts": device}, device_id_type=MESH
            )

        self.others(lambda depth: tell(self.along(depth)))
        tell(self.beside)
        tell(self.twin)

    def meet(self):
        pl.semaphore_wait(pltpu.get_barrier_semaphore(), self.depths + 1)

    def push(self, source, landing, send_sem, recv_sem, device):
        return pltpu.make_async_remote_copy(
            src_ref=source,
            dst_ref=landing,
            send_sem=send_sem,
            recv_sem=recv_sem,
            device_id={"pts": device},
            device_id_type=MESH,
        )


class Relay:
    def __init__(self, place, own, buf, sems, halved=False):
        self.place = place
        self.own = own
        self.buf = buf
        self.line_sem, self.side_sem, self.twin_sem, self.recv = sems
        self.pieces = self.recv.shape[1]
        self.size = buf.shape[1] // self.pieces
        self.halved = halved

    def own_rows(self, piece, depth):
        first = piece * self.size
        if self.halved:
            first = first + lax.rem(depth, 2) * self.buf.shape[1]
        return self.own.at[pl.ds(first, self.size)]

    def landing(self, slot, piece):
        return self.buf.at[slot, pl.ds(piece * self.size, self.size)]

    def line_copy(self, piece, depth):
        here = self.place
        return here.push(
            self.own_rows(piece, depth),
            self.landing(here.me, piece),
            self.line_sem.at[depth, piece],
            self.recv.at[here.me, piece],
            here.along(depth),
        )

    def side_copy(self, piece, depth, mine=False):
        here = self.place
        slot = here.along(depth)
        landing = self.landing(slot, piece)
        return here.push(
            self.own_rows(piece, depth) if mine else landing,
            landing,
            self.side_sem.at[depth, piece],
            self.recv.at[slot, piece],
            here.beside,
        )

    def twin_copy(self, piece, depth, side, mine=False):
        here = self.place
        slot = here.slot(depth, side, here.core)
        landing = self.landing(slot, piece)
        return here.push(
            self.own_rows(piece, depth) if mine else landing,
            landing,
            self.twin_sem.at[depth * 2 + side, piece],
            self.recv.at[slot, piece],
            here.twin,
        )

    def take(self, slot, piece):
        here = self.place
        landing = self.landing(slot, piece)
        here.push(
            landing, landing, self.twin_sem.at[0, piece], self.recv.at[slot, piece], here.twin
        ).wait_recv()

    def keep_own(self):
        here = self.place
        count = self.buf.shape[1]
        first = here.half * count if self.halved else 0
        self.buf[here.me] = self.own[pl.ds(first, count)]

    def start_piece(self, piece):
        here = self.place
        here.others(lambda depth: self.line_copy(piece, depth).start())
        self.side_copy(piece, here.depth, mine=True).start()
        self.twin_copy(piece, here.depth, here.side, mine=True).start()

    def start_own(self):
        def one(piece, carry):
            self.start_piece(piece)
            return carry

        lax.fori_loop(0, self.pieces, one, 0)

    def line_events(self, piece):
        here = self.place

        def one(depth):
            self.take(here.along(depth), piece)
            self.side_copy(piece, depth).start()
            self.twin_copy(piece, depth, here.side).start()

        here.others(one)

    def side_events(self, piece):
        here = self.place

        def one(depth):
            self.take(here.slot(depth, 1 - here.side, here.core), piece)
            self.twin_copy(piece, depth, 1 - here.side).start()

        one(here.depth)
        here.others(one)

    def twin_events(self, piece):
        here = self.place

        def one(pair, carry):
            self.take(pair * 2 + (1 - here.core), piece)
            return carry

        lax.fori_loop(0, here.devices // 2, one, 0)

    def run(self, work=None, steps=0, mix=None, tail=None, riders=()):
        pieces = self.pieces

        def one(wave, carry):
            for rider in riders:

                @pl.when(wave == 0)
                def _():
                    rider.line_events(0)

                @pl.when(wave == 1)
                def _():
                    rider.side_events(0)

                @pl.when(wave == 2)
                def _():
                    rider.twin_events(0)

            @pl.when(wave < pieces)
            def _():
                self.line_events(wave)

            if tail is not None:

                @pl.when(wave == pieces - 1)
                def _():
                    tail()

            @pl.when((wave >= 1) & (wave < pieces + 1))
            def _():
                self.side_events(wave - 1)

            if work is not None:

                @pl.when(wave < steps)
                def _():
                    work(wave)

            @pl.when(wave >= 2)
            def _():
                self.twin_events(wave - 2)
                if mix is not None:
                    mix(wave - 2)

            return carry

        lax.fori_loop(0, pieces + 2, one, 0)

    def finish(self):
        here = self.place

        def one(step, carry):
            piece = lax.div(step, here.depths)
            depth = lax.rem(step, here.depths)

            @pl.when(depth != here.depth)
            def _():
                self.line_copy(piece, depth).wait_send()

            self.side_copy(piece, depth).wait_send()
            self.twin_copy(piece, depth, 0).wait_send()
            self.twin_copy(piece, depth, 1).wait_send()
            return carry

        lax.fori_loop(0, self.pieces * here.depths, one, 0)


def relay_sems(devices, pieces):
    depths = devices // 4
    return [
        pltpu.SemaphoreType.DMA((depths, pieces)),
        pltpu.SemaphoreType.DMA((depths, pieces)),
        pltpu.SemaphoreType.DMA((depths * 2, pieces)),
        pltpu.SemaphoreType.DMA((devices, pieces)),
    ]


def mix_depth(planes_ref, kh_ref, kl_ref, image, group, size_x, first, count):
    devices, _, pack, lanes = planes_ref.shape

    def one(step, carry):
        at = first + step * 2
        pair = [planes_ref[:, at + t].reshape(devices * pack, lanes) for t in range(2)]
        rhs = jnp.concatenate(pair, axis=1)
        mixed = jnp.dot(kh_ref[...], rhs, preferred_element_type=F32)
        mixed = mixed + jnp.dot(kl_ref[...], rhs, preferred_element_type=F32)
        for t in range(2):
            for g in range(group):
                image[(at + t) * group + g] = mixed[
                    g * size_x : (g + 1) * size_x, t * lanes : (t + 1) * lanes
                ]
        return carry

    lax.fori_loop(0, count // 2, one, 0)


def split_offset(offset):
    bits_y, bits_z = BOXY.bit_length() - 1, BOXZ.bit_length() - 1
    return offset >> (bits_y + bits_z), (offset >> bits_z) & (BOXY - 1), offset & (BOXZ - 1)


def pick_values(image, half, corner, offset):
    half_z, _, size_y = image.shape
    cols = offset.shape[-1]
    at_x, at_y, at_z = corner & 255, (corner >> 8) & 255, corner >> 16
    from_z = at_z - half * half_z
    first = jnp.clip(from_z, 0, half_z - BOXZ)
    off_x, off_y, off_z = split_offset(offset)
    cell_z = off_z + (from_z - first)
    wide = BESIDE * BOXY
    box_rows = BOXZ // BESIDE * BOXX
    box_row = (cell_z >> (BESIDE.bit_length() - 1)) * BOXX + off_x
    box_cell = (cell_z & (BESIDE - 1)) * BOXY + off_y
    box = image[pl.ds(first, BOXZ), pl.ds(at_x, BOXX), :]
    lane = lax.broadcasted_iota(jnp.int32, (BOXX, size_y), 1)
    groups = []
    for z in range(0, BOXZ, BESIDE):
        group = pltpu.roll(box[z], lax.rem(size_y - at_y, size_y), axis=1)
        for k in range(1, BESIDE):
            shift = lax.rem(size_y + k * BOXY - at_y, size_y)
            plane = pltpu.roll(box[z + k], shift, axis=1)
            group = jnp.where(lane >= k * BOXY, plane, group)
        groups.append(group[:, :wide])
    box = jnp.concatenate(groups, axis=0).astype(BF16)
    cell_line = lax.broadcasted_iota(jnp.int32, (wide, cols), 0)
    pick_cell = jnp.where(cell_line == box_cell, 1.0, 0.0).astype(BF16)
    lines = jnp.dot(box, pick_cell, preferred_element_type=F32)
    row_line = lax.broadcasted_iota(jnp.int32, (box_rows, cols), 0)
    line = jnp.where(row_line == box_row, lines, 0.0)
    return jnp.sum(line, axis=0, keepdims=True)


def pick_blocks(image, half, corner_ref, line, offsets_ref, base, values, first, count):
    unroll = min(UNROLL, count)

    def some(part, carry):
        for k in range(unroll):
            block = first + part * unroll + k
            values[pl.ds(block, 1), :] = pick_values(
                image, half, corner_ref[line, block], offsets_ref[pl.ds(base + block, 1), :]
            )
        return carry

    lax.fori_loop(0, count // unroll, some, 0)


def power_below(value):
    return 1 << (value.bit_length() - 1)


def two_parts(value):
    high = value.astype(BF16)
    return high, (value - high.astype(F32)).astype(BF16)


def dot_parts(left, right):
    (left_high, left_low), (right_high, right_low) = left, right
    small = lax.dot_general(left_high, right_low, NT, preferred_element_type=F32)
    small = small + lax.dot_general(left_low, right_high, NT, preferred_element_type=F32)
    return small + lax.dot_general(left_high, right_high, NT, preferred_element_type=F32)


def mix_planes(field_of, kern_y, kern_z, rows, planes_ref, slab):
    size_z = kern_z[0].shape[0]
    for x in range(slab):
        inner = dot_parts(kern_z, two_parts(field_of(x)))
        rows[pl.ds(x, size_z, stride=slab), :] = dot_parts(two_parts(inner), kern_y)
    planes_ref[...] = rows[...].astype(BF16).reshape(planes_ref.shape)


def planes_kernel(
    weights_ref,
    direction_ref,
    kern_x_ref,
    kern_y_ref,
    kern_z_ref,
    corner_ref,
    offsets_ref,
    out_u,
    out_d,
    kh_ref,
    kl_ref,
    packed_ref,
    offs_ref,
    rows,
    rows_d,
):
    slab = weights_ref.shape[0]
    kern_y, kern_z = two_parts(kern_y_ref[...]), two_parts(kern_z_ref[...])
    mix_planes(lambda x: weights_ref[x], kern_y, kern_z, rows, out_u, slab)
    mix_planes(lambda x: direction_ref[x], kern_y, kern_z, rows_d, out_d, slab)
    packed = corner_ref[0:1] + corner_ref[1:2] * 256 + corner_ref[2:3] * 65536
    packed_ref[...] = jnp.broadcast_to(packed, packed_ref.shape)
    offs_ref[...] = offsets_ref[...].astype(jnp.int16)
    size_x, wide = kern_x_ref.shape[0], kh_ref.shape[1]
    group = kh_ref.shape[0] // size_x
    pack = group * slab
    source = lax.broadcasted_iota(jnp.int32, (size_x, wide), 0)
    column = lax.broadcasted_iota(jnp.int32, (size_x, wide), 1)
    same = source == lax.div(column, pack) * slab + lax.rem(column, slab)
    layer = lax.div(lax.rem(column, pack), slab)
    for part, out_ref in zip(two_parts(kern_x_ref[...]), (kh_ref, kl_ref)):
        for g in range(group):
            select = jnp.where(same & (layer == g), 1.0, 0.0).astype(BF16)
            spot = jnp.dot(part, select, preferred_element_type=F32)
            out_ref[g * size_x : (g + 1) * size_x] = spot.astype(BF16)


def rank_blocks(corners, me, slab, ranks_ref, list_ref):
    devices, blocks = corners.shape
    from_x = (corners & 255) - me * slab
    touch = jnp.where((from_x < slab) & (from_x > -BOXX), 1.0, 0.0)
    earlier = lax.broadcasted_iota(jnp.int32, (blocks, blocks), 0)
    earlier = earlier < lax.broadcasted_iota(jnp.int32, (blocks, blocks), 1)
    within = jnp.dot(
        touch.astype(BF16), jnp.where(earlier, 1.0, 0.0).astype(BF16), preferred_element_type=F32
    )
    count = jnp.sum(touch, axis=1, keepdims=True)
    below = lax.broadcasted_iota(jnp.int32, (devices, devices), 1)
    below = below < lax.broadcasted_iota(jnp.int32, (devices, devices), 0)
    base = jnp.dot(
        jnp.where(below, 1.0, 0.0).astype(BF16),
        jnp.broadcast_to(count, (devices, blocks)).astype(BF16),
        preferred_element_type=F32,
    )
    ranks = jnp.where(touch > 0.0, base + within, -1.0)
    for device in range(devices):
        line = jnp.broadcast_to(ranks[device : device + 1], (blocks, blocks))
        ranks_ref[device] = jnp.transpose(line)
    total = jnp.sum(touch)
    list_ref[pl.ds(devices, 8), :] = jnp.full((8, blocks), total, F32).astype(jnp.int32)


def list_blocks(ranks_ref, list_ref, line):
    devices, blocks, _ = ranks_ref.shape
    wanted = lax.broadcasted_iota(jnp.int32, (blocks, blocks), 1) + line * blocks
    wanted = wanted.astype(F32)
    block = lax.broadcasted_iota(jnp.int32, (blocks, blocks), 0).astype(F32)

    def one(device, ids):
        hit = ranks_ref[device] == wanted
        start = (device * blocks).astype(F32)
        return ids + jnp.where(hit, block + start, 0.0)

    ids = lax.fori_loop(0, devices, one, jnp.zeros((blocks, blocks), F32))
    ids = jnp.sum(ids, axis=0, keepdims=True)
    list_ref[pl.ds(line, 1), :] = ids.astype(jnp.int32)


def log_sigmoid(value):
    return jnp.minimum(value, 0.0) - jnp.log1p(jnp.exp(-jnp.abs(value)))


def apply_interp(values, interp, outs, first, count):
    unroll = min(UNROLL, count)
    cols = values[0].shape[1]

    def some(part, carry):
        for k in range(unroll):
            block = first + part * unroll + k
            top = lax.broadcasted_iota(jnp.int32, (8, cols), 0)
            rows = jnp.broadcast_to(values[0][pl.ds(block, 1), :], (8, cols))
            for f in range(1, len(values)):
                rows = jnp.where(top == f, values[f][pl.ds(block, 1), :], rows)
            line = lax.dot_general(
                rows.astype(BF16), interp[block], NT, preferred_element_type=F32
            )
            for f, out_ref in enumerate(outs):
                out_ref[pl.ds(block, 1), :] = line[f : f + 1]
        return carry

    lax.fori_loop(0, count // unroll, some, 0)


def forward_kernel(
    group,
    trial_ref,
    accept_ref,
    own_u,
    own_d,
    packed_ref,
    offs_ref,
    kh_ref,
    kl_ref,
    offsets_ref,
    labels_ref,
    weights_ref,
    direction_ref,
    interp_ref,
    prob_ref,
    split_ref,
    list_ref,
    corners_ref,
    pair_packed,
    pair_offsets,
    all_offs,
    all_terms,
    buf_u,
    buf_d,
    all_packed,
    image_u,
    image_d,
    interp,
    mine_u,
    mine_d,
    theirs,
    out_u,
    out_d,
    in_u,
    in_d,
    mate_offs,
    rows_u,
    rows_d,
    mate_u,
    mate_d,
    latent_ref,
    slope_ref,
    res_ref,
    own_terms,
    weights_t,
    direction_t,
    ranks_ref,
    corner_smem,
    local_sem,
    mate_send,
    mate_recv,
    *sems,
):
    devices = buf_u.shape[0]
    blocks, per_block = labels_ref.shape
    slab, size_y, size_z = weights_ref.shape
    half_z, size_x, _ = image_u.shape
    place = Place(devices)
    load = pltpu.make_async_copy(interp_ref, interp, local_sem.at[0])
    load.start()
    u = Relay(place, own_u, buf_u, sems[0:4], halved=True)
    d = Relay(place, own_d, buf_d, sems[4:8], halved=True)
    o = Relay(place, offs_ref, all_offs, sems[8:12])
    t = Relay(place, own_terms, all_terms, sems[12:16])
    c = Relay(place, packed_ref, all_packed, sems[16:20])

    def swap(source, landing, k):
        return place.push(source, landing, mate_send.at[k], mate_recv.at[k], place.mate)

    swaps = [
        swap(offs_ref, mate_offs, 0),
        swap(out_u, in_u, 1),
        swap(out_d, in_d, 2),
        swap(rows_u, mate_u, 3),
        swap(rows_d, mate_d, 4),
    ]
    place.greet()
    for relay in (c, u, d, o):
        relay.keep_own()
    pair_offsets[pl.ds(0, blocks)] = offsets_ref[...]
    for x in range(slab):
        weights_t[pl.ds(x, size_z, stride=slab), :] = jnp.transpose(weights_ref[x])
        direction_t[pl.ds(x, size_z, stride=slab), :] = jnp.transpose(direction_ref[x])
    place.meet()
    c.start_own()
    u.start_own()
    swaps[0].start()

    def mixer(relay, image):
        return lambda piece: mix_depth(
            relay.buf, kh_ref, kl_ref, image, group, size_x, piece * relay.size, relay.size
        )

    u.run(mix=mixer(u, image_u), tail=d.start_own, riders=(c,))
    swaps[0].wait()
    pair_offsets[pl.ds(blocks, blocks)] = mate_offs[...].astype(jnp.int32)
    corners = all_packed[:, 0, :]
    corners_ref[...] = corners
    pair_packed[...] = jnp.concatenate([packed_ref[0:4], all_packed[place.mate, 0:4]], axis=0)
    rank_blocks(corners, place.me, slab, ranks_ref, list_ref)
    to_smem = pltpu.make_async_copy(pair_packed, corner_smem, local_sem.at[1])
    to_smem.start()
    to_smem.wait()
    steps = power_below(u.pieces + 2)
    some, lines = blocks // steps, -(-devices // steps)

    def pick(image, mine, first, count):
        line, base = (0, 0) if mine is not theirs else (4, blocks)
        pick_blocks(
            image, place.half, corner_smem, line, pair_offsets, base, mine, first, count
        )

    both = (half_z * slab, size_y)
    mate_rows = pl.ds(pl.multiple_of(place.mate * slab, slab), slab)

    def early(step):
        pick(image_u, theirs, step * some, some)
        pick(image_u, mine_u, step * some, some)
        for k in range(lines):
            list_blocks(ranks_ref, list_ref, step * lines + k)

        @pl.when(step == steps - 1)
        def _():
            out_u[...] = theirs[...].astype(BF16)
            rows_u[...] = image_u[:, mate_rows, :].reshape(both).astype(BF16)

    d.run(work=early, steps=steps, mix=mixer(d, image_d))
    swaps[1].start()
    pick(image_d, theirs, 0, blocks)
    out_d[...] = theirs[...].astype(BF16)
    rows_d[...] = image_d[:, mate_rows, :].reshape(both).astype(BF16)
    pick(image_d, mine_d, 0, blocks // 4)
    swaps[2].start()
    o.start_own()
    pick(image_d, mine_d, blocks // 4, blocks - blocks // 4)
    swaps[1].wait()
    mine_u[...] = mine_u[...] + in_u[...].astype(F32)
    load.wait()
    swaps[2].wait()
    swaps[3].start()
    swaps[4].start()
    mine_d[...] = mine_d[...] + in_d[...].astype(F32)
    target = labels_ref[...].astype(F32)
    part = blocks // 2
    unroll = min(UNROLL, part)

    def back(first):
        def one(step, carry):
            for k in range(unroll):
                block = first + step * unroll + k
                row = jnp.broadcast_to(res_ref[pl.ds(block, 1), :], (8, per_block))
                term = jnp.dot(row.astype(BF16), interp[block], preferred_element_type=F32)
                theirs[pl.ds(block, 1), :] = term[0:1]
            return carry

        lax.fori_loop(0, part // unroll, one, 0)

    for piece in range(2):
        rows = slice(piece * part, (piece + 1) * part)
        apply_interp((mine_u, mine_d), interp, (latent_ref, slope_ref), piece * part, part)
        if piece > 0:
            t.start_piece(0)
            o.line_events(0)
        prob = jax.nn.sigmoid(latent_ref[rows] + trial_ref[accept_ref[0]] * slope_ref[rows])
        prob_ref[rows] = prob
        res_ref[rows] = (target[rows] - prob).astype(BF16).astype(F32)
        back(piece * part)
        own_terms[rows] = theirs[rows].astype(BF16)
    o.side_events(0)
    t.keep_own()
    for relay in (c, u, d):
        relay.finish()
    t.start_piece(1)
    t.line_events(0)
    slope = slope_ref[...]
    latent = latent_ref[...]
    swaps[3].wait()
    swaps[4].wait()
    own_rows = pl.ds(pl.multiple_of(place.me * slab, slab), slab)
    here_z = pl.ds(pl.multiple_of(place.half * half_z * slab, slab), half_z * slab)
    there_z = pl.ds(pl.multiple_of((1 - place.half) * half_z * slab, slab), half_z * slab)

    def quad(field_t, image, mate):
        near = field_t[here_z] * image[:, own_rows, :].reshape(both)
        return jnp.sum(near + field_t[there_z] * mate[...].astype(F32))

    signed = 2.0 * target - 1.0
    line = lax.broadcasted_iota(jnp.int32, (8, 128), 0)
    lane = lax.broadcasted_iota(jnp.int32, (8, 128), 1)
    sums = jnp.zeros((8, 128), F32)
    for k in range(NTRIAL):
        at_trial = latent + trial_ref[k] * slope
        loglik = jnp.sum(log_sigmoid(signed * at_trial))
        descent = jnp.sum((target - jax.nn.sigmoid(at_trial)) * slope)
        sums = jnp.where((line == 0) & (lane == k), loglik, sums)
        sums = jnp.where((line == 1) & (lane == k), descent, sums)
    sums = jnp.where(line == 2, quad(weights_t, image_u, mate_u), sums)
    sums = jnp.where(line == 3, quad(direction_t, image_u, mate_u), sums)
    sums = jnp.where(line == 4, quad(direction_t, image_d, mate_d), sums)
    first = sums.astype(BF16).astype(F32)
    second = (sums - first).astype(BF16).astype(F32)
    third = sums - first - second
    split_ref[...] = jnp.concatenate([first, second, third], axis=0).astype(BF16)
    t.side_events(0)
    t.line_events(1)
    o.twin_events(0)
    t.side_events(1)
    t.twin_events(0)
    o.finish()
    t.twin_events(1)
    t.finish()


def bend_kernel(
    group,
    points,
    corner_smem,
    trial_ref,
    own_ref,
    split_ref,
    kh_ref,
    kl_ref,
    pair_offsets,
    prob_ref,
    interp_ref,
    out_ref,
    trials_ref,
    buf,
    all_split,
    image,
    interp,
    mine,
    theirs,
    sent,
    got,
    local_sem,
    mate_send,
    mate_recv,
    *sems,
):
    devices = buf.shape[0]
    blocks = prob_ref.shape[0]
    size_x = image.shape[1]
    place = Place(devices)
    load = pltpu.make_async_copy(interp_ref, interp, local_sem)
    load.start()
    b = Relay(place, own_ref, buf, sems[0:4], halved=True)
    s = Relay(place, split_ref, all_split, sems[4:8])
    swap = place.push(sent, got, mate_send, mate_recv, place.mate)
    place.greet()
    b.keep_own()
    s.keep_own()
    place.meet()
    s.start_own()
    b.start_own()
    b.run(
        mix=lambda piece: mix_depth(
            buf, kh_ref, kl_ref, image, group, size_x, piece * b.size, b.size
        ),
        riders=(s,),
    )

    def pick(line, base, values, first, count):
        pick_blocks(
            image, place.half, corner_smem, line, pair_offsets, base, values, first, count
        )

    pick(4, blocks, theirs, 0, blocks)
    sent[...] = theirs[...].astype(BF16)
    pick(0, 0, mine, 0, blocks // 4)
    swap.start()
    pick(0, 0, mine, blocks // 4, blocks - blocks // 4)
    total = jnp.sum(all_split[...].astype(F32), axis=0)
    total = total[0:8] + total[8:16] + total[16:24]
    lane = lax.broadcasted_iota(jnp.int32, (1, 128), 1)
    step = jnp.zeros((1, 128), F32)
    for k in range(NTRIAL):
        step = jnp.where(lane == k, trial_ref[k], step)
    loglik, descent, quad_gu, quad_du, quad_dv = (total[k : k + 1] for k in range(5))
    prior = 0.5 * (quad_gu + 2.0 * step * quad_du + step * step * quad_dv)
    trials_ref[0:1] = (loglik - prior) / points
    trials_ref[1:2] = (descent - quad_du - step * quad_dv) / points
    load.wait()
    swap.wait()
    mine[...] = mine[...] + got[...].astype(F32)
    apply_interp((mine,), interp, (out_ref,), 0, blocks)
    prob = prob_ref[...]
    out_ref[...] = prob * (1.0 - prob) * out_ref[...]
    b.finish()
    s.finish()


def spread_kernel(
    list_ref,
    corners_ref,
    trial_ref,
    accept_ref,
    offs_ref,
    terms_ref,
    weights_ref,
    direction_ref,
    kern_y_ref,
    kern_z_ref,
    new_ref,
    grad_ref,
    planes_ref,
    offs,
    terms,
    spread,
):
    devices, blocks, cols = offs_ref.shape
    slab, size_y, size_z = weights_ref.shape
    rows = BOXZ * slab
    unroll = UNROLL
    me = lax.axis_index("pts")
    spread[...] = jnp.zeros_like(spread)

    def widen(device, carry):
        offs[pl.ds(pl.multiple_of(device * blocks, blocks), blocks)] = offs_ref[device].astype(
            jnp.int32
        )
        terms[pl.ds(pl.multiple_of(device * blocks, blocks), blocks)] = terms_ref[device].astype(
            F32
        )
        return carry

    lax.fori_loop(0, devices, widen, 0)
    count = list_ref[devices, 0]

    def some(part, carry):
        sums = []
        for k in range(unroll):
            at = part * unroll + k
            block = list_ref[lax.div(at, blocks), lax.rem(at, blocks)]
            packed = corners_ref[lax.div(block, blocks), lax.rem(block, blocks)]
            from_x = jnp.where(at < count, (packed & 255) - me * slab, -2 * BOXX)
            at_y = (packed >> 8) & 255
            at_z = packed >> 16
            off_x, off_y, off_z = split_offset(offs[pl.ds(block, 1), :])
            cell = off_x + from_x
            key = jnp.where((cell >= 0) & (cell < slab), off_z * slab + cell, -1)
            row_line = lax.broadcasted_iota(jnp.int32, (rows, cols), 0)
            y_line = lax.broadcasted_iota(jnp.int32, (BOXY, cols), 0)
            left = jnp.where(row_line == key, terms[pl.ds(block, 1), :], 0.0).astype(BF16)
            right = jnp.where(y_line == off_y, 1.0, 0.0).astype(BF16)
            piece = lax.dot_general(left, right, NT, preferred_element_type=F32)
            piece = jnp.concatenate([piece, jnp.zeros((rows, size_y - BOXY), F32)], axis=1)
            sums.append((at_z, pltpu.roll(piece, at_y, axis=1)))
        for at_z, piece in sums:
            spread[pl.ds(pl.multiple_of(at_z * slab, slab), rows), :] += piece
        return carry

    lax.fori_loop(0, lax.div(count + unroll - 1, unroll), some, 0)
    chosen = trial_ref[accept_ref[0]]
    for x in range(slab):
        new = weights_ref[x] + chosen * direction_ref[x]
        new_ref[x] = new
        grad_ref[x] = jnp.transpose(spread[pl.ds(x, size_z, stride=slab), :]) - new
    kern_y, kern_z = two_parts(kern_y_ref[...]), two_parts(kern_z_ref[...])
    mix_planes(lambda x: grad_ref[x], kern_y, kern_z, spread, planes_ref, slab)


def body(
    grid_weights,
    direction,
    kern_x,
    kern_y,
    kern_z,
    interp,
    block_corner,
    block_offsets,
    labels,
    trial_steps,
    accept,
):
    slab, size_y, size_z = grid_weights.shape
    size_x = kern_x.shape[0]
    devices = lax.axis_size("pts")
    blocks, cols = block_offsets.shape
    per_block = interp.shape[1]
    points = blocks * per_block * devices
    group = max(1, PACK // slab)
    pack = group * slab
    units = size_z // group
    pieces = max(1, 64 // devices)

    smem = pl.BlockSpec(memory_space=pltpu.SMEM)
    vmem = pl.BlockSpec(memory_space=pltpu.VMEM)
    hbm = pl.BlockSpec(memory_space=pl.ANY)
    limit = dict(vmem_limit_bytes=VMEM_BYTES)
    planes_shape = jax.ShapeDtypeStruct((units, pack, size_y), BF16)
    rows_scratch = pltpu.VMEM((size_z * slab, size_y), F32)
    planes_scratch = pltpu.VMEM((devices, units // 2, pack, size_y), BF16)
    image_scratch = pltpu.VMEM((size_z // 2, size_x, size_y), F32)
    interp_scratch = pltpu.VMEM(interp.shape, BF16)
    point_scratch = pltpu.VMEM((blocks, per_block), F32)
    point_shape = jax.ShapeDtypeStruct((blocks, per_block), F32)

    wide_shape = jax.ShapeDtypeStruct((group * size_x, devices * pack), BF16)
    planes_w, planes_d, kern_high, kern_low, packed, offs = pl.pallas_call(
        planes_kernel,
        in_specs=[vmem] * 7,
        out_specs=[vmem] * 6,
        out_shape=[
            planes_shape,
            planes_shape,
            wide_shape,
            wide_shape,
            jax.ShapeDtypeStruct((8, blocks), jnp.int32),
            jax.ShapeDtypeStruct((blocks, cols), jnp.int16),
        ],
        scratch_shapes=[rows_scratch, rows_scratch],
        compiler_params=pltpu.CompilerParams(**limit),
        name="planes",
    )(grid_weights, direction, kern_x, kern_y, kern_z, block_corner, block_offsets)

    pick_scratch = pltpu.VMEM((blocks, cols), F32)
    swap_scratch = pltpu.VMEM((blocks, cols), BF16)
    mate_scratch = pltpu.VMEM((size_z // 2 * slab, size_y), BF16)
    probability, split, block_list, corners, pair_packed, pair_offsets, offsets, terms = (
        pl.pallas_call(
            functools.partial(forward_kernel, group),
            in_specs=[smem] * 2 + [vmem] * 10 + [hbm],
            out_specs=[vmem] * 8,
            out_shape=[
                point_shape,
                jax.ShapeDtypeStruct((24, 128), BF16),
                jax.ShapeDtypeStruct((devices + 8, blocks), jnp.int32),
                jax.ShapeDtypeStruct((devices, blocks), jnp.int32),
                jax.ShapeDtypeStruct((8, blocks), jnp.int32),
                jax.ShapeDtypeStruct((2 * blocks, cols), jnp.int32),
                jax.ShapeDtypeStruct((devices, blocks, cols), jnp.int16),
                jax.ShapeDtypeStruct((devices, blocks, cols), BF16),
            ],
            scratch_shapes=[
                planes_scratch,
                planes_scratch,
                pltpu.VMEM((devices, 8, blocks), jnp.int32),
                image_scratch,
                image_scratch,
                interp_scratch,
                pick_scratch,
                pick_scratch,
                pick_scratch,
                swap_scratch,
                swap_scratch,
                swap_scratch,
                swap_scratch,
                pltpu.VMEM((blocks, cols), jnp.int16),
                mate_scratch,
                mate_scratch,
                mate_scratch,
                mate_scratch,
                point_scratch,
                point_scratch,
                point_scratch,
                swap_scratch,
                rows_scratch,
                rows_scratch,
                pltpu.VMEM((devices, blocks, blocks), F32),
                pltpu.SMEM((8, blocks), jnp.int32),
                pltpu.SemaphoreType.DMA((2,)),
                pltpu.SemaphoreType.DMA((5,)),
                pltpu.SemaphoreType.DMA((5,)),
                *relay_sems(devices, pieces),
                *relay_sems(devices, pieces),
                *relay_sems(devices, 1),
                *relay_sems(devices, 2),
                *relay_sems(devices, 1),
            ],
            compiler_params=pltpu.CompilerParams(
                collective_id=0, has_side_effects=True, **limit
            ),
            name="forward",
        )(
            trial_steps,
            accept,
            planes_w,
            planes_d,
            packed,
            offs,
            kern_high,
            kern_low,
            block_offsets,
            labels,
            grid_weights,
            direction,
            interp,
        )
    )

    new_weights, grid_gradient, bend_planes = pl.pallas_call(
        spread_kernel,
        in_specs=[smem] * 4 + [vmem] * 6,
        out_specs=[vmem] * 3,
        out_shape=[
            jax.ShapeDtypeStruct(grid_weights.shape, F32),
            jax.ShapeDtypeStruct(grid_weights.shape, F32),
            planes_shape,
        ],
        scratch_shapes=[
            pltpu.VMEM((devices * blocks, cols), jnp.int32),
            pltpu.VMEM((devices * blocks, cols), F32),
            rows_scratch,
        ],
        compiler_params=pltpu.CompilerParams(**limit),
        name="spread",
    )(
        block_list,
        corners,
        trial_steps,
        accept,
        offsets,
        terms,
        grid_weights,
        direction,
        kern_y,
        kern_z,
    )

    curvature, trials = pl.pallas_call(
        functools.partial(bend_kernel, group, points),
        in_specs=[smem] * 2 + [vmem] * 6 + [hbm],
        out_specs=[vmem] * 2,
        out_shape=[point_shape, jax.ShapeDtypeStruct((2, 128), F32)],
        scratch_shapes=[
            planes_scratch,
            pltpu.VMEM((devices, 24, 128), BF16),
            image_scratch,
            interp_scratch,
            pick_scratch,
            pick_scratch,
            swap_scratch,
            swap_scratch,
            pltpu.SemaphoreType.DMA,
            pltpu.SemaphoreType.DMA,
            pltpu.SemaphoreType.DMA,
            *relay_sems(devices, pieces),
            *relay_sems(devices, 1),
        ],
        compiler_params=pltpu.CompilerParams(collective_id=1, has_side_effects=True, **limit),
        name="bend",
    )(
        pair_packed,
        trial_steps,
        bend_planes,
        split,
        kern_high,
        kern_low,
        pair_offsets,
        probability,
        interp,
    )
    return (new_weights, grid_gradient, curvature, trials[0, :NTRIAL], trials[1, :NTRIAL])


def solution(mesh):
    return jax.shard_map(
        body,
        mesh=mesh,
        in_specs=(
            P(("parts", "pts"), None, None),
            P(("parts", "pts"), None, None),
            P(),
            P(),
            P(),
            P(("parts", "pts"), None, None),
            P(None, ("parts", "pts")),
            P(("parts", "pts"), None),
            P(("parts", "pts"), None),
            P(),
            P(),
        ),
        out_specs=(
            P(("parts", "pts"), None, None),
            P(("parts", "pts"), None, None),
            P(("parts", "pts"), None),
            P("parts"),
            P("parts"),
        ),
        check_vma=False,
    )
```

```python
import functools

import jax
import jax.numpy as jnp
from jax import lax
from jax.experimental import pallas as pl
from jax.experimental.pallas import tpu as pltpu
from jax.sharding import PartitionSpec as P

BOXX = 16
BOXY = 16
BOXZ = 8
NTRIAL = 5
PACK = 16
BESIDE = 4
UNROLL = 32
VMEM_BYTES = 62 * 1024 * 1024

F32 = jnp.float32
BF16 = jnp.bfloat16
NT = (((1,), (1,)), ((), ()))
MESH = pl.DeviceIdType.MESH


class Place:
    def __init__(self, devices):
        me = lax.axis_index("pts")
        self.devices = devices
        self.depths = devices // 4
        self.me = me
        self.core = lax.rem(me, 2)
        self.side = lax.rem(lax.div(me, 2), 2)
        self.depth = lax.div(me, 4)
        self.half = lax.rem(self.depth, 2)
        self.beside = self.slot(self.depth, 1 - self.side, self.core)
        self.twin = self.slot(self.depth, self.side, 1 - self.core)
        self.mate = self.slot(self.depth + 1 - 2 * self.half, self.side, self.core)

    def slot(self, depth, side, core):
        return (depth * 2 + side) * 2 + core

    def along(self, depth):
        return self.slot(depth, self.side, self.core)

    def others(self, act):
        def one(far, carry):
            for way in (-1, 1):
                depth = self.depth + way * far

                @pl.when((depth >= 0) & (depth < self.depths))
                def _():
                    act(depth)

            return carry

        lax.fori_loop(1, self.depths, one, 0)

    def greet(self):
        barrier = pltpu.get_barrier_semaphore()

        def tell(device):
            pl.semaphore_signal(
                barrier, inc=1, device_id={"pts": device}, device_id_type=MESH
            )

        self.others(lambda depth: tell(self.along(depth)))
        tell(self.beside)
        tell(self.twin)

    def meet(self):
        pl.semaphore_wait(pltpu.get_barrier_semaphore(), self.depths + 1)

    def push(self, source, landing, send_sem, recv_sem, device):
        return pltpu.make_async_remote_copy(
            src_ref=source,
            dst_ref=landing,
            send_sem=send_sem,
            recv_sem=recv_sem,
            device_id={"pts": device},
            device_id_type=MESH,
        )


class Relay:
    def __init__(self, place, own, buf, sems, halved=False):
        self.place = place
        self.own = own
        self.buf = buf
        self.line_sem, self.side_sem, self.twin_sem, self.recv = sems
        self.pieces = self.recv.shape[1]
        self.size = buf.shape[1] // self.pieces
        self.halved = halved

    def own_rows(self, piece, depth):
        first = piece * self.size
        if self.halved:
            first = first + lax.rem(depth, 2) * self.buf.shape[1]
        return self.own.at[pl.ds(first, self.size)]

    def landing(self, slot, piece):
        return self.buf.at[slot, pl.ds(piece * self.size, self.size)]

    def line_copy(self, piece, depth):
        here = self.place
        return here.push(
            self.own_rows(piece, depth),
            self.landing(here.me, piece),
            self.line_sem.at[depth, piece],
            self.recv.at[here.me, piece],
            here.along(depth),
        )

    def side_copy(self, piece, depth, mine=False):
        here = self.place
        slot = here.along(depth)
        landing = self.landing(slot, piece)
        return here.push(
            self.own_rows(piece, depth) if mine else landing,
            landing,
            self.side_sem.at[depth, piece],
            self.recv.at[slot, piece],
            here.beside,
        )

    def twin_copy(self, piece, depth, side, mine=False):
        here = self.place
        slot = here.slot(depth, side, here.core)
        landing = self.landing(slot, piece)
        return here.push(
            self.own_rows(piece, depth) if mine else landing,
            landing,
            self.twin_sem.at[depth * 2 + side, piece],
            self.recv.at[slot, piece],
            here.twin,
        )

    def take(self, slot, piece):
        here = self.place
        landing = self.landing(slot, piece)
        here.push(
            landing, landing, self.twin_sem.at[0, piece], self.recv.at[slot, piece], here.twin
        ).wait_recv()

    def keep_own(self):
        here = self.place
        count = self.buf.shape[1]
        first = here.half * count if self.halved else 0
        self.buf[here.me] = self.own[pl.ds(first, count)]

    def start_lines(self):
        def one(piece, carry):
            self.place.others(lambda depth: self.line_copy(piece, depth).start())
            return carry

        lax.fori_loop(0, self.pieces, one, 0)

    def start_near(self, piece):
        here = self.place
        self.side_copy(piece, here.depth, mine=True).start()
        self.twin_copy(piece, here.depth, here.side, mine=True).start()

    def start_all_near(self):
        def one(piece, carry):
            self.start_near(piece)
            return carry

        lax.fori_loop(0, self.pieces, one, 0)

    def start_piece(self, piece):
        self.place.others(lambda depth: self.line_copy(piece, depth).start())
        self.start_near(piece)

    def start_own(self):
        def one(piece, carry):
            self.start_piece(piece)
            return carry

        lax.fori_loop(0, self.pieces, one, 0)

    def line_events(self, piece):
        here = self.place

        def one(depth):
            self.take(here.along(depth), piece)
            self.side_copy(piece, depth).start()
            self.twin_copy(piece, depth, here.side).start()

        here.others(one)

    def side_events(self, piece):
        here = self.place

        def one(depth):
            self.take(here.slot(depth, 1 - here.side, here.core), piece)
            self.twin_copy(piece, depth, 1 - here.side).start()

        one(here.depth)
        here.others(one)

    def twin_events(self, piece):
        here = self.place

        def one(pair, carry):
            self.take(pair * 2 + (1 - here.core), piece)
            return carry

        lax.fori_loop(0, here.devices // 2, one, 0)

    def run(self, work=None, steps=0, mix=None, tail=None, riders=()):
        pieces = self.pieces

        def one(wave, carry):
            for rider in riders:

                @pl.when(wave == 0)
                def _():
                    rider.line_events(0)

                @pl.when(wave == 1)
                def _():
                    rider.side_events(0)

                @pl.when(wave == 2)
                def _():
                    rider.twin_events(0)

            @pl.when(wave < pieces)
            def _():
                self.line_events(wave)

            if tail is not None:

                @pl.when(wave == pieces - 1)
                def _():
                    tail()

            @pl.when((wave >= 1) & (wave < pieces + 1))
            def _():
                self.side_events(wave - 1)

            if work is not None:

                @pl.when(wave < steps)
                def _():
                    work(wave)

            @pl.when(wave >= 2)
            def _():
                self.twin_events(wave - 2)
                if mix is not None:
                    mix(wave - 2)

            return carry

        lax.fori_loop(0, pieces + 2, one, 0)

    def finish(self):
        here = self.place

        def one(step, carry):
            piece = lax.div(step, here.depths)
            depth = lax.rem(step, here.depths)

            @pl.when(depth != here.depth)
            def _():
                self.line_copy(piece, depth).wait_send()

            self.side_copy(piece, depth).wait_send()
            self.twin_copy(piece, depth, 0).wait_send()
            self.twin_copy(piece, depth, 1).wait_send()
            return carry

        lax.fori_loop(0, self.pieces * here.depths, one, 0)


def relay_sems(devices, pieces):
    depths = devices // 4
    return [
        pltpu.SemaphoreType.DMA((depths, pieces)),
        pltpu.SemaphoreType.DMA((depths, pieces)),
        pltpu.SemaphoreType.DMA((depths * 2, pieces)),
        pltpu.SemaphoreType.DMA((devices, pieces)),
    ]


def mix_depth(planes_ref, kh_ref, kl_ref, image, group, size_x, first, count):
    devices, _, pack, lanes = planes_ref.shape

    def one(step, carry):
        at = first + step * 2
        pair = [planes_ref[:, at + t].reshape(devices * pack, lanes) for t in range(2)]
        rhs = jnp.concatenate(pair, axis=1)
        mixed = jnp.dot(kh_ref[...], rhs, preferred_element_type=F32)
        mixed = mixed + jnp.dot(kl_ref[...], rhs, preferred_element_type=F32)
        for t in range(2):
            for g in range(group):
                image[(at + t) * group + g] = mixed[
                    g * size_x : (g + 1) * size_x, t * lanes : (t + 1) * lanes
                ]
        return carry

    lax.fori_loop(0, count // 2, one, 0)


def split_offset(offset):
    bits_y, bits_z = BOXY.bit_length() - 1, BOXZ.bit_length() - 1
    return offset >> (bits_y + bits_z), (offset >> bits_z) & (BOXY - 1), offset & (BOXZ - 1)


def pick_values(image, half, corner, offset):
    half_z, _, size_y = image.shape
    cols = offset.shape[-1]
    at_x, at_y, at_z = corner & 255, (corner >> 8) & 255, corner >> 16
    from_z = at_z - half * half_z
    first = jnp.clip(from_z, 0, half_z - BOXZ)
    off_x, off_y, off_z = split_offset(offset)
    cell_z = off_z + (from_z - first)
    wide = BESIDE * BOXY
    box_rows = BOXZ // BESIDE * BOXX
    box_row = (cell_z >> (BESIDE.bit_length() - 1)) * BOXX + off_x
    box_cell = (cell_z & (BESIDE - 1)) * BOXY + off_y
    box = image[pl.ds(first, BOXZ), pl.ds(at_x, BOXX), :]
    lane = lax.broadcasted_iota(jnp.int32, (BOXX, size_y), 1)
    groups = []
    for z in range(0, BOXZ, BESIDE):
        group = pltpu.roll(box[z], lax.rem(size_y - at_y, size_y), axis=1)
        for k in range(1, BESIDE):
            shift = lax.rem(size_y + k * BOXY - at_y, size_y)
            plane = pltpu.roll(box[z + k], shift, axis=1)
            group = jnp.where(lane >= k * BOXY, plane, group)
        groups.append(group[:, :wide])
    box = jnp.concatenate(groups, axis=0).astype(BF16)
    cell_line = lax.broadcasted_iota(jnp.int32, (wide, cols), 0)
    pick_cell = jnp.where(cell_line == box_cell, 1.0, 0.0).astype(BF16)
    lines = jnp.dot(box, pick_cell, preferred_element_type=F32)
    row_line = lax.broadcasted_iota(jnp.int32, (box_rows, cols), 0)
    line = jnp.where(row_line == box_row, lines, 0.0)
    return jnp.sum(line, axis=0, keepdims=True)


def pick_blocks(image, half, corner_ref, line, offsets_ref, base, values, first, count):
    unroll = min(UNROLL, count)

    def some(part, carry):
        for k in range(unroll):
            block = first + part * unroll + k
            values[pl.ds(block, 1), :] = pick_values(
                image, half, corner_ref[line, block], offsets_ref[pl.ds(base + block, 1), :]
            )
        return carry

    lax.fori_loop(0, count // unroll, some, 0)


def power_below(value):
    return 1 << (value.bit_length() - 1)


def two_parts(value):
    high = value.astype(BF16)
    return high, (value - high.astype(F32)).astype(BF16)


def dot_parts(left, right):
    (left_high, left_low), (right_high, right_low) = left, right
    small = lax.dot_general(left_high, right_low, NT, preferred_element_type=F32)
    small = small + lax.dot_general(left_low, right_high, NT, preferred_element_type=F32)
    return small + lax.dot_general(left_high, right_high, NT, preferred_element_type=F32)


def mix_planes(field_of, kern_y, kern_z, rows, planes_ref, slab):
    size_z = kern_z[0].shape[0]
    for x in range(slab):
        inner = dot_parts(kern_z, two_parts(field_of(x)))
        rows[pl.ds(x, size_z, stride=slab), :] = dot_parts(two_parts(inner), kern_y)
    planes_ref[...] = rows[...].astype(BF16).reshape(planes_ref.shape)


def widen_kern(kern_x, slab, kh_ref, kl_ref):
    size_x, wide = kern_x.shape[0], kh_ref.shape[1]
    group = kh_ref.shape[0] // size_x
    pack = group * slab
    source = lax.broadcasted_iota(jnp.int32, (size_x, wide), 0)
    column = lax.broadcasted_iota(jnp.int32, (size_x, wide), 1)
    same = source == lax.div(column, pack) * slab + lax.rem(column, slab)
    layer = lax.div(lax.rem(column, pack), slab)
    for part, out_ref in zip(two_parts(kern_x), (kh_ref, kl_ref)):
        for g in range(group):
            select = jnp.where(same & (layer == g), 1.0, 0.0).astype(BF16)
            spot = jnp.dot(part, select, preferred_element_type=F32)
            out_ref[g * size_x : (g + 1) * size_x] = spot.astype(BF16)


def rank_blocks(corners, me, slab, ranks_ref, list_ref):
    devices, blocks = corners.shape
    from_x = (corners & 255) - me * slab
    touch = jnp.where((from_x < slab) & (from_x > -BOXX), 1.0, 0.0)
    earlier = lax.broadcasted_iota(jnp.int32, (blocks, blocks), 0)
    earlier = earlier < lax.broadcasted_iota(jnp.int32, (blocks, blocks), 1)
    within = jnp.dot(
        touch.astype(BF16), jnp.where(earlier, 1.0, 0.0).astype(BF16), preferred_element_type=F32
    )
    count = jnp.sum(touch, axis=1, keepdims=True)
    below = lax.broadcasted_iota(jnp.int32, (devices, devices), 1)
    below = below < lax.broadcasted_iota(jnp.int32, (devices, devices), 0)
    base = jnp.dot(
        jnp.where(below, 1.0, 0.0).astype(BF16),
        jnp.broadcast_to(count, (devices, blocks)).astype(BF16),
        preferred_element_type=F32,
    )
    ranks = jnp.where(touch > 0.0, base + within, -1.0)
    for device in range(devices):
        line = jnp.broadcast_to(ranks[device : device + 1], (blocks, blocks))
        ranks_ref[device] = jnp.transpose(line)
    total = jnp.sum(touch)
    list_ref[pl.ds(devices, 8), :] = jnp.full((8, blocks), total, F32).astype(jnp.int32)


def list_blocks(ranks_ref, list_ref, line):
    devices, blocks, _ = ranks_ref.shape
    wanted = lax.broadcasted_iota(jnp.int32, (blocks, blocks), 1) + line * blocks
    wanted = wanted.astype(F32)
    block = lax.broadcasted_iota(jnp.int32, (blocks, blocks), 0).astype(F32)

    def one(device, ids):
        hit = ranks_ref[device] == wanted
        start = (device * blocks).astype(F32)
        return ids + jnp.where(hit, block + start, 0.0)

    ids = lax.fori_loop(0, devices, one, jnp.zeros((blocks, blocks), F32))
    ids = jnp.sum(ids, axis=0, keepdims=True)
    list_ref[pl.ds(line, 1), :] = ids.astype(jnp.int32)


def log_sigmoid(value):
    return jnp.minimum(value, 0.0) - jnp.log1p(jnp.exp(-jnp.abs(value)))


def apply_interp(values, interp, outs, first, count):
    unroll = min(UNROLL, count)
    cols = values[0].shape[1]

    def some(part, carry):
        for k in range(unroll):
            block = first + part * unroll + k
            top = lax.broadcasted_iota(jnp.int32, (8, cols), 0)
            rows = jnp.broadcast_to(values[0][pl.ds(block, 1), :], (8, cols))
            for f in range(1, len(values)):
                rows = jnp.where(top == f, values[f][pl.ds(block, 1), :], rows)
            line = lax.dot_general(
                rows.astype(BF16), interp[block], NT, preferred_element_type=F32
            )
            for f, out_ref in enumerate(outs):
                out_ref[pl.ds(block, 1), :] = line[f : f + 1]
        return carry

    lax.fori_loop(0, count // unroll, some, 0)


def forward_kernel(
    group,
    trial_ref,
    accept_ref,
    corner_ref,
    offsets_ref,
    kern_x_ref,
    kern_y_ref,
    kern_z_ref,
    labels_ref,
    weights_ref,
    direction_ref,
    interp_ref,
    prob_ref,
    split_ref,
    list_ref,
    corners_ref,
    pair_packed,
    pair_offsets,
    all_offs,
    all_terms,
    kh_ref,
    kl_ref,
    own_u,
    own_d,
    packed_ref,
    offs_ref,
    buf_u,
    buf_d,
    all_packed,
    image_u,
    image_d,
    interp,
    mine_u,
    mine_d,
    theirs,
    out_u,
    out_d,
    in_u,
    in_d,
    mate_offs,
    rows_u,
    rows_d,
    mate_u,
    mate_d,
    latent_ref,
    slope_ref,
    res_ref,
    own_terms,
    weights_t,
    direction_t,
    ranks_ref,
    corner_smem,
    local_sem,
    mate_send,
    mate_recv,
    *sems,
):
    devices = buf_u.shape[0]
    blocks, per_block = labels_ref.shape
    slab, size_y, size_z = weights_ref.shape
    half_z, size_x, _ = image_u.shape
    place = Place(devices)
    place.greet()
    load = pltpu.make_async_copy(interp_ref, interp, local_sem.at[0])
    load.start()
    u = Relay(place, own_u, buf_u, sems[0:4], halved=True)
    d = Relay(place, own_d, buf_d, sems[4:8], halved=True)
    o = Relay(place, offs_ref, all_offs, sems[8:12])
    t = Relay(place, own_terms, all_terms, sems[12:16])
    c = Relay(place, packed_ref, all_packed, sems[16:20])

    def swap(source, landing, k):
        return place.push(source, landing, mate_send.at[k], mate_recv.at[k], place.mate)

    swaps = [
        swap(offs_ref, mate_offs, 0),
        swap(out_u, in_u, 1),
        swap(out_d, in_d, 2),
        swap(rows_u, mate_u, 3),
        swap(rows_d, mate_d, 4),
    ]
    kern_y, kern_z = two_parts(kern_y_ref[...]), two_parts(kern_z_ref[...])
    packed = corner_ref[0:1] + corner_ref[1:2] * 256 + corner_ref[2:3] * 65536
    packed_ref[...] = jnp.broadcast_to(packed, packed_ref.shape)
    offs_ref[...] = offsets_ref[...].astype(jnp.int16)
    mix_planes(lambda x: weights_ref[x], kern_y, kern_z, weights_t, own_u, slab)
    pair_offsets[pl.ds(0, blocks)] = offsets_ref[...]
    widen_kern(kern_x_ref[...], slab, kh_ref, kl_ref)
    place.meet()
    c.start_own()
    u.start_own()
    swaps[0].start()
    mix_planes(lambda x: direction_ref[x], kern_y, kern_z, direction_t, own_d, slab)
    for relay in (c, u, d, o):
        relay.keep_own()
    for x in range(slab):
        weights_t[pl.ds(x, size_z, stride=slab), :] = jnp.transpose(weights_ref[x])
        direction_t[pl.ds(x, size_z, stride=slab), :] = jnp.transpose(direction_ref[x])
    d.start_lines()
    o.start_lines()

    def mixer(relay, image):
        return lambda piece: mix_depth(
            relay.buf, kh_ref, kl_ref, image, group, size_x, piece * relay.size, relay.size
        )

    u.run(mix=mixer(u, image_u), tail=d.start_all_near, riders=(c,))
    swaps[0].wait()
    pair_offsets[pl.ds(blocks, blocks)] = mate_offs[...].astype(jnp.int32)
    corners = all_packed[:, 0, :]
    corners_ref[...] = corners
    pair_packed[...] = jnp.concatenate([packed_ref[0:4], all_packed[place.mate, 0:4]], axis=0)
    rank_blocks(corners, place.me, slab, ranks_ref, list_ref)
    to_smem = pltpu.make_async_copy(pair_packed, corner_smem, local_sem.at[1])
    to_smem.start()
    to_smem.wait()
    steps = power_below(u.pieces + 2)
    some, lines = blocks // steps, -(-devices // steps)

    def pick(image, mine, first, count):
        line, base = (0, 0) if mine is not theirs else (4, blocks)
        pick_blocks(
            image, place.half, corner_smem, line, pair_offsets, base, mine, first, count
        )

    both = (half_z * slab, size_y)
    mate_rows = pl.ds(pl.multiple_of(place.mate * slab, slab), slab)

    def early(step):
        pick(image_u, theirs, step * some, some)
        pick(image_u, mine_u, step * some, some)
        for k in range(lines):
            list_blocks(ranks_ref, list_ref, step * lines + k)

        @pl.when(step == steps - 1)
        def _():
            out_u[...] = theirs[...].astype(BF16)
            rows_u[...] = image_u[:, mate_rows, :].reshape(both).astype(BF16)

    d.run(work=early, steps=steps, mix=mixer(d, image_d), tail=o.start_all_near)
    swaps[1].start()
    pick(image_d, theirs, 0, blocks)
    out_d[...] = theirs[...].astype(BF16)
    rows_d[...] = image_d[:, mate_rows, :].reshape(both).astype(BF16)
    pick(image_d, mine_d, 0, blocks // 4)
    swaps[2].start()
    o.line_events(0)
    pick(image_d, mine_d, blocks // 4, blocks - blocks // 4)
    swaps[1].wait()
    mine_u[...] = mine_u[...] + in_u[...].astype(F32)
    load.wait()
    swaps[2].wait()
    swaps[3].start()
    swaps[4].start()
    mine_d[...] = mine_d[...] + in_d[...].astype(F32)
    target = labels_ref[...].astype(F32)
    part = blocks // 2
    unroll = min(UNROLL, part)

    def back(first):
        def one(step, carry):
            for k in range(unroll):
                block = first + step * unroll + k
                row = jnp.broadcast_to(res_ref[pl.ds(block, 1), :], (8, per_block))
                term = jnp.dot(row.astype(BF16), interp[block], preferred_element_type=F32)
                theirs[pl.ds(block, 1), :] = term[0:1]
            return carry

        lax.fori_loop(0, part // unroll, one, 0)

    for piece in range(2):
        rows = slice(piece * part, (piece + 1) * part)
        apply_interp((mine_u, mine_d), interp, (latent_ref, slope_ref), piece * part, part)
        if piece > 0:
            t.start_piece(0)
            o.side_events(0)
        prob = jax.nn.sigmoid(latent_ref[rows] + trial_ref[accept_ref[0]] * slope_ref[rows])
        prob_ref[rows] = prob
        res_ref[rows] = (target[rows] - prob).astype(BF16).astype(F32)
        back(piece * part)
        own_terms[rows] = theirs[rows].astype(BF16)
    t.keep_own()
    for relay in (c, u, d):
        relay.finish()
    t.start_piece(1)
    t.line_events(0)
    slope = slope_ref[...]
    latent = latent_ref[...]
    swaps[3].wait()
    swaps[4].wait()
    own_rows = pl.ds(pl.multiple_of(place.me * slab, slab), slab)
    here_z = pl.ds(pl.multiple_of(place.half * half_z * slab, slab), half_z * slab)
    there_z = pl.ds(pl.multiple_of((1 - place.half) * half_z * slab, slab), half_z * slab)

    def quad(field_t, image, mate):
        near = field_t[here_z] * image[:, own_rows, :].reshape(both)
        return jnp.sum(near + field_t[there_z] * mate[...].astype(F32))

    signed = 2.0 * target - 1.0
    line = lax.broadcasted_iota(jnp.int32, (8, 128), 0)
    lane = lax.broadcasted_iota(jnp.int32, (8, 128), 1)
    sums = jnp.zeros((8, 128), F32)
    for k in range(NTRIAL):
        at_trial = latent + trial_ref[k] * slope
        loglik = jnp.sum(log_sigmoid(signed * at_trial))
        descent = jnp.sum((target - jax.nn.sigmoid(at_trial)) * slope)
        sums = jnp.where((line == 0) & (lane == k), loglik, sums)
        sums = jnp.where((line == 1) & (lane == k), descent, sums)
    sums = jnp.where(line == 2, quad(weights_t, image_u, mate_u), sums)
    sums = jnp.where(line == 3, quad(direction_t, image_u, mate_u), sums)
    sums = jnp.where(line == 4, quad(direction_t, image_d, mate_d), sums)
    first = sums.astype(BF16).astype(F32)
    second = (sums - first).astype(BF16).astype(F32)
    third = sums - first - second
    split_ref[...] = jnp.concatenate([first, second, third], axis=0).astype(BF16)
    t.side_events(0)
    t.line_events(1)
    o.twin_events(0)
    t.side_events(1)
    t.twin_events(0)
    o.finish()
    t.twin_events(1)
    t.finish()


def bend_kernel(
    group,
    points,
    corner_smem,
    trial_ref,
    own_ref,
    split_ref,
    kh_ref,
    kl_ref,
    pair_offsets,
    prob_ref,
    interp_ref,
    out_ref,
    trials_ref,
    buf,
    all_split,
    image,
    interp,
    mine,
    theirs,
    sent,
    got,
    local_sem,
    mate_send,
    mate_recv,
    *sems,
):
    devices = buf.shape[0]
    blocks = prob_ref.shape[0]
    size_x = image.shape[1]
    place = Place(devices)
    load = pltpu.make_async_copy(interp_ref, interp, local_sem)
    load.start()
    b = Relay(place, own_ref, buf, sems[0:4], halved=True)
    s = Relay(place, split_ref, all_split, sems[4:8])
    swap = place.push(sent, got, mate_send, mate_recv, place.mate)
    place.greet()
    b.keep_own()
    s.keep_own()
    place.meet()
    s.start_own()
    b.start_own()
    b.run(
        mix=lambda piece: mix_depth(
            buf, kh_ref, kl_ref, image, group, size_x, piece * b.size, b.size
        ),
        riders=(s,),
    )

    def pick(line, base, values, first, count):
        pick_blocks(
            image, place.half, corner_smem, line, pair_offsets, base, values, first, count
        )

    pick(4, blocks, theirs, 0, blocks)
    sent[...] = theirs[...].astype(BF16)
    pick(0, 0, mine, 0, blocks // 4)
    swap.start()
    pick(0, 0, mine, blocks // 4, blocks - blocks // 4)
    total = jnp.sum(all_split[...].astype(F32), axis=0)
    total = total[0:8] + total[8:16] + total[16:24]
    lane = lax.broadcasted_iota(jnp.int32, (1, 128), 1)
    step = jnp.zeros((1, 128), F32)
    for k in range(NTRIAL):
        step = jnp.where(lane == k, trial_ref[k], step)
    loglik, descent, quad_gu, quad_du, quad_dv = (total[k : k + 1] for k in range(5))
    prior = 0.5 * (quad_gu + 2.0 * step * quad_du + step * step * quad_dv)
    trials_ref[0:1] = (loglik - prior) / points
    trials_ref[1:2] = (descent - quad_du - step * quad_dv) / points
    load.wait()
    swap.wait()
    mine[...] = mine[...] + got[...].astype(F32)
    apply_interp((mine,), interp, (out_ref,), 0, blocks)
    prob = prob_ref[...]
    out_ref[...] = prob * (1.0 - prob) * out_ref[...]
    b.finish()
    s.finish()


def spread_kernel(
    list_ref,
    corners_ref,
    trial_ref,
    accept_ref,
    offs_ref,
    terms_ref,
    weights_ref,
    direction_ref,
    kern_y_ref,
    kern_z_ref,
    new_ref,
    grad_ref,
    planes_ref,
    offs,
    terms,
    spread,
):
    devices, blocks, cols = offs_ref.shape
    slab, size_y, size_z = weights_ref.shape
    rows = BOXZ * slab
    unroll = UNROLL
    me = lax.axis_index("pts")
    spread[...] = jnp.zeros_like(spread)

    def widen(device, carry):
        offs[pl.ds(pl.multiple_of(device * blocks, blocks), blocks)] = offs_ref[device].astype(
            jnp.int32
        )
        terms[pl.ds(pl.multiple_of(device * blocks, blocks), blocks)] = terms_ref[device].astype(
            F32
        )
        return carry

    lax.fori_loop(0, devices, widen, 0)
    count = list_ref[devices, 0]

    def some(part, carry):
        sums = []
        for k in range(unroll):
            at = part * unroll + k
            block = list_ref[lax.div(at, blocks), lax.rem(at, blocks)]
            packed = corners_ref[lax.div(block, blocks), lax.rem(block, blocks)]
            from_x = jnp.where(at < count, (packed & 255) - me * slab, -2 * BOXX)
            at_y = (packed >> 8) & 255
            at_z = packed >> 16
            off_x, off_y, off_z = split_offset(offs[pl.ds(block, 1), :])
            cell = off_x + from_x
            key = jnp.where((cell >= 0) & (cell < slab), off_z * slab + cell, -1)
            row_line = lax.broadcasted_iota(jnp.int32, (rows, cols), 0)
            y_line = lax.broadcasted_iota(jnp.int32, (BOXY, cols), 0)
            left = jnp.where(row_line == key, terms[pl.ds(block, 1), :], 0.0).astype(BF16)
            right = jnp.where(y_line == off_y, 1.0, 0.0).astype(BF16)
            piece = lax.dot_general(left, right, NT, preferred_element_type=F32)
            piece = jnp.concatenate([piece, jnp.zeros((rows, size_y - BOXY), F32)], axis=1)
            sums.append((at_z, pltpu.roll(piece, at_y, axis=1)))
        for at_z, piece in sums:
            spread[pl.ds(pl.multiple_of(at_z * slab, slab), rows), :] += piece
        return carry

    lax.fori_loop(0, lax.div(count + unroll - 1, unroll), some, 0)
    chosen = trial_ref[accept_ref[0]]
    for x in range(slab):
        new = weights_ref[x] + chosen * direction_ref[x]
        new_ref[x] = new
        grad_ref[x] = jnp.transpose(spread[pl.ds(x, size_z, stride=slab), :]) - new
    kern_y, kern_z = two_parts(kern_y_ref[...]), two_parts(kern_z_ref[...])
    mix_planes(lambda x: grad_ref[x], kern_y, kern_z, spread, planes_ref, slab)


def body(
    grid_weights,
    direction,
    kern_x,
    kern_y,
    kern_z,
    interp,
    block_corner,
    block_offsets,
    labels,
    trial_steps,
    accept,
):
    slab, size_y, size_z = grid_weights.shape
    size_x = kern_x.shape[0]
    devices = lax.axis_size("pts")
    blocks, cols = block_offsets.shape
    per_block = interp.shape[1]
    points = blocks * per_block * devices
    group = max(1, PACK // slab)
    pack = group * slab
    units = size_z // group
    pieces = max(1, 64 // devices)

    smem = pl.BlockSpec(memory_space=pltpu.SMEM)
    vmem = pl.BlockSpec(memory_space=pltpu.VMEM)
    hbm = pl.BlockSpec(memory_space=pl.ANY)
    limit = dict(vmem_limit_bytes=VMEM_BYTES)
    planes_shape = jax.ShapeDtypeStruct((units, pack, size_y), BF16)
    rows_scratch = pltpu.VMEM((size_z * slab, size_y), F32)
    planes_scratch = pltpu.VMEM((devices, units // 2, pack, size_y), BF16)
    image_scratch = pltpu.VMEM((size_z // 2, size_x, size_y), F32)
    interp_scratch = pltpu.VMEM(interp.shape, BF16)
    point_scratch = pltpu.VMEM((blocks, per_block), F32)
    point_shape = jax.ShapeDtypeStruct((blocks, per_block), F32)

    wide_shape = jax.ShapeDtypeStruct((group * size_x, devices * pack), BF16)
    chunk_scratch = pltpu.VMEM((units, pack, size_y), BF16)
    pick_scratch = pltpu.VMEM((blocks, cols), F32)
    swap_scratch = pltpu.VMEM((blocks, cols), BF16)
    mate_scratch = pltpu.VMEM((size_z // 2 * slab, size_y), BF16)
    (
        probability,
        split,
        block_list,
        corners,
        pair_packed,
        pair_offsets,
        offsets,
        terms,
        kern_high,
        kern_low,
    ) = (
        pl.pallas_call(
            functools.partial(forward_kernel, group),
            in_specs=[smem] * 2 + [vmem] * 8 + [hbm],
            out_specs=[vmem] * 10,
            out_shape=[
                point_shape,
                jax.ShapeDtypeStruct((24, 128), BF16),
                jax.ShapeDtypeStruct((devices + 8, blocks), jnp.int32),
                jax.ShapeDtypeStruct((devices, blocks), jnp.int32),
                jax.ShapeDtypeStruct((8, blocks), jnp.int32),
                jax.ShapeDtypeStruct((2 * blocks, cols), jnp.int32),
                jax.ShapeDtypeStruct((devices, blocks, cols), jnp.int16),
                jax.ShapeDtypeStruct((devices, blocks, cols), BF16),
                wide_shape,
                wide_shape,
            ],
            scratch_shapes=[
                chunk_scratch,
                chunk_scratch,
                pltpu.VMEM((8, blocks), jnp.int32),
                pltpu.VMEM((blocks, cols), jnp.int16),
                planes_scratch,
                planes_scratch,
                pltpu.VMEM((devices, 8, blocks), jnp.int32),
                image_scratch,
                image_scratch,
                interp_scratch,
                pick_scratch,
                pick_scratch,
                pick_scratch,
                swap_scratch,
                swap_scratch,
                swap_scratch,
                swap_scratch,
                pltpu.VMEM((blocks, cols), jnp.int16),
                mate_scratch,
                mate_scratch,
                mate_scratch,
                mate_scratch,
                point_scratch,
                point_scratch,
                point_scratch,
                swap_scratch,
                rows_scratch,
                rows_scratch,
                pltpu.VMEM((devices, blocks, blocks), F32),
                pltpu.SMEM((8, blocks), jnp.int32),
                pltpu.SemaphoreType.DMA((2,)),
                pltpu.SemaphoreType.DMA((5,)),
                pltpu.SemaphoreType.DMA((5,)),
                *relay_sems(devices, pieces),
                *relay_sems(devices, pieces),
                *relay_sems(devices, 1),
                *relay_sems(devices, 2),
                *relay_sems(devices, 1),
            ],
            compiler_params=pltpu.CompilerParams(
                collective_id=0, has_side_effects=True, **limit
            ),
            name="forward",
        )(
            trial_steps,
            accept,
            block_corner,
            block_offsets,
            kern_x,
            kern_y,
            kern_z,
            labels,
            grid_weights,
            direction,
            interp,
        )
    )

    new_weights, grid_gradient, bend_planes = pl.pallas_call(
        spread_kernel,
        in_specs=[smem] * 4 + [vmem] * 6,
        out_specs=[vmem] * 3,
        out_shape=[
            jax.ShapeDtypeStruct(grid_weights.shape, F32),
            jax.ShapeDtypeStruct(grid_weights.shape, F32),
            planes_shape,
        ],
        scratch_shapes=[
            pltpu.VMEM((devices * blocks, cols), jnp.int32),
            pltpu.VMEM((devices * blocks, cols), F32),
            rows_scratch,
        ],
        compiler_params=pltpu.CompilerParams(**limit),
        name="spread",
    )(
        block_list,
        corners,
        trial_steps,
        accept,
        offsets,
        terms,
        grid_weights,
        direction,
        kern_y,
        kern_z,
    )

    curvature, trials = pl.pallas_call(
        functools.partial(bend_kernel, group, points),
        in_specs=[smem] * 2 + [vmem] * 6 + [hbm],
        out_specs=[vmem] * 2,
        out_shape=[point_shape, jax.ShapeDtypeStruct((2, 128), F32)],
        scratch_shapes=[
            planes_scratch,
            pltpu.VMEM((devices, 24, 128), BF16),
            image_scratch,
            interp_scratch,
            pick_scratch,
            pick_scratch,
            swap_scratch,
            swap_scratch,
            pltpu.SemaphoreType.DMA,
            pltpu.SemaphoreType.DMA,
            pltpu.SemaphoreType.DMA,
            *relay_sems(devices, pieces),
            *relay_sems(devices, 1),
        ],
        compiler_params=pltpu.CompilerParams(collective_id=1, has_side_effects=True, **limit),
        name="bend",
    )(
        pair_packed,
        trial_steps,
        bend_planes,
        split,
        kern_high,
        kern_low,
        pair_offsets,
        probability,
        interp,
    )
    return (new_weights, grid_gradient, curvature, trials[0, :NTRIAL], trials[1, :NTRIAL])


def solution(mesh):
    return jax.shard_map(
        body,
        mesh=mesh,
        in_specs=(
            P(("parts", "pts"), None, None),
            P(("parts", "pts"), None, None),
            P(),
            P(),
            P(),
            P(("parts", "pts"), None, None),
            P(None, ("parts", "pts")),
            P(("parts", "pts"), None),
            P(("parts", "pts"), None),
            P(),
            P(),
        ),
        out_specs=(
            P(("parts", "pts"), None, None),
            P(("parts", "pts"), None, None),
            P(("parts", "pts"), None),
            P("parts"),
            P("parts"),
        ),
        check_vma=False,
    )
```

```python
import functools

import jax
import jax.numpy as jnp
from jax import lax
from jax.experimental import pallas as pl
from jax.experimental.pallas import tpu as pltpu
from jax.sharding import PartitionSpec as P

BOXX = 16
BOXY = 16
BOXZ = 8
NTRIAL = 5
PACK = 16
BESIDE = 4
UNROLL = 32
VMEM_BYTES = 62 * 1024 * 1024

F32 = jnp.float32
BF16 = jnp.bfloat16
NT = (((1,), (1,)), ((), ()))
MESH = pl.DeviceIdType.MESH


class Place:
    def __init__(self, devices):
        me = lax.axis_index("pts")
        self.devices = devices
        self.depths = devices // 4
        self.me = me
        self.core = lax.rem(me, 2)
        self.side = lax.rem(lax.div(me, 2), 2)
        self.depth = lax.div(me, 4)
        self.half = lax.rem(self.depth, 2)
        self.beside = self.slot(self.depth, 1 - self.side, self.core)
        self.twin = self.slot(self.depth, self.side, 1 - self.core)
        self.mate = self.slot(self.depth + 1 - 2 * self.half, self.side, self.core)

    def slot(self, depth, side, core):
        return (depth * 2 + side) * 2 + core

    def along(self, depth):
        return self.slot(depth, self.side, self.core)

    def others(self, act):
        def one(far, carry):
            for way in (-1, 1):
                depth = self.depth + way * far

                @pl.when((depth >= 0) & (depth < self.depths))
                def _():
                    act(depth)

            return carry

        lax.fori_loop(1, self.depths, one, 0)

    def greet(self):
        barrier = pltpu.get_barrier_semaphore()

        def tell(device):
            pl.semaphore_signal(
                barrier, inc=1, device_id={"pts": device}, device_id_type=MESH
            )

        self.others(lambda depth: tell(self.along(depth)))
        tell(self.beside)
        tell(self.twin)

    def meet(self):
        pl.semaphore_wait(pltpu.get_barrier_semaphore(), self.depths + 1)

    def push(self, source, landing, send_sem, recv_sem, device):
        return pltpu.make_async_remote_copy(
            src_ref=source,
            dst_ref=landing,
            send_sem=send_sem,
            recv_sem=recv_sem,
            device_id={"pts": device},
            device_id_type=MESH,
        )


class Relay:
    def __init__(self, place, own, buf, sems, halved=False):
        self.place = place
        self.own = own
        self.buf = buf
        self.line_sem, self.side_sem, self.twin_sem, self.recv = sems
        self.pieces = self.recv.shape[1]
        self.size = buf.shape[1] // self.pieces
        self.halved = halved

    def own_rows(self, piece, depth):
        first = piece * self.size
        if self.halved:
            first = first + lax.rem(depth, 2) * self.buf.shape[1]
        return self.own.at[pl.ds(first, self.size)]

    def landing(self, slot, piece):
        return self.buf.at[slot, pl.ds(piece * self.size, self.size)]

    def line_copy(self, piece, depth):
        here = self.place
        return here.push(
            self.own_rows(piece, depth),
            self.landing(here.me, piece),
            self.line_sem.at[depth, piece],
            self.recv.at[here.me, piece],
            here.along(depth),
        )

    def side_copy(self, piece, depth, mine=False):
        here = self.place
        slot = here.along(depth)
        landing = self.landing(slot, piece)
        return here.push(
            self.own_rows(piece, depth) if mine else landing,
            landing,
            self.side_sem.at[depth, piece],
            self.recv.at[slot, piece],
            here.beside,
        )

    def twin_copy(self, piece, depth, side, mine=False):
        here = self.place
        slot = here.slot(depth, side, here.core)
        landing = self.landing(slot, piece)
        return here.push(
            self.own_rows(piece, depth) if mine else landing,
            landing,
            self.twin_sem.at[depth * 2 + side, piece],
            self.recv.at[slot, piece],
            here.twin,
        )

    def take(self, slot, piece):
        here = self.place
        landing = self.landing(slot, piece)
        here.push(
            landing, landing, self.twin_sem.at[0, piece], self.recv.at[slot, piece], here.twin
        ).wait_recv()

    def keep_own(self):
        here = self.place
        count = self.buf.shape[1]
        first = here.half * count if self.halved else 0
        self.buf[here.me] = self.own[pl.ds(first, count)]

    def start_lines(self):
        def one(piece, carry):
            self.place.others(lambda depth: self.line_copy(piece, depth).start())
            return carry

        lax.fori_loop(0, self.pieces, one, 0)

    def start_near(self, piece):
        here = self.place
        self.side_copy(piece, here.depth, mine=True).start()
        self.twin_copy(piece, here.depth, here.side, mine=True).start()

    def start_all_near(self):
        def one(piece, carry):
            self.start_near(piece)
            return carry

        lax.fori_loop(0, self.pieces, one, 0)

    def start_piece(self, piece):
        self.place.others(lambda depth: self.line_copy(piece, depth).start())
        self.start_near(piece)

    def start_own(self):
        def one(piece, carry):
            self.start_piece(piece)
            return carry

        lax.fori_loop(0, self.pieces, one, 0)

    def line_events(self, piece):
        here = self.place

        def one(depth):
            self.take(here.along(depth), piece)
            self.side_copy(piece, depth).start()
            self.twin_copy(piece, depth, here.side).start()

        here.others(one)

    def side_events(self, piece):
        here = self.place

        def one(depth):
            self.take(here.slot(depth, 1 - here.side, here.core), piece)
            self.twin_copy(piece, depth, 1 - here.side).start()

        one(here.depth)
        here.others(one)

    def twin_events(self, piece):
        here = self.place

        def one(pair, carry):
            self.take(pair * 2 + (1 - here.core), piece)
            return carry

        lax.fori_loop(0, here.devices // 2, one, 0)

    def head(self, wave):
        @pl.when(wave < self.pieces)
        def _():
            self.line_events(wave)

        @pl.when(wave == 1)
        def _():
            self.side_events(0)

    def run(self, first=0, work=None, steps=0, mix=None, tail=None, riders=(), follow=None):
        pieces = self.pieces

        def one(wave, carry):
            for rider in riders:

                @pl.when(wave == 0)
                def _():
                    rider.line_events(0)

                @pl.when(wave == 1)
                def _():
                    rider.side_events(0)

                @pl.when(wave == 2)
                def _():
                    rider.twin_events(0)

            @pl.when(wave < pieces)
            def _():
                self.line_events(wave)

            if tail is not None:

                @pl.when(wave == max(first, pieces - 1))
                def _():
                    tail()

            @pl.when((wave >= 1) & (wave < pieces + 1))
            def _():
                self.side_events(wave - 1)

            if follow is not None:

                @pl.when(wave >= pieces)
                def _():
                    follow.head(wave - pieces)

            if work is not None:

                @pl.when(wave - first < steps)
                def _():
                    work(wave - first)

            @pl.when(wave >= 2)
            def _():
                self.twin_events(wave - 2)
                if mix is not None:
                    mix(wave - 2)

            return carry

        lax.fori_loop(first, pieces + 2, one, 0)

    def finish(self):
        here = self.place

        def one(step, carry):
            piece = lax.div(step, here.depths)
            depth = lax.rem(step, here.depths)

            @pl.when(depth != here.depth)
            def _():
                self.line_copy(piece, depth).wait_send()

            self.side_copy(piece, depth).wait_send()
            self.twin_copy(piece, depth, 0).wait_send()
            self.twin_copy(piece, depth, 1).wait_send()
            return carry

        lax.fori_loop(0, self.pieces * here.depths, one, 0)


def relay_sems(devices, pieces):
    depths = devices // 4
    return [
        pltpu.SemaphoreType.DMA((depths, pieces)),
        pltpu.SemaphoreType.DMA((depths, pieces)),
        pltpu.SemaphoreType.DMA((depths * 2, pieces)),
        pltpu.SemaphoreType.DMA((devices, pieces)),
    ]


def mix_depth(planes_ref, kh_ref, kl_ref, image, group, size_x, first, count):
    devices, _, pack, lanes = planes_ref.shape

    def one(step, carry):
        at = first + step * 2
        pair = [planes_ref[:, at + t].reshape(devices * pack, lanes) for t in range(2)]
        rhs = jnp.concatenate(pair, axis=1)
        mixed = jnp.dot(kh_ref[...], rhs, preferred_element_type=F32)
        mixed = mixed + jnp.dot(kl_ref[...], rhs, preferred_element_type=F32)
        for t in range(2):
            for g in range(group):
                image[(at + t) * group + g] = mixed[
                    g * size_x : (g + 1) * size_x, t * lanes : (t + 1) * lanes
                ]
        return carry

    lax.fori_loop(0, count // 2, one, 0)


def split_offset(offset):
    bits_y, bits_z = BOXY.bit_length() - 1, BOXZ.bit_length() - 1
    return offset >> (bits_y + bits_z), (offset >> bits_z) & (BOXY - 1), offset & (BOXZ - 1)


def pick_values(image, half, corner, offset):
    half_z, _, size_y = image.shape
    cols = offset.shape[-1]
    at_x, at_y, at_z = corner & 255, (corner >> 8) & 255, corner >> 16
    from_z = at_z - half * half_z
    first = jnp.clip(from_z, 0, half_z - BOXZ)
    off_x, off_y, off_z = split_offset(offset)
    cell_z = off_z + (from_z - first)
    wide = BESIDE * BOXY
    box_rows = BOXZ // BESIDE * BOXX
    box_row = (cell_z >> (BESIDE.bit_length() - 1)) * BOXX + off_x
    box_cell = (cell_z & (BESIDE - 1)) * BOXY + off_y
    box = image[pl.ds(first, BOXZ), pl.ds(at_x, BOXX), :]
    lane = lax.broadcasted_iota(jnp.int32, (BOXX, size_y), 1)
    groups = []
    for z in range(0, BOXZ, BESIDE):
        group = pltpu.roll(box[z], lax.rem(size_y - at_y, size_y), axis=1)
        for k in range(1, BESIDE):
            shift = lax.rem(size_y + k * BOXY - at_y, size_y)
            plane = pltpu.roll(box[z + k], shift, axis=1)
            group = jnp.where(lane >= k * BOXY, plane, group)
        groups.append(group[:, :wide])
    box = jnp.concatenate(groups, axis=0).astype(BF16)
    cell_line = lax.broadcasted_iota(jnp.int32, (wide, cols), 0)
    pick_cell = jnp.where(cell_line == box_cell, 1.0, 0.0).astype(BF16)
    lines = jnp.dot(box, pick_cell, preferred_element_type=F32)
    row_line = lax.broadcasted_iota(jnp.int32, (box_rows, cols), 0)
    line = jnp.where(row_line == box_row, lines, 0.0)
    return jnp.sum(line, axis=0, keepdims=True)


def pick_blocks(image, half, corner_ref, line, offsets_ref, base, values, first, count):
    unroll = min(UNROLL, count)

    def some(part, carry):
        for k in range(unroll):
            block = first + part * unroll + k
            values[pl.ds(block, 1), :] = pick_values(
                image, half, corner_ref[line, block], offsets_ref[pl.ds(base + block, 1), :]
            )
        return carry

    lax.fori_loop(0, count // unroll, some, 0)


def power_below(value):
    return 1 << (value.bit_length() - 1)


def two_parts(value):
    high = value.astype(BF16)
    return high, (value - high.astype(F32)).astype(BF16)


def dot_parts(left, right):
    (left_high, left_low), (right_high, right_low) = left, right
    small = lax.dot_general(left_high, right_low, NT, preferred_element_type=F32)
    small = small + lax.dot_general(left_low, right_high, NT, preferred_element_type=F32)
    return small + lax.dot_general(left_high, right_high, NT, preferred_element_type=F32)


def mix_planes(field_of, kern_y, kern_z, rows, planes_ref, slab):
    size_z = kern_z[0].shape[0]
    for x in range(slab):
        inner = dot_parts(kern_z, two_parts(field_of(x)))
        rows[pl.ds(x, size_z, stride=slab), :] = dot_parts(two_parts(inner), kern_y)
    planes_ref[...] = rows[...].astype(BF16).reshape(planes_ref.shape)


def widen_kern(kern_x, slab, kh_ref, kl_ref):
    size_x, wide = kern_x.shape[0], kh_ref.shape[1]
    group = kh_ref.shape[0] // size_x
    pack = group * slab
    source = lax.broadcasted_iota(jnp.int32, (size_x, wide), 0)
    column = lax.broadcasted_iota(jnp.int32, (size_x, wide), 1)
    same = source == lax.div(column, pack) * slab + lax.rem(column, slab)
    layer = lax.div(lax.rem(column, pack), slab)
    for part, out_ref in zip(two_parts(kern_x), (kh_ref, kl_ref)):
        for g in range(group):
            select = jnp.where(same & (layer == g), 1.0, 0.0).astype(BF16)
            spot = jnp.dot(part, select, preferred_element_type=F32)
            out_ref[g * size_x : (g + 1) * size_x] = spot.astype(BF16)


def rank_blocks(corners, me, slab, ranks_ref, list_ref):
    devices, blocks = corners.shape
    from_x = (corners & 255) - me * slab
    touch = jnp.where((from_x < slab) & (from_x > -BOXX), 1.0, 0.0)
    earlier = lax.broadcasted_iota(jnp.int32, (blocks, blocks), 0)
    earlier = earlier < lax.broadcasted_iota(jnp.int32, (blocks, blocks), 1)
    within = jnp.dot(
        touch.astype(BF16), jnp.where(earlier, 1.0, 0.0).astype(BF16), preferred_element_type=F32
    )
    count = jnp.sum(touch, axis=1, keepdims=True)
    below = lax.broadcasted_iota(jnp.int32, (devices, devices), 1)
    below = below < lax.broadcasted_iota(jnp.int32, (devices, devices), 0)
    base = jnp.dot(
        jnp.where(below, 1.0, 0.0).astype(BF16),
        jnp.broadcast_to(count, (devices, blocks)).astype(BF16),
        preferred_element_type=F32,
    )
    ranks = jnp.where(touch > 0.0, base + within, -1.0)
    for device in range(devices):
        line = jnp.broadcast_to(ranks[device : device + 1], (blocks, blocks))
        ranks_ref[device] = jnp.transpose(line)
    total = jnp.sum(touch)
    list_ref[pl.ds(devices, 8), :] = jnp.full((8, blocks), total, F32).astype(jnp.int32)


def list_blocks(ranks_ref, list_ref, line):
    devices, blocks, _ = ranks_ref.shape
    wanted = lax.broadcasted_iota(jnp.int32, (blocks, blocks), 1) + line * blocks
    wanted = wanted.astype(F32)
    block = lax.broadcasted_iota(jnp.int32, (blocks, blocks), 0).astype(F32)

    def one(device, ids):
        hit = ranks_ref[device] == wanted
        start = (device * blocks).astype(F32)
        return ids + jnp.where(hit, block + start, 0.0)

    ids = lax.fori_loop(0, devices, one, jnp.zeros((blocks, blocks), F32))
    ids = jnp.sum(ids, axis=0, keepdims=True)
    list_ref[pl.ds(line, 1), :] = ids.astype(jnp.int32)


def log_sigmoid(value):
    return jnp.minimum(value, 0.0) - jnp.log1p(jnp.exp(-jnp.abs(value)))


def apply_interp(values, interp, outs, first, count):
    unroll = min(UNROLL, count)
    cols = values[0].shape[1]

    def some(part, carry):
        for k in range(unroll):
            block = first + part * unroll + k
            top = lax.broadcasted_iota(jnp.int32, (8, cols), 0)
            rows = jnp.broadcast_to(values[0][pl.ds(block, 1), :], (8, cols))
            for f in range(1, len(values)):
                rows = jnp.where(top == f, values[f][pl.ds(block, 1), :], rows)
            line = lax.dot_general(
                rows.astype(BF16), interp[block], NT, preferred_element_type=F32
            )
            for f, out_ref in enumerate(outs):
                out_ref[pl.ds(block, 1), :] = line[f : f + 1]
        return carry

    lax.fori_loop(0, count // unroll, some, 0)


def forward_kernel(
    group,
    trial_ref,
    accept_ref,
    corner_ref,
    offsets_ref,
    kern_x_ref,
    kern_y_ref,
    kern_z_ref,
    labels_ref,
    weights_ref,
    direction_ref,
    interp_ref,
    prob_ref,
    split_ref,
    list_ref,
    corners_ref,
    pair_packed,
    pair_offsets,
    all_offs,
    all_terms,
    kh_ref,
    kl_ref,
    own_u,
    own_d,
    packed_ref,
    offs_ref,
    buf_u,
    buf_d,
    all_packed,
    image_u,
    image_d,
    interp,
    mine_u,
    mine_d,
    theirs,
    out_u,
    out_d,
    in_u,
    in_d,
    mate_offs,
    rows_u,
    rows_d,
    mate_u,
    mate_d,
    latent_ref,
    slope_ref,
    res_ref,
    own_terms,
    weights_t,
    direction_t,
    ranks_ref,
    corner_smem,
    local_sem,
    mate_send,
    mate_recv,
    *sems,
):
    devices = buf_u.shape[0]
    blocks, per_block = labels_ref.shape
    slab, size_y, size_z = weights_ref.shape
    half_z, size_x, _ = image_u.shape
    place = Place(devices)
    place.greet()
    load = pltpu.make_async_copy(interp_ref, interp, local_sem.at[0])
    load.start()
    u = Relay(place, own_u, buf_u, sems[0:4], halved=True)
    d = Relay(place, own_d, buf_d, sems[4:8], halved=True)
    o = Relay(place, offs_ref, all_offs, sems[8:12])
    t = Relay(place, own_terms, all_terms, sems[12:16])
    c = Relay(place, packed_ref, all_packed, sems[16:20])

    def swap(source, landing, k):
        return place.push(source, landing, mate_send.at[k], mate_recv.at[k], place.mate)

    swaps = [
        swap(offs_ref, mate_offs, 0),
        swap(out_u, in_u, 1),
        swap(out_d, in_d, 2),
        swap(rows_u, mate_u, 3),
        swap(rows_d, mate_d, 4),
    ]
    kern_y, kern_z = two_parts(kern_y_ref[...]), two_parts(kern_z_ref[...])
    packed = corner_ref[0:1] + corner_ref[1:2] * 256 + corner_ref[2:3] * 65536
    packed_ref[...] = jnp.broadcast_to(packed, packed_ref.shape)
    offs_ref[...] = offsets_ref[...].astype(jnp.int16)
    mix_planes(lambda x: weights_ref[x], kern_y, kern_z, weights_t, own_u, slab)
    pair_offsets[pl.ds(0, blocks)] = offsets_ref[...]
    widen_kern(kern_x_ref[...], slab, kh_ref, kl_ref)
    place.meet()
    c.start_own()
    u.start_own()
    swaps[0].start()
    mix_planes(lambda x: direction_ref[x], kern_y, kern_z, direction_t, own_d, slab)
    for relay in (c, u, d, o):
        relay.keep_own()
    for x in range(slab):
        weights_t[pl.ds(x, size_z, stride=slab), :] = jnp.transpose(weights_ref[x])
        direction_t[pl.ds(x, size_z, stride=slab), :] = jnp.transpose(direction_ref[x])
    d.start_lines()
    o.start_lines()

    def mixer(relay, image):
        return lambda piece: mix_depth(
            relay.buf, kh_ref, kl_ref, image, group, size_x, piece * relay.size, relay.size
        )

    last = u.pieces + 1
    to_smem = pltpu.make_async_copy(pair_packed, corner_smem, local_sem.at[1])

    def list_lines(first, count):
        def one(line, carry):
            list_blocks(ranks_ref, list_ref, line)
            return carry

        lax.fori_loop(first, first + count, one, 0)

    def prepare(wave):
        @pl.when(wave == 2)
        def _():
            corners = all_packed[:, 0, :]
            corners_ref[...] = corners
            pair_packed[...] = jnp.concatenate(
                [packed_ref[0:4], all_packed[place.mate, 0:4]], axis=0
            )
            rank_blocks(corners, place.me, slab, ranks_ref, list_ref)
            to_smem.start()

        for k in range(2):

            @pl.when(wave == min(3 + k, last))
            def _():
                list_lines(devices // 2 * k, devices // 2)

    u.run(
        work=prepare,
        steps=last + 1,
        mix=mixer(u, image_u),
        tail=d.start_all_near,
        riders=(c,),
        follow=d,
    )
    swaps[0].wait()
    pair_offsets[pl.ds(blocks, blocks)] = mate_offs[...].astype(jnp.int32)
    to_smem.wait()
    steps = power_below(u.pieces)
    some = blocks // steps

    def pick(image, mine, first, count):
        line, base = (0, 0) if mine is not theirs else (4, blocks)
        pick_blocks(
            image, place.half, corner_smem, line, pair_offsets, base, mine, first, count
        )

    both = (half_z * slab, size_y)
    mate_rows = pl.ds(pl.multiple_of(place.mate * slab, slab), slab)

    def early(step):
        pick(image_u, theirs, step * some, some)
        pick(image_u, mine_u, step * some, some)

        @pl.when(step == steps - 1)
        def _():
            out_u[...] = theirs[...].astype(BF16)
            rows_u[...] = image_u[:, mate_rows, :].reshape(both).astype(BF16)

    d.run(first=2, work=early, steps=steps, mix=mixer(d, image_d), tail=o.start_all_near)
    swaps[1].start()
    pick(image_d, theirs, 0, blocks)
    out_d[...] = theirs[...].astype(BF16)
    rows_d[...] = image_d[:, mate_rows, :].reshape(both).astype(BF16)
    pick(image_d, mine_d, 0, blocks // 4)
    for k in (2, 3, 4):
        swaps[k].start()
    o.line_events(0)
    pick(image_d, mine_d, blocks // 4, blocks - blocks // 4)
    swaps[1].wait()
    mine_u[...] = mine_u[...] + in_u[...].astype(F32)
    load.wait()
    swaps[2].wait()
    mine_d[...] = mine_d[...] + in_d[...].astype(F32)
    target = labels_ref[...].astype(F32)
    part = blocks // 2
    unroll = min(UNROLL, part)

    def back(first):
        def one(step, carry):
            for k in range(unroll):
                block = first + step * unroll + k
                row = jnp.broadcast_to(res_ref[pl.ds(block, 1), :], (8, per_block))
                term = jnp.dot(row.astype(BF16), interp[block], preferred_element_type=F32)
                theirs[pl.ds(block, 1), :] = term[0:1]
            return carry

        lax.fori_loop(0, part // unroll, one, 0)

    for piece in range(2):
        rows = slice(piece * part, (piece + 1) * part)
        apply_interp((mine_u, mine_d), interp, (latent_ref, slope_ref), piece * part, part)
        if piece > 0:
            t.start_piece(0)
            o.side_events(0)
        prob = jax.nn.sigmoid(latent_ref[rows] + trial_ref[accept_ref[0]] * slope_ref[rows])
        prob_ref[rows] = prob
        res_ref[rows] = (target[rows] - prob).astype(BF16).astype(F32)
        back(piece * part)
        own_terms[rows] = theirs[rows].astype(BF16)
    t.keep_own()
    for relay in (c, u, d):
        relay.finish()
    t.start_piece(1)
    t.line_events(0)
    slope = slope_ref[...]
    latent = latent_ref[...]
    swaps[3].wait()
    swaps[4].wait()
    own_rows = pl.ds(pl.multiple_of(place.me * slab, slab), slab)
    here_z = pl.ds(pl.multiple_of(place.half * half_z * slab, slab), half_z * slab)
    there_z = pl.ds(pl.multiple_of((1 - place.half) * half_z * slab, slab), half_z * slab)

    def quad(field_t, image, mate):
        near = field_t[here_z] * image[:, own_rows, :].reshape(both)
        return jnp.sum(near + field_t[there_z] * mate[...].astype(F32))

    signed = 2.0 * target - 1.0
    line = lax.broadcasted_iota(jnp.int32, (8, 128), 0)
    lane = lax.broadcasted_iota(jnp.int32, (8, 128), 1)
    sums = jnp.zeros((8, 128), F32)
    for k in range(NTRIAL):
        at_trial = latent + trial_ref[k] * slope
        loglik = jnp.sum(log_sigmoid(signed * at_trial))
        descent = jnp.sum((target - jax.nn.sigmoid(at_trial)) * slope)
        sums = jnp.where((line == 0) & (lane == k), loglik, sums)
        sums = jnp.where((line == 1) & (lane == k), descent, sums)
    sums = jnp.where(line == 2, quad(weights_t, image_u, mate_u), sums)
    sums = jnp.where(line == 3, quad(direction_t, image_u, mate_u), sums)
    sums = jnp.where(line == 4, quad(direction_t, image_d, mate_d), sums)
    first = sums.astype(BF16).astype(F32)
    second = (sums - first).astype(BF16).astype(F32)
    third = sums - first - second
    split_ref[...] = jnp.concatenate([first, second, third], axis=0).astype(BF16)
    t.side_events(0)
    t.line_events(1)
    o.twin_events(0)
    t.side_events(1)
    t.twin_events(0)
    o.finish()
    t.twin_events(1)
    t.finish()


def bend_kernel(
    group,
    points,
    corner_smem,
    trial_ref,
    own_ref,
    split_ref,
    kh_ref,
    kl_ref,
    pair_offsets,
    prob_ref,
    interp_ref,
    out_ref,
    trials_ref,
    buf,
    all_split,
    image,
    interp,
    mine,
    theirs,
    sent,
    got,
    local_sem,
    mate_send,
    mate_recv,
    *sems,
):
    devices = buf.shape[0]
    blocks = prob_ref.shape[0]
    size_x = image.shape[1]
    place = Place(devices)
    load = pltpu.make_async_copy(interp_ref, interp, local_sem)
    load.start()
    b = Relay(place, own_ref, buf, sems[0:4], halved=True)
    s = Relay(place, split_ref, all_split, sems[4:8])
    swap = place.push(sent, got, mate_send, mate_recv, place.mate)
    place.greet()
    b.keep_own()
    s.keep_own()
    place.meet()
    s.start_own()
    b.start_own()
    b.run(
        mix=lambda piece: mix_depth(
            buf, kh_ref, kl_ref, image, group, size_x, piece * b.size, b.size
        ),
        riders=(s,),
    )

    def pick(line, base, values, first, count):
        pick_blocks(
            image, place.half, corner_smem, line, pair_offsets, base, values, first, count
        )

    pick(4, blocks, theirs, 0, blocks)
    sent[...] = theirs[...].astype(BF16)
    pick(0, 0, mine, 0, blocks // 4)
    swap.start()
    pick(0, 0, mine, blocks // 4, blocks - blocks // 4)
    total = jnp.sum(all_split[...].astype(F32), axis=0)
    total = total[0:8] + total[8:16] + total[16:24]
    lane = lax.broadcasted_iota(jnp.int32, (1, 128), 1)
    step = jnp.zeros((1, 128), F32)
    for k in range(NTRIAL):
        step = jnp.where(lane == k, trial_ref[k], step)
    loglik, descent, quad_gu, quad_du, quad_dv = (total[k : k + 1] for k in range(5))
    prior = 0.5 * (quad_gu + 2.0 * step * quad_du + step * step * quad_dv)
    trials_ref[0:1] = (loglik - prior) / points
    trials_ref[1:2] = (descent - quad_du - step * quad_dv) / points
    load.wait()
    swap.wait()
    mine[...] = mine[...] + got[...].astype(F32)
    apply_interp((mine,), interp, (out_ref,), 0, blocks)
    prob = prob_ref[...]
    out_ref[...] = prob * (1.0 - prob) * out_ref[...]
    b.finish()
    s.finish()


def spread_kernel(
    list_ref,
    corners_ref,
    trial_ref,
    accept_ref,
    offs_ref,
    terms_ref,
    weights_ref,
    direction_ref,
    kern_y_ref,
    kern_z_ref,
    new_ref,
    grad_ref,
    planes_ref,
    offs,
    terms,
    spread,
):
    devices, blocks, cols = offs_ref.shape
    slab, size_y, size_z = weights_ref.shape
    rows = BOXZ * slab
    unroll = UNROLL
    me = lax.axis_index("pts")
    spread[...] = jnp.zeros_like(spread)

    def widen(device, carry):
        offs[pl.ds(pl.multiple_of(device * blocks, blocks), blocks)] = offs_ref[device].astype(
            jnp.int32
        )
        terms[pl.ds(pl.multiple_of(device * blocks, blocks), blocks)] = terms_ref[device].astype(
            F32
        )
        return carry

    lax.fori_loop(0, devices, widen, 0)
    count = list_ref[devices, 0]

    def some(part, carry):
        sums = []
        for k in range(unroll):
            at = part * unroll + k
            block = list_ref[lax.div(at, blocks), lax.rem(at, blocks)]
            packed = corners_ref[lax.div(block, blocks), lax.rem(block, blocks)]
            from_x = jnp.where(at < count, (packed & 255) - me * slab, -2 * BOXX)
            at_y = (packed >> 8) & 255
            at_z = packed >> 16
            off_x, off_y, off_z = split_offset(offs[pl.ds(block, 1), :])
            cell = off_x + from_x
            key = jnp.where((cell >= 0) & (cell < slab), off_z * slab + cell, -1)
            row_line = lax.broadcasted_iota(jnp.int32, (rows, cols), 0)
            y_line = lax.broadcasted_iota(jnp.int32, (BOXY, cols), 0)
            left = jnp.where(row_line == key, terms[pl.ds(block, 1), :], 0.0).astype(BF16)
            right = jnp.where(y_line == off_y, 1.0, 0.0).astype(BF16)
            piece = lax.dot_general(left, right, NT, preferred_element_type=F32)
            piece = jnp.concatenate([piece, jnp.zeros((rows, size_y - BOXY), F32)], axis=1)
            sums.append((at_z, pltpu.roll(piece, at_y, axis=1)))
        for at_z, piece in sums:
            spread[pl.ds(pl.multiple_of(at_z * slab, slab), rows), :] += piece
        return carry

    lax.fori_loop(0, lax.div(count + unroll - 1, unroll), some, 0)
    chosen = trial_ref[accept_ref[0]]
    for x in range(slab):
        new = weights_ref[x] + chosen * direction_ref[x]
        new_ref[x] = new
        grad_ref[x] = jnp.transpose(spread[pl.ds(x, size_z, stride=slab), :]) - new
    kern_y, kern_z = two_parts(kern_y_ref[...]), two_parts(kern_z_ref[...])
    mix_planes(lambda x: grad_ref[x], kern_y, kern_z, spread, planes_ref, slab)


def body(
    grid_weights,
    direction,
    kern_x,
    kern_y,
    kern_z,
    interp,
    block_corner,
    block_offsets,
    labels,
    trial_steps,
    accept,
):
    slab, size_y, size_z = grid_weights.shape
    size_x = kern_x.shape[0]
    devices = lax.axis_size("pts")
    blocks, cols = block_offsets.shape
    per_block = interp.shape[1]
    points = blocks * per_block * devices
    group = max(1, PACK // slab)
    pack = group * slab
    units = size_z // group
    pieces = max(1, 64 // devices)

    smem = pl.BlockSpec(memory_space=pltpu.SMEM)
    vmem = pl.BlockSpec(memory_space=pltpu.VMEM)
    hbm = pl.BlockSpec(memory_space=pl.ANY)
    limit = dict(vmem_limit_bytes=VMEM_BYTES)
    planes_shape = jax.ShapeDtypeStruct((units, pack, size_y), BF16)
    rows_scratch = pltpu.VMEM((size_z * slab, size_y), F32)
    planes_scratch = pltpu.VMEM((devices, units // 2, pack, size_y), BF16)
    image_scratch = pltpu.VMEM((size_z // 2, size_x, size_y), F32)
    interp_scratch = pltpu.VMEM(interp.shape, BF16)
    point_scratch = pltpu.VMEM((blocks, per_block), F32)
    point_shape = jax.ShapeDtypeStruct((blocks, per_block), F32)

    wide_shape = jax.ShapeDtypeStruct((group * size_x, devices * pack), BF16)
    chunk_scratch = pltpu.VMEM((units, pack, size_y), BF16)
    pick_scratch = pltpu.VMEM((blocks, cols), F32)
    swap_scratch = pltpu.VMEM((blocks, cols), BF16)
    mate_scratch = pltpu.VMEM((size_z // 2 * slab, size_y), BF16)
    (
        probability,
        split,
        block_list,
        corners,
        pair_packed,
        pair_offsets,
        offsets,
        terms,
        kern_high,
        kern_low,
    ) = (
        pl.pallas_call(
            functools.partial(forward_kernel, group),
            in_specs=[smem] * 2 + [vmem] * 8 + [hbm],
            out_specs=[vmem] * 10,
            out_shape=[
                point_shape,
                jax.ShapeDtypeStruct((24, 128), BF16),
                jax.ShapeDtypeStruct((devices + 8, blocks), jnp.int32),
                jax.ShapeDtypeStruct((devices, blocks), jnp.int32),
                jax.ShapeDtypeStruct((8, blocks), jnp.int32),
                jax.ShapeDtypeStruct((2 * blocks, cols), jnp.int32),
                jax.ShapeDtypeStruct((devices, blocks, cols), jnp.int16),
                jax.ShapeDtypeStruct((devices, blocks, cols), BF16),
                wide_shape,
                wide_shape,
            ],
            scratch_shapes=[
                chunk_scratch,
                chunk_scratch,
                pltpu.VMEM((8, blocks), jnp.int32),
                pltpu.VMEM((blocks, cols), jnp.int16),
                planes_scratch,
                planes_scratch,
                pltpu.VMEM((devices, 8, blocks), jnp.int32),
                image_scratch,
                image_scratch,
                interp_scratch,
                pick_scratch,
                pick_scratch,
                pick_scratch,
                swap_scratch,
                swap_scratch,
                swap_scratch,
                swap_scratch,
                pltpu.VMEM((blocks, cols), jnp.int16),
                mate_scratch,
                mate_scratch,
                mate_scratch,
                mate_scratch,
                point_scratch,
                point_scratch,
                point_scratch,
                swap_scratch,
                rows_scratch,
                rows_scratch,
                pltpu.VMEM((devices, blocks, blocks), F32),
                pltpu.SMEM((8, blocks), jnp.int32),
                pltpu.SemaphoreType.DMA((2,)),
                pltpu.SemaphoreType.DMA((5,)),
                pltpu.SemaphoreType.DMA((5,)),
                *relay_sems(devices, pieces),
                *relay_sems(devices, pieces),
                *relay_sems(devices, 1),
                *relay_sems(devices, 2),
                *relay_sems(devices, 1),
            ],
            compiler_params=pltpu.CompilerParams(
                collective_id=0, has_side_effects=True, **limit
            ),
            name="forward",
        )(
            trial_steps,
            accept,
            block_corner,
            block_offsets,
            kern_x,
            kern_y,
            kern_z,
            labels,
            grid_weights,
            direction,
            interp,
        )
    )

    new_weights, grid_gradient, bend_planes = pl.pallas_call(
        spread_kernel,
        in_specs=[smem] * 4 + [vmem] * 6,
        out_specs=[vmem] * 3,
        out_shape=[
            jax.ShapeDtypeStruct(grid_weights.shape, F32),
            jax.ShapeDtypeStruct(grid_weights.shape, F32),
            planes_shape,
        ],
        scratch_shapes=[
            pltpu.VMEM((devices * blocks, cols), jnp.int32),
            pltpu.VMEM((devices * blocks, cols), F32),
            rows_scratch,
        ],
        compiler_params=pltpu.CompilerParams(**limit),
        name="spread",
    )(
        block_list,
        corners,
        trial_steps,
        accept,
        offsets,
        terms,
        grid_weights,
        direction,
        kern_y,
        kern_z,
    )

    curvature, trials = pl.pallas_call(
        functools.partial(bend_kernel, group, points),
        in_specs=[smem] * 2 + [vmem] * 6 + [hbm],
        out_specs=[vmem] * 2,
        out_shape=[point_shape, jax.ShapeDtypeStruct((2, 128), F32)],
        scratch_shapes=[
            planes_scratch,
            pltpu.VMEM((devices, 24, 128), BF16),
            image_scratch,
            interp_scratch,
            pick_scratch,
            pick_scratch,
            swap_scratch,
            swap_scratch,
            pltpu.SemaphoreType.DMA,
            pltpu.SemaphoreType.DMA,
            pltpu.SemaphoreType.DMA,
            *relay_sems(devices, pieces),
            *relay_sems(devices, 1),
        ],
        compiler_params=pltpu.CompilerParams(collective_id=1, has_side_effects=True, **limit),
        name="bend",
    )(
        pair_packed,
        trial_steps,
        bend_planes,
        split,
        kern_high,
        kern_low,
        pair_offsets,
        probability,
        interp,
    )
    return (new_weights, grid_gradient, curvature, trials[0, :NTRIAL], trials[1, :NTRIAL])


def solution(mesh):
    return jax.shard_map(
        body,
        mesh=mesh,
        in_specs=(
            P(("parts", "pts"), None, None),
            P(("parts", "pts"), None, None),
            P(),
            P(),
            P(),
            P(("parts", "pts"), None, None),
            P(None, ("parts", "pts")),
            P(("parts", "pts"), None),
            P(("parts", "pts"), None),
            P(),
            P(),
        ),
        out_specs=(
            P(("parts", "pts"), None, None),
            P(("parts", "pts"), None, None),
            P(("parts", "pts"), None),
            P("parts"),
            P("parts"),
        ),
        check_vma=False,
    )
```

```python
import functools

import jax
import jax.numpy as jnp
from jax import lax
from jax.experimental import pallas as pl
from jax.experimental.pallas import tpu as pltpu
from jax.sharding import PartitionSpec as P

BOXX = 16
BOXY = 16
BOXZ = 8
NTRIAL = 5
PACK = 16
BESIDE = 4
UNROLL = 32
VMEM_BYTES = 62 * 1024 * 1024

F32 = jnp.float32
BF16 = jnp.bfloat16
NT = (((1,), (1,)), ((), ()))
MESH = pl.DeviceIdType.MESH


class Place:
    def __init__(self, devices):
        me = lax.axis_index("pts")
        self.devices = devices
        self.depths = devices // 4
        self.me = me
        self.core = lax.rem(me, 2)
        self.side = lax.rem(lax.div(me, 2), 2)
        self.depth = lax.div(me, 4)
        self.half = lax.rem(self.depth, 2)
        self.beside = self.slot(self.depth, 1 - self.side, self.core)
        self.twin = self.slot(self.depth, self.side, 1 - self.core)
        self.mate = self.slot(self.depth + 1 - 2 * self.half, self.side, self.core)

    def slot(self, depth, side, core):
        return (depth * 2 + side) * 2 + core

    def along(self, depth):
        return self.slot(depth, self.side, self.core)

    def others(self, act):
        def one(far, carry):
            for way in (-1, 1):
                depth = self.depth + way * far

                @pl.when((depth >= 0) & (depth < self.depths))
                def _():
                    act(depth)

            return carry

        lax.fori_loop(1, self.depths, one, 0)

    def greet(self):
        barrier = pltpu.get_barrier_semaphore()

        def tell(device):
            pl.semaphore_signal(
                barrier, inc=1, device_id={"pts": device}, device_id_type=MESH
            )

        self.others(lambda depth: tell(self.along(depth)))
        tell(self.beside)
        tell(self.twin)

    def meet(self):
        pl.semaphore_wait(pltpu.get_barrier_semaphore(), self.depths + 1)

    def push(self, source, landing, send_sem, recv_sem, device):
        return pltpu.make_async_remote_copy(
            src_ref=source,
            dst_ref=landing,
            send_sem=send_sem,
            recv_sem=recv_sem,
            device_id={"pts": device},
            device_id_type=MESH,
        )


class Relay:
    def __init__(self, place, own, buf, sems, halved=False):
        self.place = place
        self.own = own
        self.buf = buf
        self.line_sem, self.side_sem, self.twin_sem, self.recv = sems
        self.pieces = self.recv.shape[1]
        self.size = buf.shape[1] // self.pieces
        self.halved = halved

    def own_rows(self, piece, depth):
        first = piece * self.size
        if self.halved:
            first = first + lax.rem(depth, 2) * self.buf.shape[1]
        return self.own.at[pl.ds(first, self.size)]

    def landing(self, slot, piece):
        return self.buf.at[slot, pl.ds(piece * self.size, self.size)]

    def line_copy(self, piece, depth):
        here = self.place
        return here.push(
            self.own_rows(piece, depth),
            self.landing(here.me, piece),
            self.line_sem.at[depth, piece],
            self.recv.at[here.me, piece],
            here.along(depth),
        )

    def side_copy(self, piece, depth, mine=False):
        here = self.place
        slot = here.along(depth)
        landing = self.landing(slot, piece)
        return here.push(
            self.own_rows(piece, depth) if mine else landing,
            landing,
            self.side_sem.at[depth, piece],
            self.recv.at[slot, piece],
            here.beside,
        )

    def twin_copy(self, piece, depth, side, mine=False):
        here = self.place
        slot = here.slot(depth, side, here.core)
        landing = self.landing(slot, piece)
        return here.push(
            self.own_rows(piece, depth) if mine else landing,
            landing,
            self.twin_sem.at[depth * 2 + side, piece],
            self.recv.at[slot, piece],
            here.twin,
        )

    def take(self, slot, piece):
        here = self.place
        landing = self.landing(slot, piece)
        here.push(
            landing, landing, self.twin_sem.at[0, piece], self.recv.at[slot, piece], here.twin
        ).wait_recv()

    def keep_own(self):
        here = self.place
        count = self.buf.shape[1]
        first = here.half * count if self.halved else 0
        self.buf[here.me] = self.own[pl.ds(first, count)]

    def start_lines(self):
        def one(piece, carry):
            self.place.others(lambda depth: self.line_copy(piece, depth).start())
            return carry

        lax.fori_loop(0, self.pieces, one, 0)

    def start_near(self, piece):
        here = self.place
        self.side_copy(piece, here.depth, mine=True).start()
        self.twin_copy(piece, here.depth, here.side, mine=True).start()

    def start_all_near(self):
        def one(piece, carry):
            self.start_near(piece)
            return carry

        lax.fori_loop(0, self.pieces, one, 0)

    def start_piece(self, piece):
        self.place.others(lambda depth: self.line_copy(piece, depth).start())
        self.start_near(piece)

    def start_own(self):
        def one(piece, carry):
            self.start_piece(piece)
            return carry

        lax.fori_loop(0, self.pieces, one, 0)

    def line_events(self, piece):
        here = self.place

        def one(depth):
            self.take(here.along(depth), piece)
            self.side_copy(piece, depth).start()
            self.twin_copy(piece, depth, here.side).start()

        here.others(one)

    def side_events(self, piece):
        here = self.place

        def one(depth):
            self.take(here.slot(depth, 1 - here.side, here.core), piece)
            self.twin_copy(piece, depth, 1 - here.side).start()

        one(here.depth)
        here.others(one)

    def twin_events(self, piece):
        here = self.place

        def one(pair, carry):
            self.take(pair * 2 + (1 - here.core), piece)
            return carry

        lax.fori_loop(0, here.devices // 2, one, 0)

    def head(self, wave):
        @pl.when(wave < self.pieces)
        def _():
            self.line_events(wave)

        @pl.when(wave == 1)
        def _():
            self.side_events(0)

    def run(self, first=0, work=None, steps=0, mix=None, tail=None, riders=(), follow=None):
        pieces = self.pieces

        def one(wave, carry):
            for rider in riders:

                @pl.when(wave == 0)
                def _():
                    rider.line_events(0)

                @pl.when(wave == 1)
                def _():
                    rider.side_events(0)

                @pl.when(wave == 2)
                def _():
                    rider.twin_events(0)

            @pl.when(wave < pieces)
            def _():
                self.line_events(wave)

            if tail is not None:

                @pl.when(wave == max(first, pieces - 1))
                def _():
                    tail()

            @pl.when((wave >= 1) & (wave < pieces + 1))
            def _():
                self.side_events(wave - 1)

            if follow is not None:

                @pl.when(wave >= pieces)
                def _():
                    follow.head(wave - pieces)

            if work is not None:

                @pl.when(wave - first < steps)
                def _():
                    work(wave - first)

            @pl.when(wave >= 2)
            def _():
                self.twin_events(wave - 2)
                if mix is not None:
                    mix(wave - 2)

            return carry

        lax.fori_loop(first, pieces + 2, one, 0)

    def finish(self):
        here = self.place

        def one(step, carry):
            piece = lax.div(step, here.depths)
            depth = lax.rem(step, here.depths)

            @pl.when(depth != here.depth)
            def _():
                self.line_copy(piece, depth).wait_send()

            self.side_copy(piece, depth).wait_send()
            self.twin_copy(piece, depth, 0).wait_send()
            self.twin_copy(piece, depth, 1).wait_send()
            return carry

        lax.fori_loop(0, self.pieces * here.depths, one, 0)


def relay_sems(devices, pieces):
    depths = devices // 4
    return [
        pltpu.SemaphoreType.DMA((depths, pieces)),
        pltpu.SemaphoreType.DMA((depths, pieces)),
        pltpu.SemaphoreType.DMA((depths * 2, pieces)),
        pltpu.SemaphoreType.DMA((devices, pieces)),
    ]


def mix_depth(planes_ref, kh_ref, kl_ref, image, group, size_x, first, count):
    devices, _, pack, lanes = planes_ref.shape

    def one(step, carry):
        at = first + step * 2
        pair = [planes_ref[:, at + t].reshape(devices * pack, lanes) for t in range(2)]
        rhs = jnp.concatenate(pair, axis=1)
        mixed = jnp.dot(kh_ref[...], rhs, preferred_element_type=F32)
        mixed = mixed + jnp.dot(kl_ref[...], rhs, preferred_element_type=F32)
        for t in range(2):
            for g in range(group):
                image[(at + t) * group + g] = mixed[
                    g * size_x : (g + 1) * size_x, t * lanes : (t + 1) * lanes
                ]
        return carry

    lax.fori_loop(0, count // 2, one, 0)


def split_offset(offset):
    bits_y, bits_z = BOXY.bit_length() - 1, BOXZ.bit_length() - 1
    return offset >> (bits_y + bits_z), (offset >> bits_z) & (BOXY - 1), offset & (BOXZ - 1)


def pick_values(image, half, corner, offset):
    half_z, _, size_y = image.shape
    cols = offset.shape[-1]
    at_x, at_y, at_z = corner & 255, (corner >> 8) & 255, corner >> 16
    from_z = at_z - half * half_z
    first = jnp.clip(from_z, 0, half_z - BOXZ)
    off_x, off_y, off_z = split_offset(offset)
    cell_z = off_z + (from_z - first)
    wide = BESIDE * BOXY
    box_rows = BOXZ // BESIDE * BOXX
    box_row = (cell_z >> (BESIDE.bit_length() - 1)) * BOXX + off_x
    box_cell = (cell_z & (BESIDE - 1)) * BOXY + off_y
    box = image[pl.ds(first, BOXZ), pl.ds(at_x, BOXX), :]
    lane = lax.broadcasted_iota(jnp.int32, (BOXX, size_y), 1)
    groups = []
    for z in range(0, BOXZ, BESIDE):
        group = pltpu.roll(box[z], lax.rem(size_y - at_y, size_y), axis=1)
        for k in range(1, BESIDE):
            shift = lax.rem(size_y + k * BOXY - at_y, size_y)
            plane = pltpu.roll(box[z + k], shift, axis=1)
            group = jnp.where(lane >= k * BOXY, plane, group)
        groups.append(group[:, :wide])
    box = jnp.concatenate(groups, axis=0).astype(BF16)
    cell_line = lax.broadcasted_iota(jnp.int32, (wide, cols), 0)
    pick_cell = jnp.where(cell_line == box_cell, 1.0, 0.0).astype(BF16)
    lines = jnp.dot(box, pick_cell, preferred_element_type=F32)
    row_line = lax.broadcasted_iota(jnp.int32, (box_rows, cols), 0)
    line = jnp.where(row_line == box_row, lines, 0.0)
    return jnp.sum(line, axis=0, keepdims=True)


def pick_blocks(image, half, corner_ref, line, offsets_ref, base, values, first, count):
    unroll = min(UNROLL, count)

    def some(part, carry):
        for k in range(unroll):
            block = first + part * unroll + k
            values[pl.ds(block, 1), :] = pick_values(
                image, half, corner_ref[line, block], offsets_ref[pl.ds(base + block, 1), :]
            )
        return carry

    lax.fori_loop(0, count // unroll, some, 0)


def power_below(value):
    return 1 << (value.bit_length() - 1)


def two_parts(value):
    high = value.astype(BF16)
    return high, (value - high.astype(F32)).astype(BF16)


def dot_parts(left, right):
    (left_high, left_low), (right_high, right_low) = left, right
    small = lax.dot_general(left_high, right_low, NT, preferred_element_type=F32)
    small = small + lax.dot_general(left_low, right_high, NT, preferred_element_type=F32)
    return small + lax.dot_general(left_high, right_high, NT, preferred_element_type=F32)


def mix_planes(field_of, kern_y, kern_z, rows, planes_ref, slab):
    size_z = kern_z[0].shape[0]
    for x in range(slab):
        inner = dot_parts(kern_z, two_parts(field_of(x)))
        rows[pl.ds(x, size_z, stride=slab), :] = dot_parts(two_parts(inner), kern_y)
    planes_ref[...] = rows[...].astype(BF16).reshape(planes_ref.shape)


def widen_kern(kern_x, slab, kh_ref, kl_ref):
    size_x, wide = kern_x.shape[0], kh_ref.shape[1]
    group = kh_ref.shape[0] // size_x
    pack = group * slab
    source = lax.broadcasted_iota(jnp.int32, (size_x, wide), 0)
    column = lax.broadcasted_iota(jnp.int32, (size_x, wide), 1)
    same = source == lax.div(column, pack) * slab + lax.rem(column, slab)
    layer = lax.div(lax.rem(column, pack), slab)
    for part, out_ref in zip(two_parts(kern_x), (kh_ref, kl_ref)):
        for g in range(group):
            select = jnp.where(same & (layer == g), 1.0, 0.0).astype(BF16)
            spot = jnp.dot(part, select, preferred_element_type=F32)
            out_ref[g * size_x : (g + 1) * size_x] = spot.astype(BF16)


def rank_blocks(corners, me, slab, ranks_ref, list_ref):
    devices, blocks = corners.shape
    from_x = (corners & 255) - me * slab
    touch = jnp.where((from_x < slab) & (from_x > -BOXX), 1.0, 0.0)
    earlier = lax.broadcasted_iota(jnp.int32, (blocks, blocks), 0)
    earlier = earlier < lax.broadcasted_iota(jnp.int32, (blocks, blocks), 1)
    within = jnp.dot(
        touch.astype(BF16), jnp.where(earlier, 1.0, 0.0).astype(BF16), preferred_element_type=F32
    )
    count = jnp.sum(touch, axis=1, keepdims=True)
    below = lax.broadcasted_iota(jnp.int32, (devices, devices), 1)
    below = below < lax.broadcasted_iota(jnp.int32, (devices, devices), 0)
    base = jnp.dot(
        jnp.where(below, 1.0, 0.0).astype(BF16),
        jnp.broadcast_to(count, (devices, blocks)).astype(BF16),
        preferred_element_type=F32,
    )
    ranks = jnp.where(touch > 0.0, base + within, -1.0)
    for device in range(devices):
        line = jnp.broadcast_to(ranks[device : device + 1], (blocks, blocks))
        ranks_ref[device] = jnp.transpose(line)
    total = jnp.sum(touch)
    list_ref[pl.ds(devices, 8), :] = jnp.full((8, blocks), total, F32).astype(jnp.int32)


def list_blocks(ranks_ref, list_ref, line):
    devices, blocks, _ = ranks_ref.shape
    wanted = lax.broadcasted_iota(jnp.int32, (blocks, blocks), 1) + line * blocks
    wanted = wanted.astype(F32)
    block = lax.broadcasted_iota(jnp.int32, (blocks, blocks), 0).astype(F32)

    def one(device, ids):
        hit = ranks_ref[device] == wanted
        start = (device * blocks).astype(F32)
        return ids + jnp.where(hit, block + start, 0.0)

    ids = lax.fori_loop(0, devices, one, jnp.zeros((blocks, blocks), F32))
    ids = jnp.sum(ids, axis=0, keepdims=True)
    list_ref[pl.ds(line, 1), :] = ids.astype(jnp.int32)


def log_sigmoid(value):
    return jnp.minimum(value, 0.0) - jnp.log1p(jnp.exp(-jnp.abs(value)))


def apply_interp(values, interp, outs, first, count):
    unroll = min(UNROLL, count)
    cols = values[0].shape[1]

    def some(part, carry):
        for k in range(unroll):
            block = first + part * unroll + k
            top = lax.broadcasted_iota(jnp.int32, (8, cols), 0)
            rows = jnp.broadcast_to(values[0][pl.ds(block, 1), :], (8, cols))
            for f in range(1, len(values)):
                rows = jnp.where(top == f, values[f][pl.ds(block, 1), :], rows)
            line = lax.dot_general(
                rows.astype(BF16), interp[block], NT, preferred_element_type=F32
            )
            for f, out_ref in enumerate(outs):
                out_ref[pl.ds(block, 1), :] = line[f : f + 1]
        return carry

    lax.fori_loop(0, count // unroll, some, 0)


def forward_kernel(
    group,
    trial_ref,
    accept_ref,
    corner_ref,
    offsets_ref,
    kern_x_ref,
    kern_y_ref,
    kern_z_ref,
    labels_ref,
    weights_ref,
    direction_ref,
    interp_ref,
    prob_ref,
    split_ref,
    list_ref,
    corners_ref,
    pair_packed,
    pair_offsets,
    all_offs,
    all_terms,
    kh_ref,
    kl_ref,
    own_u,
    own_d,
    packed_ref,
    offs_ref,
    buf_u,
    buf_d,
    all_packed,
    image_u,
    image_d,
    interp,
    mine_u,
    mine_d,
    theirs,
    out_u,
    out_d,
    in_u,
    in_d,
    mate_offs,
    rows_u,
    rows_d,
    mate_u,
    mate_d,
    latent_ref,
    slope_ref,
    res_ref,
    own_terms,
    weights_t,
    direction_t,
    ranks_ref,
    corner_smem,
    local_sem,
    mate_send,
    mate_recv,
    *sems,
):
    devices = buf_u.shape[0]
    blocks, per_block = labels_ref.shape
    slab, size_y, size_z = weights_ref.shape
    half_z, size_x, _ = image_u.shape
    place = Place(devices)
    place.greet()
    load = pltpu.make_async_copy(interp_ref, interp, local_sem.at[0])
    load.start()
    u = Relay(place, own_u, buf_u, sems[0:4], halved=True)
    d = Relay(place, own_d, buf_d, sems[4:8], halved=True)
    o = Relay(place, offs_ref, all_offs, sems[8:12])
    t = Relay(place, own_terms, all_terms, sems[12:16])
    c = Relay(place, packed_ref, all_packed, sems[16:20])

    def swap(source, landing, k):
        return place.push(source, landing, mate_send.at[k], mate_recv.at[k], place.mate)

    swaps = [
        swap(offs_ref, mate_offs, 0),
        swap(out_u, in_u, 1),
        swap(out_d, in_d, 2),
        swap(rows_u, mate_u, 3),
        swap(rows_d, mate_d, 4),
    ]
    kern_y, kern_z = two_parts(kern_y_ref[...]), two_parts(kern_z_ref[...])
    packed = corner_ref[0:1] + corner_ref[1:2] * 256 + corner_ref[2:3] * 65536
    packed_ref[...] = jnp.broadcast_to(packed, packed_ref.shape)
    offs_ref[...] = offsets_ref[...].astype(jnp.int16)
    mix_planes(lambda x: weights_ref[x], kern_y, kern_z, weights_t, own_u, slab)
    pair_offsets[pl.ds(0, blocks)] = offsets_ref[...]
    widen_kern(kern_x_ref[...], slab, kh_ref, kl_ref)
    place.meet()
    c.start_own()
    u.start_own()
    swaps[0].start()
    mix_planes(lambda x: direction_ref[x], kern_y, kern_z, direction_t, own_d, slab)
    for relay in (c, u, d, o):
        relay.keep_own()
    for x in range(slab):
        weights_t[pl.ds(x, size_z, stride=slab), :] = jnp.transpose(weights_ref[x])
        direction_t[pl.ds(x, size_z, stride=slab), :] = jnp.transpose(direction_ref[x])
    d.start_lines()
    o.start_lines()

    def mixer(relay, image):
        return lambda piece: mix_depth(
            relay.buf, kh_ref, kl_ref, image, group, size_x, piece * relay.size, relay.size
        )

    last = u.pieces + 1
    to_smem = pltpu.make_async_copy(pair_packed, corner_smem, local_sem.at[1])

    def list_lines(first, count):
        def one(line, carry):
            list_blocks(ranks_ref, list_ref, line)
            return carry

        lax.fori_loop(first, first + count, one, 0)

    def prepare(wave):
        @pl.when(wave == 2)
        def _():
            corners = all_packed[:, 0, :]
            corners_ref[...] = corners
            pair_packed[...] = jnp.concatenate(
                [packed_ref[0:4], all_packed[place.mate, 0:4]], axis=0
            )
            rank_blocks(corners, place.me, slab, ranks_ref, list_ref)
            to_smem.start()

        for k in range(2):

            @pl.when(wave == min(3 + k, last))
            def _():
                list_lines(devices // 2 * k, devices // 2)

    u.run(
        work=prepare,
        steps=last + 1,
        mix=mixer(u, image_u),
        tail=d.start_all_near,
        riders=(c,),
        follow=d,
    )
    swaps[0].wait()
    pair_offsets[pl.ds(blocks, blocks)] = mate_offs[...].astype(jnp.int32)
    to_smem.wait()
    steps = power_below(u.pieces)
    some = blocks // steps

    def pick(image, mine, first, count):
        line, base = (0, 0) if mine is not theirs else (4, blocks)
        pick_blocks(
            image, place.half, corner_smem, line, pair_offsets, base, mine, first, count
        )

    both = (half_z * slab, size_y)
    mate_rows = pl.ds(pl.multiple_of(place.mate * slab, slab), slab)

    def early(step):
        pick(image_u, theirs, step * some, some)
        pick(image_u, mine_u, step * some, some)

        @pl.when(step == steps - 1)
        def _():
            out_u[...] = theirs[...].astype(BF16)
            rows_u[...] = image_u[:, mate_rows, :].reshape(both).astype(BF16)

    d.run(first=2, work=early, steps=steps, mix=mixer(d, image_d), tail=o.start_all_near)
    swaps[1].start()
    pick(image_d, theirs, 0, blocks)
    out_d[...] = theirs[...].astype(BF16)
    rows_d[...] = image_d[:, mate_rows, :].reshape(both).astype(BF16)
    pick(image_d, mine_d, 0, blocks // 4)
    for k in (2, 3, 4):
        swaps[k].start()
    o.line_events(0)
    pick(image_d, mine_d, blocks // 4, blocks - blocks // 4)
    swaps[1].wait()
    mine_u[...] = mine_u[...] + in_u[...].astype(F32)
    load.wait()
    swaps[2].wait()
    mine_d[...] = mine_d[...] + in_d[...].astype(F32)
    target = labels_ref[...].astype(F32)
    part = blocks // 2
    unroll = min(UNROLL, part)

    def back(first):
        def one(step, carry):
            for k in range(unroll):
                block = first + step * unroll + k
                row = jnp.broadcast_to(res_ref[pl.ds(block, 1), :], (8, per_block))
                term = jnp.dot(row.astype(BF16), interp[block], preferred_element_type=F32)
                theirs[pl.ds(block, 1), :] = term[0:1]
            return carry

        lax.fori_loop(0, part // unroll, one, 0)

    for piece in range(2):
        rows = slice(piece * part, (piece + 1) * part)
        apply_interp((mine_u, mine_d), interp, (latent_ref, slope_ref), piece * part, part)
        if piece > 0:
            t.start_piece(0)
            o.side_events(0)
        prob = jax.nn.sigmoid(latent_ref[rows] + trial_ref[accept_ref[0]] * slope_ref[rows])
        prob_ref[rows] = prob
        res_ref[rows] = (target[rows] - prob).astype(BF16).astype(F32)
        back(piece * part)
        own_terms[rows] = theirs[rows].astype(BF16)
    t.keep_own()
    for relay in (c, u, d):
        relay.finish()
    t.start_piece(1)
    t.line_events(0)
    slope = slope_ref[...]
    latent = latent_ref[...]
    swaps[3].wait()
    swaps[4].wait()
    own_rows = pl.ds(pl.multiple_of(place.me * slab, slab), slab)
    here_z = pl.ds(pl.multiple_of(place.half * half_z * slab, slab), half_z * slab)
    there_z = pl.ds(pl.multiple_of((1 - place.half) * half_z * slab, slab), half_z * slab)

    def quad(field_t, image, mate):
        near = field_t[here_z] * image[:, own_rows, :].reshape(both)
        return jnp.sum(near + field_t[there_z] * mate[...].astype(F32))

    signed = 2.0 * target - 1.0
    line = lax.broadcasted_iota(jnp.int32, (8, 128), 0)
    lane = lax.broadcasted_iota(jnp.int32, (8, 128), 1)
    sums = jnp.zeros((8, 128), F32)
    for k in range(NTRIAL):
        at_trial = latent + trial_ref[k] * slope
        loglik = jnp.sum(log_sigmoid(signed * at_trial))
        descent = jnp.sum((target - jax.nn.sigmoid(at_trial)) * slope)
        sums = jnp.where((line == 0) & (lane == k), loglik, sums)
        sums = jnp.where((line == 1) & (lane == k), descent, sums)
    sums = jnp.where(line == 2, quad(weights_t, image_u, mate_u), sums)
    sums = jnp.where(line == 3, quad(direction_t, image_u, mate_u), sums)
    sums = jnp.where(line == 4, quad(direction_t, image_d, mate_d), sums)
    first = sums.astype(BF16).astype(F32)
    second = (sums - first).astype(BF16).astype(F32)
    third = sums - first - second
    split_ref[...] = jnp.concatenate([first, second, third], axis=0).astype(BF16)
    t.side_events(0)
    t.line_events(1)
    o.twin_events(0)
    t.side_events(1)
    t.twin_events(0)
    o.finish()
    t.twin_events(1)
    t.finish()


def bend_kernel(
    group,
    points,
    corner_smem,
    trial_ref,
    own_ref,
    split_ref,
    kh_ref,
    kl_ref,
    pair_offsets,
    prob_ref,
    interp_ref,
    out_ref,
    trials_ref,
    buf,
    all_split,
    image,
    interp,
    mine,
    theirs,
    sent,
    got,
    local_sem,
    mate_send,
    mate_recv,
    *sems,
):
    devices = buf.shape[0]
    blocks = prob_ref.shape[0]
    size_x = image.shape[1]
    place = Place(devices)
    load = pltpu.make_async_copy(interp_ref, interp, local_sem)
    load.start()
    b = Relay(place, own_ref, buf, sems[0:4], halved=True)
    s = Relay(place, split_ref, all_split, sems[4:8])
    swap = place.push(sent, got, mate_send, mate_recv, place.mate)
    place.greet()
    b.keep_own()
    s.keep_own()
    place.meet()
    s.start_own()
    b.start_own()
    b.run(
        mix=lambda piece: mix_depth(
            buf, kh_ref, kl_ref, image, group, size_x, piece * b.size, b.size
        ),
        riders=(s,),
    )

    def pick(line, base, values, first, count):
        pick_blocks(
            image, place.half, corner_smem, line, pair_offsets, base, values, first, count
        )

    pick(4, blocks, theirs, 0, blocks)
    sent[...] = theirs[...].astype(BF16)
    pick(0, 0, mine, 0, blocks // 4)
    swap.start()
    pick(0, 0, mine, blocks // 4, blocks - blocks // 4)
    total = jnp.sum(all_split[...].astype(F32), axis=0)
    total = total[0:8] + total[8:16] + total[16:24]
    lane = lax.broadcasted_iota(jnp.int32, (1, 128), 1)
    step = jnp.zeros((1, 128), F32)
    for k in range(NTRIAL):
        step = jnp.where(lane == k, trial_ref[k], step)
    loglik, descent, quad_gu, quad_du, quad_dv = (total[k : k + 1] for k in range(5))
    prior = 0.5 * (quad_gu + 2.0 * step * quad_du + step * step * quad_dv)
    trials_ref[0:1] = (loglik - prior) / points
    trials_ref[1:2] = (descent - quad_du - step * quad_dv) / points
    load.wait()
    swap.wait()
    mine[...] = mine[...] + got[...].astype(F32)
    apply_interp((mine,), interp, (out_ref,), 0, blocks)
    prob = prob_ref[...]
    out_ref[...] = prob * (1.0 - prob) * out_ref[...]
    b.finish()
    s.finish()


def spread_kernel(
    list_ref,
    corners_ref,
    trial_ref,
    accept_ref,
    offs_ref,
    terms_ref,
    weights_ref,
    direction_ref,
    kern_y_ref,
    kern_z_ref,
    new_ref,
    grad_ref,
    planes_ref,
    offs,
    terms,
    spread,
):
    devices, blocks, cols = offs_ref.shape
    slab, size_y, size_z = weights_ref.shape
    rows = BOXZ * slab
    unroll = UNROLL
    me = lax.axis_index("pts")
    spread[...] = jnp.zeros_like(spread)

    def widen(device, carry):
        offs[pl.ds(pl.multiple_of(device * blocks, blocks), blocks)] = offs_ref[device].astype(
            jnp.int32
        )
        terms[pl.ds(pl.multiple_of(device * blocks, blocks), blocks)] = terms_ref[device].astype(
            F32
        )
        return carry

    lax.fori_loop(0, devices, widen, 0)
    count = list_ref[devices, 0]

    def some(part, carry):
        sums = []
        for k in range(unroll):
            at = part * unroll + k
            block = list_ref[lax.div(at, blocks), lax.rem(at, blocks)]
            packed = corners_ref[lax.div(block, blocks), lax.rem(block, blocks)]
            from_x = jnp.where(at < count, (packed & 255) - me * slab, -2 * BOXX)
            at_y = (packed >> 8) & 255
            at_z = packed >> 16
            off_x, off_y, off_z = split_offset(offs[pl.ds(block, 1), :])
            cell = off_x + from_x
            key = jnp.where((cell >= 0) & (cell < slab), off_z * slab + cell, -1)
            row_line = lax.broadcasted_iota(jnp.int32, (rows, cols), 0)
            y_line = lax.broadcasted_iota(jnp.int32, (BOXY, cols), 0)
            left = jnp.where(row_line == key, terms[pl.ds(block, 1), :], 0.0).astype(BF16)
            right = jnp.where(y_line == off_y, 1.0, 0.0).astype(BF16)
            piece = lax.dot_general(left, right, NT, preferred_element_type=F32)
            piece = jnp.concatenate([piece, jnp.zeros((rows, size_y - BOXY), F32)], axis=1)
            sums.append((at_z, pltpu.roll(piece, at_y, axis=1)))
        for at_z, piece in sums:
            spread[pl.ds(pl.multiple_of(at_z * slab, slab), rows), :] += piece
        return carry

    lax.fori_loop(0, lax.div(count + unroll - 1, unroll), some, 0)
    chosen = trial_ref[accept_ref[0]]
    for x in range(slab):
        new = weights_ref[x] + chosen * direction_ref[x]
        new_ref[x] = new
        grad_ref[x] = jnp.transpose(spread[pl.ds(x, size_z, stride=slab), :]) - new
    kern_y, kern_z = two_parts(kern_y_ref[...]), two_parts(kern_z_ref[...])
    mix_planes(lambda x: grad_ref[x], kern_y, kern_z, spread, planes_ref, slab)


def body(
    grid_weights,
    direction,
    kern_x,
    kern_y,
    kern_z,
    interp,
    block_corner,
    block_offsets,
    labels,
    trial_steps,
    accept,
):
    slab, size_y, size_z = grid_weights.shape
    size_x = kern_x.shape[0]
    devices = lax.axis_size("pts")
    blocks, cols = block_offsets.shape
    per_block = interp.shape[1]
    points = blocks * per_block * devices
    group = max(1, PACK // slab)
    pack = group * slab
    units = size_z // group
    pieces = max(1, 64 // devices)

    smem = pl.BlockSpec(memory_space=pltpu.SMEM)
    vmem = pl.BlockSpec(memory_space=pltpu.VMEM)
    hbm = pl.BlockSpec(memory_space=pl.ANY)
    limit = dict(vmem_limit_bytes=VMEM_BYTES)
    planes_shape = jax.ShapeDtypeStruct((units, pack, size_y), BF16)
    rows_scratch = pltpu.VMEM((size_z * slab, size_y), F32)
    planes_scratch = pltpu.VMEM((devices, units // 2, pack, size_y), BF16)
    image_scratch = pltpu.VMEM((size_z // 2, size_x, size_y), F32)
    interp_scratch = pltpu.VMEM(interp.shape, BF16)
    point_scratch = pltpu.VMEM((blocks, per_block), F32)
    point_shape = jax.ShapeDtypeStruct((blocks, per_block), F32)

    wide_shape = jax.ShapeDtypeStruct((group * size_x, devices * pack), BF16)
    chunk_scratch = pltpu.VMEM((units, pack, size_y), BF16)
    pick_scratch = pltpu.VMEM((blocks, cols), F32)
    swap_scratch = pltpu.VMEM((blocks, cols), BF16)
    mate_scratch = pltpu.VMEM((size_z // 2 * slab, size_y), BF16)
    (
        probability,
        split,
        block_list,
        corners,
        pair_packed,
        pair_offsets,
        offsets,
        terms,
        kern_high,
        kern_low,
    ) = (
        pl.pallas_call(
            functools.partial(forward_kernel, group),
            in_specs=[smem] * 2 + [vmem] * 8 + [hbm],
            out_specs=[vmem] * 10,
            out_shape=[
                point_shape,
                jax.ShapeDtypeStruct((24, 128), BF16),
                jax.ShapeDtypeStruct((devices + 8, blocks), jnp.int32),
                jax.ShapeDtypeStruct((devices, blocks), jnp.int32),
                jax.ShapeDtypeStruct((8, blocks), jnp.int32),
                jax.ShapeDtypeStruct((2 * blocks, cols), jnp.int32),
                jax.ShapeDtypeStruct((devices, blocks, cols), jnp.int16),
                jax.ShapeDtypeStruct((devices, blocks, cols), BF16),
                wide_shape,
                wide_shape,
            ],
            scratch_shapes=[
                chunk_scratch,
                chunk_scratch,
                pltpu.VMEM((8, blocks), jnp.int32),
                pltpu.VMEM((blocks, cols), jnp.int16),
                planes_scratch,
                planes_scratch,
                pltpu.VMEM((devices, 8, blocks), jnp.int32),
                image_scratch,
                image_scratch,
                interp_scratch,
                pick_scratch,
                pick_scratch,
                pick_scratch,
                swap_scratch,
                swap_scratch,
                swap_scratch,
                swap_scratch,
                pltpu.VMEM((blocks, cols), jnp.int16),
                mate_scratch,
                mate_scratch,
                mate_scratch,
                mate_scratch,
                point_scratch,
                point_scratch,
                point_scratch,
                swap_scratch,
                rows_scratch,
                rows_scratch,
                pltpu.VMEM((devices, blocks, blocks), F32),
                pltpu.SMEM((8, blocks), jnp.int32),
                pltpu.SemaphoreType.DMA((2,)),
                pltpu.SemaphoreType.DMA((5,)),
                pltpu.SemaphoreType.DMA((5,)),
                *relay_sems(devices, pieces),
                *relay_sems(devices, pieces),
                *relay_sems(devices, 1),
                *relay_sems(devices, 2),
                *relay_sems(devices, 1),
            ],
            compiler_params=pltpu.CompilerParams(
                collective_id=0, has_side_effects=True, **limit
            ),
            name="forward",
        )(
            trial_steps,
            accept,
            block_corner,
            block_offsets,
            kern_x,
            kern_y,
            kern_z,
            labels,
            grid_weights,
            direction,
            interp,
        )
    )

    new_weights, grid_gradient, bend_planes = pl.pallas_call(
        spread_kernel,
        in_specs=[smem] * 4 + [vmem] * 6,
        out_specs=[vmem] * 3,
        out_shape=[
            jax.ShapeDtypeStruct(grid_weights.shape, F32),
            jax.ShapeDtypeStruct(grid_weights.shape, F32),
            planes_shape,
        ],
        scratch_shapes=[
            pltpu.VMEM((devices * blocks, cols), jnp.int32),
            pltpu.VMEM((devices * blocks, cols), F32),
            rows_scratch,
        ],
        compiler_params=pltpu.CompilerParams(**limit),
        name="spread",
    )(
        block_list,
        corners,
        trial_steps,
        accept,
        offsets,
        terms,
        grid_weights,
        direction,
        kern_y,
        kern_z,
    )

    curvature, trials = pl.pallas_call(
        functools.partial(bend_kernel, group, points),
        in_specs=[smem] * 2 + [vmem] * 6 + [hbm],
        out_specs=[vmem] * 2,
        out_shape=[point_shape, jax.ShapeDtypeStruct((2, 128), F32)],
        scratch_shapes=[
            planes_scratch,
            pltpu.VMEM((devices, 24, 128), BF16),
            image_scratch,
            interp_scratch,
            pick_scratch,
            pick_scratch,
            swap_scratch,
            swap_scratch,
            pltpu.SemaphoreType.DMA,
            pltpu.SemaphoreType.DMA,
            pltpu.SemaphoreType.DMA,
            *relay_sems(devices, max(1, pieces // 2)),
            *relay_sems(devices, 1),
        ],
        compiler_params=pltpu.CompilerParams(collective_id=1, has_side_effects=True, **limit),
        name="bend",
    )(
        pair_packed,
        trial_steps,
        bend_planes,
        split,
        kern_high,
        kern_low,
        pair_offsets,
        probability,
        interp,
    )
    return (new_weights, grid_gradient, curvature, trials[0, :NTRIAL], trials[1, :NTRIAL])


def solution(mesh):
    return jax.shard_map(
        body,
        mesh=mesh,
        in_specs=(
            P(("parts", "pts"), None, None),
            P(("parts", "pts"), None, None),
            P(),
            P(),
            P(),
            P(("parts", "pts"), None, None),
            P(None, ("parts", "pts")),
            P(("parts", "pts"), None),
            P(("parts", "pts"), None),
            P(),
            P(),
        ),
        out_specs=(
            P(("parts", "pts"), None, None),
            P(("parts", "pts"), None, None),
            P(("parts", "pts"), None),
            P("parts"),
            P("parts"),
        ),
        check_vma=False,
    )
```
